256 devices in a mesh: lat: 8 (over z), lon: 16 (over x, y), obs: 2 (over core).
Axes of the slice: x: 4, y: 4, z: 8, core: 2. Of those that a mesh axis runs over, the one named last changes fastest.
Arguments:
- innovation: float32 [32768, 128], P(('lat', 'lon', 'obs')), may hold values from -6 to 6
- obs_error: float32 [32768, 128], P(('lat', 'lon', 'obs')), may hold values from 0.5 to 2
- obs_offset: float32 [2, 32768, 128], P(None, ('lat', 'lon', 'obs')), may hold values from 0 to 1
- obs_cell: int32 [32768, 128], P(('lat', 'lon', 'obs')), may hold values from 0 to 65535
- obs_owner: int32 [256, 128], P(('lat', 'lon', 'obs')), may hold values from 0 to 127, as said below
- block_count: int32 [256], P(('lat', 'lon', 'obs')), may hold values from 64 to 128
- land_mask: int32 [512, 16384], P(('lat', 'obs'), 'lon'), may hold values from 0 to 1, as said below
- inertia: float32 [512, 16384], P(('lat', 'obs'), 'lon'), may hold values from 0.002 to 0.05
- sea_depth: float32 [512, 16384], P(('lat', 'obs'), 'lon'), may hold values from 0.5 to 5
Outputs:
- adjoint_field: float32 [512, 16384], P(('lat', 'obs'), 'lon')
- residual: float32 [512, 16384], P(('lat', 'obs'), 'lon')
The draws below stay inside these ranges and needn't reach their ends.
Inputs may be any that keep to these rules, and one draw needn't show every extreme that they name: `obs_owner`: among the live blocks of one device at most 3 name the same tile; in every draw some tile is named by exactly 3 live blocks of every device. `land_mask`: the first and the last grid row are land.
All inputs are finite; a program needn't handle non-finite values.
Results may differ from the reference program's by a relative error of at most 0.0003.
Values sent between devices are 32-bit elements; how exact they have to be, the bound alone decides.
No kernel may reach another device: no remote copies, remote signals or barrier semaphores. Data moves between devices by JAX's collectives and lax.ppermute only.
A program may use at most 64 MiB of HBM per device.

```python
import math
import jax
import jax.numpy as jnp

TILE_R = 64
TILE_C = 1024
NBLK = 128
BLOCK = 128
ITERS = 5
CAPB = 3
NLAT = 512
NLON = 16384
N_LAT = 8
N_LON = 16
DEVICES = 256


def owner_plan(key):
    tile_count = N_LAT * N_LON
    slot_total = tile_count * CAPB
    base_key = jax.random.fold_in(key, 7711)
    block_counts = jax.random.randint(jax.random.fold_in(base_key, 1), (DEVICES,), NBLK // 2, NBLK + 1)
    hot_tile = jax.random.randint(jax.random.fold_in(base_key, 2), (), 0, tile_count)
    device_keys = jax.random.split(jax.random.fold_in(base_key, 3), DEVICES)

    def device_plan(dev_key, live_total):
        perm_key, mix_key = jax.random.split(dev_key)
        shuffled = jax.random.permutation(perm_key, slot_total)
        slot_ids = jnp.arange(slot_total)
        is_hot = slot_ids // CAPB == hot_tile
        sort_key = jnp.where(is_hot, slot_ids - slot_total, shuffled)
        chosen = jnp.argsort(sort_key)[:NBLK]
        owners = chosen // CAPB
        block_ids = jnp.arange(NBLK)
        mixing = jax.random.permutation(mix_key, NBLK)
        live_key = jnp.where(block_ids < live_total, mixing, NBLK + block_ids)
        return owners[jnp.argsort(live_key)]
    owners = jax.vmap(device_plan)(device_keys, block_counts)
    return (block_counts.astype(jnp.int32), owners.astype(jnp.int32))


def draw_obs_owner(key, part):
    return owner_plan(key)[1]


def draw_block_count(key, part):
    return owner_plan(key)[0]


def draw_land_mask(key, part):
    land_bits = jax.random.randint(jax.random.fold_in(key, 913), (NLAT, NLON), 0, 10)
    row_ids = jnp.arange(NLAT)[:, None]
    ocean = (land_bits < 7) & (row_ids > 0) & (row_ids < NLAT - 1)
    return ocean.astype(jnp.int32)


def touch_ends(result, rng, smallest, top_value):
    shape = result.shape
    index_at = [jax.random.randint(jax.random.fold_in(rng, axis), (), 0, shape[axis]) for axis in range(len(shape))]
    result = result.at[tuple(index_at)].set(smallest)
    longest = shape.index(max(shape))
    index_at[longest] = (index_at[longest] + 1) % shape[longest]
    return result.at[tuple(index_at)].set(top_value)


def block_levels(own_key, extent, cuts, smallest, high):
    level, own = 1.0, jax.random.fold_in(own_key, 6)
    for axis_at, blocks in cuts:
        steps = jnp.exp(jax.random.uniform(jax.random.fold_in(own, axis_at), (blocks,), jnp.float32, smallest / len(cuts), high / len(cuts)))
        level = level * jnp.repeat(steps, extent[axis_at] // blocks).reshape([-1 if axis == axis_at else 1 for axis in range(len(extent))])
    return level


def bell_draw(key, shape, deviation, limit, cuts=(), held_as=jnp.bfloat16):
    gain = block_levels(key, shape, cuts, -0.22, 0.18) if cuts else 1.0
    array = jax.random.normal(key, shape, jnp.float32) * deviation * gain
    return jnp.minimum(jnp.maximum(array, -limit), limit).astype(held_as)


def setup_inputs(seed: int = 0) -> dict:
    splits = jax.random.split(jax.random.key(seed), 10)
    return {
        "innovation": bell_draw(splits[0], (DEVICES * NBLK, BLOCK), 1.0, 6.0, ((0, 256),), jnp.float32),
        "obs_error": jnp.clip(jnp.exp(math.log(2.0) - 1.3862944 * jax.random.uniform(splits[1], (DEVICES * NBLK, BLOCK), jnp.float32) ** block_levels(splits[1], (DEVICES * NBLK, BLOCK), ((0, 256),), -0.2, 0.2)), 0.5, 2.0),
        "obs_offset": jnp.clip(1.0 * jax.random.uniform(splits[2], (2, DEVICES * NBLK, BLOCK), jnp.float32) ** block_levels(splits[2], (2, DEVICES * NBLK, BLOCK), ((1, 256),), -0.2, 0.2), 0.0, 1.0),
        "obs_cell": touch_ends(jax.random.randint(splits[3], (DEVICES * NBLK, BLOCK), 0, TILE_R * TILE_C), jax.random.fold_in(splits[3], 1), 0, (TILE_R * TILE_C) - 1).astype(jnp.int32),
        "obs_owner": draw_obs_owner(jax.random.fold_in(splits[9], 71), 0),
        "block_count": draw_block_count(jax.random.fold_in(splits[9], 71), 0),
        "land_mask": draw_land_mask(jax.random.fold_in(splits[9], 71), 0),
        "inertia": jnp.clip(jnp.exp(math.log(0.05) - 3.218876 * jax.random.uniform(splits[7], (NLAT, NLON), jnp.float32) ** block_levels(splits[7], (NLAT, NLON), ((0, 16), (1, 16)), -0.2, 0.2)), 0.002, 0.05),
        "sea_depth": jnp.clip(jnp.exp(math.log(5.0) - 2.3025851 * jax.random.uniform(splits[8], (NLAT, NLON), jnp.float32) ** block_levels(splits[8], (NLAT, NLON), ((0, 16), (1, 16)), -0.2, 0.2)), 0.5, 5.0),
    }


def reference(innovation, obs_error, obs_offset, obs_cell, obs_owner, block_count, land_mask, inertia, sea_depth):
    is_live = (jnp.arange(NBLK)[None, :] < block_count[:, None]).reshape(-1)
    owner_tile = obs_owner.reshape(-1)
    scaled = jnp.where(is_live[:, None], innovation / (obs_error * obs_error), jnp.float32(0.0))
    north_frac = obs_offset[0]
    east_frac = obs_offset[1]
    cell_row = (owner_tile // N_LON)[:, None] * TILE_R + obs_cell // TILE_C
    cell_col = (owner_tile % N_LON)[:, None] * TILE_C + obs_cell % TILE_C
    next_col = (cell_col + 1) % NLON
    next_row = cell_row + 1
    cell_total = NLAT * NLON
    inside = next_row < NLAT
    segment_ids = jnp.concatenate([(cell_row * NLON + cell_col).reshape(-1), (cell_row * NLON + next_col).reshape(-1), jnp.where(inside, next_row * NLON + cell_col, cell_total).reshape(-1), jnp.where(inside, next_row * NLON + next_col, cell_total).reshape(-1)]).astype(jnp.int32)
    contribs = jnp.concatenate([(scaled * ((1.0 - north_frac) * (1.0 - east_frac))).reshape(-1), (scaled * ((1.0 - north_frac) * east_frac)).reshape(-1), (scaled * (north_frac * (1.0 - east_frac))).reshape(-1), (scaled * (north_frac * east_frac)).reshape(-1)])
    partial_value = jax.ops.segment_sum(contribs, segment_ids, num_segments=cell_total + 1)[:cell_total]
    ocean = land_mask.astype(jnp.float32)
    forcing = partial_value.reshape(NLAT, NLON) * ocean
    conduct = ocean * sea_depth
    cond_north = jnp.sqrt(conduct * jnp.roll(conduct, 1, 0))
    cond_south = jnp.sqrt(conduct * jnp.roll(conduct, -1, 0))
    cond_west = jnp.sqrt(conduct * jnp.roll(conduct, 1, 1))
    cond_east = jnp.sqrt(conduct * jnp.roll(conduct, -1, 1))
    diagonal = inertia + cond_north + cond_south + cond_west + cond_east

    def operate(field):
        return diagonal * field - cond_north * jnp.roll(field, 1, 0) - cond_south * jnp.roll(field, -1, 0) - cond_west * jnp.roll(field, 1, 1) - cond_east * jnp.roll(field, -1, 1)
    adjoint_field = jnp.zeros_like(forcing)
    residual = forcing
    direction = forcing
    norm_now = jnp.sum(residual * residual)
    for iteration in range(ITERS):
        applied = operate(direction)
        step_size = norm_now / jnp.sum(direction * applied)
        adjoint_field = adjoint_field + step_size * direction
        residual = residual - step_size * applied
        norm_next = jnp.sum(residual * residual)
        direction = residual + norm_next / norm_now * direction
        norm_now = norm_next
    return (adjoint_field, residual)
```

```python
import jax
import jax.numpy as jnp
from jax import lax
from jax.experimental import pallas as pl
from jax.experimental.pallas import tpu as pltpu
from jax.sharding import Mesh
from jax.sharding import PartitionSpec as P

ITERS = 5
MOMENTS = 2 * ITERS
CAP = 3
WORDS = 4
LON = ("lon_0", "lon_1")
LAT_OBS = ("lat", "obs")
LAT_LON_OBS = ("lat", "lon_0", "lon_1", "obs")
LAT_LON = ("lat", "lon_0", "lon_1")
F32 = jnp.float32
BF16 = jnp.bfloat16
GROUPS = 2
CHUNK = 8


def vmem():
    return pl.BlockSpec(memory_space=pltpu.VMEM)


def smem():
    return pl.BlockSpec(memory_space=pltpu.SMEM)


def pack_kernel(owner, count, innovation, error, offset, cell, out, rows, seen):
    blocks = innovation.shape[0]
    tiles = out.shape[0] // (CAP * WORDS)
    err = error[...]
    rows[pl.ds(0, blocks, stride=WORDS), :] = innovation[...] / (err * err)
    rows[pl.ds(1, blocks, stride=WORDS), :] = offset[0]
    rows[pl.ds(2, blocks, stride=WORDS), :] = offset[1]
    rows[pl.ds(3, blocks, stride=WORDS), :] = cell[...].astype(F32)
    out[...] = jnp.zeros(out.shape, F32)

    def clear(tile, carry):
        seen[tile] = 0
        return carry

    lax.fori_loop(0, tiles, clear, 0)

    def place(block, carry):
        tile = owner[0, block]
        rank = seen[tile]
        seen[tile] = rank + 1
        slot = tile * CAP + rank
        out[pl.ds(slot * WORDS, WORDS), :] = rows[pl.ds(block * WORDS, WORDS), :]
        return carry

    lax.fori_loop(0, count[0], place, 0)


def pack(owner, count, innovation, error, offset, cell, tiles):
    blocks = innovation.shape[0]
    return pl.pallas_call(
        pack_kernel,
        out_shape=jax.ShapeDtypeStruct((tiles * CAP * WORDS, 128), F32),
        in_specs=[smem(), smem(), vmem(), vmem(), vmem(), vmem()],
        out_specs=vmem(),
        scratch_shapes=[pltpu.VMEM((blocks * WORDS, 128), F32), pltpu.SMEM((tiles,), jnp.int32)],
        name="pack",
    )(owner, count, innovation, error, offset, cell)


def deposit(arrived, tile_rows, tile_cols):
    slots = arrived.shape[0] // WORDS
    row_pad = (tile_rows + 1 + 7) // 8 * 8
    m_one = (GROUPS * row_pad + 15) // 16 * 16
    width = tile_cols // GROUPS
    m_all = 4 * m_one
    steps = slots // CHUNK
    half_m = m_one // 2
    half_n = width // 2

    def kernel(src, out, left_a, left_b, right_a, right_b, acc):
        m_index = (lax.broadcasted_iota(jnp.int32, (m_one, 128), 0) - half_m).astype(F32).astype(BF16)
        n_index = (lax.broadcasted_iota(jnp.int32, (width, 128), 0) - half_n).astype(F32).astype(BF16)
        n_one = jnp.ones((width, 128), BF16)
        n_zero = jnp.zeros((width, 128), BF16)
        m_zero = jnp.zeros((m_one, 128), BF16)

        def spread(x, j, n):
            row = jnp.broadcast_to(x[j : j + 1, :], (16, 128)).astype(BF16)
            return jnp.broadcast_to(row[None], (n // 16, 16, 128)).reshape(n, 128)

        def build(chunk, left, right):
            base = chunk * (CHUNK * WORDS)
            amount = src[pl.ds(base, CHUNK, stride=WORDS), :]
            north = src[pl.ds(base + 1, CHUNK, stride=WORDS), :]
            east = src[pl.ds(base + 2, CHUNK, stride=WORDS), :]
            cell = src[pl.ds(base + 3, CHUNK, stride=WORDS), :].astype(jnp.int32)
            row = cell // tile_cols
            col = cell % tile_cols
            m_here = ((col // width) * row_pad + row - half_m).astype(F32)
            m_next = m_here + 1.0
            n_here = (col % width - half_n).astype(F32)
            pieces = []
            for value in (amount, amount * east):
                low = value * (1.0 - north)
                high = value * north
                low_top = low.astype(BF16).astype(F32)
                high_top = high.astype(BF16).astype(F32)
                pieces.append((low_top, high_top))
                pieces.append((low - low_top, high - high_top))
            for j in range(CHUNK):
                at_row = m_index == spread(m_here, j, m_one)
                at_next = m_index == spread(m_next, j, m_one)
                for k, (low, high) in enumerate(pieces):
                    left[k * m_one : (k + 1) * m_one, j * 128 : (j + 1) * 128] = jnp.where(
                        at_row,
                        spread(low, j, m_one),
                        jnp.where(at_next, spread(high, j, m_one), m_zero),
                    )
                right[:, j * 128 : (j + 1) * 128] = jnp.where(
                    n_index == spread(n_here, j, width), n_one, n_zero
                )

        def add(left, right):
            acc[...] += lax.dot_general(
                left[...], right[...], (((1,), (1,)), ((), ())), preferred_element_type=F32
            )

        acc[...] = jnp.zeros((m_all, width), F32)
        build(0, left_a, right_a)

        def turn(i, carry):
            build(2 * i + 1, left_b, right_b)
            add(left_a, right_a)
            build(jnp.minimum(2 * i + 2, steps - 1), left_a, right_a)
            add(left_b, right_b)
            return carry

        lax.fori_loop(0, steps // 2, turn, 0)
        lane = lax.broadcasted_iota(jnp.int32, (row_pad, width), 1)
        before = jnp.zeros((row_pad, 1), F32)
        for g in range(GROUPS):
            s = g * row_pad
            whole = acc[s : s + row_pad] + acc[m_one + s : m_one + s + row_pad]
            part = acc[2 * m_one + s : 2 * m_one + s + row_pad] + acc[3 * m_one + s : 3 * m_one + s + row_pad]
            moved = pltpu.roll(part, 1, 1)
            moved = jnp.where(lane == 0, jnp.broadcast_to(before, (row_pad, width)), moved)
            out[:, g * width : (g + 1) * width] = whole - part + moved
            before = part[:, width - 1 : width]
        edge = lax.broadcasted_iota(jnp.int32, (row_pad, 128), 1)
        out[:, tile_cols : tile_cols + 128] = jnp.where(
            edge == 0, jnp.broadcast_to(before, (row_pad, 128)), 0.0
        )

    return pl.pallas_call(
        kernel,
        out_shape=jax.ShapeDtypeStruct((row_pad, tile_cols + 128), F32),
        in_specs=[vmem()],
        out_specs=vmem(),
        scratch_shapes=[
            pltpu.VMEM((m_all, CHUNK * 128), BF16),
            pltpu.VMEM((m_all, CHUNK * 128), BF16),
            pltpu.VMEM((width, CHUNK * 128), BF16),
            pltpu.VMEM((width, CHUNK * 128), BF16),
            pltpu.VMEM((m_all, width), F32),
        ],
        name="deposit",
    )(arrived)


def two_sum(a, b):
    s = a + b
    t = s - a
    return s, (a - (s - t)) + (b - t)


def quick_sum(a, b):
    s = a + b
    return s, b - (s - a)


def halves(a):
    t = a * 4097.0
    top = t - (t - a)
    return top, a - top


def two_prod(a, b, a_halves, b_halves):
    p = a * b
    a1, a2 = a_halves
    b1, b2 = b_halves
    return p, ((a1 * b1 - p) + a1 * b2 + a2 * b1) + a2 * b2


def pair_add(a, b):
    s, e = two_sum(a[0], b[0])
    return quick_sum(s, e + (a[1] + b[1]))


def pair_mul(a, b):
    p, e = two_prod(a[0], b[0], halves(a[0]), halves(b[0]))
    return quick_sum(p, e + (a[0] * b[1] + a[1] * b[0]))


def pair_neg(a):
    return -a[0], -a[1]


def pair_div(a, b):
    q1 = a[0] / b[0]
    zero = jnp.zeros_like(q1)
    rest = pair_add(a, pair_neg(pair_mul((q1, zero), b)))
    q2 = rest[0] / b[0]
    rest = pair_add(rest, pair_neg(pair_mul((q2, zero), b)))
    q3 = rest[0] / b[0]
    s, e = quick_sum(q1, q2)
    return quick_sum(s, e + q3)


def roll_to(x, step, axis):
    return pltpu.roll(x, step % x.shape[axis], axis)


def apply_pair(v, inertia, east, south):
    h, l = v
    h_cut = halves(h)
    total, e = two_prod(inertia[0], h, inertia[1], h_cut)
    rest = e + inertia[0] * l
    for axis, (face, face_cut) in ((1, east), (0, south)):
        other = roll_to(h, -1, axis)
        d = h - other
        t = d - h
        err = (h - (d - t)) - (other + t)
        low = (l - roll_to(l, -1, axis)) + err
        p, e = two_prod(face, d, face_cut, halves(d))
        low = e + face * low
        total, e = two_sum(total, p)
        rest = rest + (e + low)
        total, e = two_sum(total, -roll_to(p, 1, axis))
        rest = rest + (e - roll_to(low, 1, axis))
    return quick_sum(total, rest)


def apply_plain(v, inertia, east, south):
    total = inertia * v
    for axis, face in ((1, east), (0, south)):
        flow = face * (v - roll_to(v, -1, axis))
        total = total + (flow - roll_to(flow, 1, axis))
    return total


def pair_fold(a):
    while a[0].shape[0] > 8:
        n = a[0].shape[0] // 2
        a = pair_add((a[0][:n], a[1][:n]), (a[0][n:], a[1][n:]))
    while a[0].shape[1] > 128:
        n = a[0].shape[1] // 2
        a = pair_add((a[0][:, :n], a[1][:, :n]), (a[0][:, n:], a[1][:, n:]))
    for step in (4, 2, 1):
        a = pair_add(a, (pltpu.roll(a[0], step, 0), pltpu.roll(a[1], step, 0)))
    return a


def basis_kernel(side, tile, other, ocean, inertia, east, south, forcing, sums):
    rows, cols = inertia.shape[0] - 16, inertia.shape[1] - 128
    first = side[0] == 0
    middle = tile[pl.ds(pl.multiple_of(side[0] * rows, 8), rows), :]
    corner = jnp.where(first, other[8:16, :], 0.0)
    top = jnp.where(first, other[0:8, :], tile[rows - 8 : rows, :])
    bottom = jnp.where(
        first, tile[rows : rows + 8, :], other[0:8, :] + tile[2 * rows : 2 * rows + 8, :]
    )
    start = jnp.concatenate([top, middle[0:8] + corner, middle[8:], bottom], axis=0) * ocean[...]
    forcing[...] = start
    weights = [(w[...], halves(w[...])) for w in (inertia, east, south)]
    vectors = [(start, jnp.zeros_like(start))]
    for k in range(ITERS):
        vectors.append(apply_pair(vectors[-1], *weights))
    inner = [(h[8 : 8 + rows, :cols], l[8 : 8 + rows, :cols]) for h, l in vectors]
    cuts = [halves(h) for h, l in inner]
    lane = lax.broadcasted_iota(jnp.int32, (8, 128), 1)
    tops, lows = [], []
    for k in range(MOMENTS):
        i, j = k // 2, (k + 1) // 2
        a, b = inner[i], inner[j]
        p, e = two_prod(a[0], b[0], cuts[i], cuts[j])
        total = pair_fold((p, e + (a[0] * b[1] + a[1] * b[0])))
        tops.append(total[0][0:1])
        lows.append(total[1][0:1])
    blank = [jnp.zeros((16 - MOMENTS, 128), F32)]
    pair = (jnp.concatenate(tops + blank, 0), jnp.concatenate(lows + blank, 0))
    for step in (64, 32, 16, 8, 4, 2, 1):
        pair = pair_add(pair, (pltpu.roll(pair[0], step, 1), pltpu.roll(pair[1], step, 1)))
    lane = lax.broadcasted_iota(jnp.int32, (16, 128), 1)
    slot = lax.broadcasted_iota(jnp.int32, (16, 128), 0)
    row = jnp.sum(
        jnp.where(lane == slot, pair[0], jnp.where(lane == slot + 64, pair[1], 0.0)),
        axis=0,
        keepdims=True,
    )
    sums[...] = jnp.broadcast_to(row, sums.shape)


def basis(side, tile, other, ocean, inertia, east, south, devices):
    return pl.pallas_call(
        basis_kernel,
        out_shape=(
            jax.ShapeDtypeStruct(inertia.shape, F32),
            jax.ShapeDtypeStruct((devices, 128), F32),
        ),
        in_specs=[smem()] + [vmem()] * 6,
        out_specs=(vmem(), vmem()),
        name="basis",
    )(side, tile, other, ocean, inertia, east, south)


def solve_kernel(sums, forcing, inertia, east, south, field, residual):
    rows, cols = field.shape
    s = sums[...]
    pair = (s, jnp.zeros_like(s))
    while pair[0].shape[0] > 8:
        n = pair[0].shape[0] // 2
        pair = pair_add((pair[0][:n], pair[1][:n]), (pair[0][n:], pair[1][n:]))
    for step in (4, 2, 1):
        pair = pair_add(pair, (pltpu.roll(pair[0], step, 0), pltpu.roll(pair[1], step, 0)))
    pair = quick_sum(pair[0], pair[1] + pltpu.roll(pair[0], 64, 1))

    def entry(k):
        return tuple(jnp.broadcast_to(x[0:1, k : k + 1], (8, 128)) for x in pair)

    right = [entry(k) for k in range(MOMENTS)]
    ahead = list(right)
    steps, ratios = [], []
    for k in range(ITERS):
        step = pair_div(right[k], ahead[k + 1])
        steps.append(step[0])
        if k + 1 < ITERS:
            last = MOMENTS - 1 - k
            new = list(right)
            for m in range(k + 1, last):
                new[m] = pair_add(right[m], pair_neg(pair_mul(step, ahead[m + 1])))
            ratio = pair_neg(pair_mul(step, pair_div(new[k + 1], right[k])))
            for m in range(k + 1, last):
                ahead[m] = pair_add(new[m], pair_mul(ratio, ahead[m]))
            right = new
            ratios.append(ratio[0])
    weights = (inertia[...], east[...], south[...])
    left = forcing[...]
    heading = left
    total = None
    for k in range(ITERS):
        step = steps[k][0:1, 0:1]
        total = step * heading if total is None else total + step * heading
        left = left - step * apply_plain(heading, *weights)
        if k + 1 < ITERS:
            heading = left + ratios[k][0:1, 0:1] * heading
    field[...] = total[8 : 8 + rows, :cols]
    residual[...] = left[8 : 8 + rows, :cols]


def solve(sums, forcing, inertia, east, south, rows, cols):
    shape = jax.ShapeDtypeStruct((rows, cols), F32)
    return pl.pallas_call(
        solve_kernel,
        out_shape=(shape, shape),
        in_specs=[vmem()] * 5,
        out_specs=(vmem(), vmem()),
        name="solve",
    )(sums, forcing, inertia, east, south)


def around(value, axis, steps):
    count = lax.axis_size(axis)
    return lax.ppermute(value, axis, [(i, (i + steps) % count) for i in range(count)])


def body(
    innovation,
    obs_error,
    obs_offset,
    obs_cell,
    obs_owner,
    block_count,
    land_mask,
    inertia,
    sea_depth,
):
    n_lat = lax.axis_size("lat")
    n_lon = lax.axis_size(LON)
    n_obs = lax.axis_size("obs")
    tiles = n_lat * n_lon
    rows, cols = land_mask.shape
    sent = pack(obs_owner, block_count, innovation, obs_error, obs_offset, obs_cell, tiles)
    arrived = lax.all_to_all(
        sent.reshape(tiles, CAP * WORDS, 1, 128), LAT_LON, split_axis=0, concat_axis=0, tiled=True
    ).reshape(tiles * CAP * WORDS, 128)

    conduct = land_mask.astype(F32) * sea_depth
    lane = lax.broadcasted_iota(jnp.int32, (1, 128), 1)
    stacked = jnp.stack([conduct, inertia])
    from_west = around(stacked[:, :, cols - 128 :], LON, 1)
    from_east = around(stacked[:, :, :128], LON, -1)
    wide = jnp.concatenate([stacked, jnp.where(lane < 64, from_east, from_west)], axis=2)
    above = around(wide[:, rows - 8 :], LAT_OBS, 1)
    below = around(wide[:, :8], LAT_OBS, -1)
    conduct, inertia = jnp.concatenate([above, wide, below], axis=1)
    ocean = (conduct > 0.0).astype(F32)
    east = jnp.sqrt(conduct * jnp.roll(conduct, -1, 1))
    south = jnp.sqrt(conduct * jnp.roll(conduct, -1, 0))

    part = deposit(arrived, rows * n_obs, cols)
    tile = part + around(part, "obs", 1)
    spill = tile[:, cols:]
    from_west = around(jnp.where(lane == 0, spill[:, :1], tile[:, cols - 128 : cols]), LON, 1)
    from_east = around(tile[:, :128], LON, -1)
    tile = jnp.concatenate(
        [
            tile[:, :128] + jnp.where(lane == 0, from_west, 0.0),
            tile[:, 128:cols],
            jnp.where(lane < 64, from_east, from_west) + spill,
        ],
        axis=1,
    )
    side = lax.axis_index("obs").astype(jnp.int32)
    outer = jnp.where(side == 0, tile[:16], tile[2 * rows - 8 : 2 * rows + 8])
    swap = []
    for i in range(n_lat):
        swap.append((2 * i + 1, (2 * i + 2) % (2 * n_lat)))
        swap.append((2 * i, (2 * i - 1) % (2 * n_lat)))
    other = lax.ppermute(outer, LAT_OBS, swap)
    forcing, sums = basis(
        side.reshape(1), tile, other, ocean, inertia, east, south, tiles * n_obs
    )
    sums = lax.all_to_all(
        sums.reshape(tiles * n_obs, 1, 128), LAT_LON_OBS, split_axis=0, concat_axis=0, tiled=True
    ).reshape(tiles * n_obs, 128)
    return solve(sums, forcing, inertia, east, south, rows, cols)


def solution(mesh):
    split = Mesh(
        mesh.devices.reshape(mesh.shape["lat"], 4, 4, mesh.shape["obs"]),
        ("lat", "lon_0", "lon_1", "obs"),
    )
    return jax.shard_map(
        body,
        mesh=split,
        in_specs=(
            P(LAT_LON_OBS, None),
            P(LAT_LON_OBS, None),
            P(None, LAT_LON_OBS, None),
            P(LAT_LON_OBS, None),
            P(LAT_LON_OBS, None),
            P(LAT_LON_OBS),
            P(LAT_OBS, LON),
            P(LAT_OBS, LON),
            P(LAT_OBS, LON),
        ),
        out_specs=(P(LAT_OBS, LON), P(LAT_OBS, LON)),
        check_vma=False,
    )
```

```python
import jax
import jax.numpy as jnp
from jax import lax
from jax.experimental import pallas as pl
from jax.experimental.pallas import tpu as pltpu
from jax.sharding import Mesh
from jax.sharding import PartitionSpec as P

ITERS = 5
MOMENTS = 2 * ITERS
CAP = 3
WORDS = 4
LON = ("lon_0", "lon_1")
LAT_OBS = ("lat", "obs")
LAT_LON_OBS = ("lat", "lon_0", "lon_1", "obs")
LAT_LON = ("lat", "lon_0", "lon_1")
F32 = jnp.float32
BF16 = jnp.bfloat16
GROUPS = 4
CHUNK = 16
EDGE = 16
EARLY = 2


def vmem():
    return pl.BlockSpec(memory_space=pltpu.VMEM)


def smem():
    return pl.BlockSpec(memory_space=pltpu.SMEM)


def pack_kernel(owner, count, innovation, error, offset, cell, early, late, rows, seen):
    blocks = innovation.shape[0]
    tiles = early.shape[0] // (EARLY * WORDS)
    err = error[...]
    rows[pl.ds(0, blocks, stride=WORDS), :] = innovation[...] / (err * err)
    rows[pl.ds(1, blocks, stride=WORDS), :] = offset[0]
    rows[pl.ds(2, blocks, stride=WORDS), :] = offset[1]
    rows[pl.ds(3, blocks, stride=WORDS), :] = cell[...].astype(F32)
    early[...] = jnp.zeros(early.shape, F32)
    late[...] = jnp.zeros(late.shape, F32)

    def clear(tile, carry):
        seen[tile] = 0
        return carry

    lax.fori_loop(0, tiles, clear, 0)

    def place(block, carry):
        tile = owner[0, block]
        rank = seen[tile]
        seen[tile] = rank + 1
        values = rows[pl.ds(block * WORDS, WORDS), :]

        @pl.when(rank < EARLY)
        def _():
            early[pl.ds((tile * EARLY + rank) * WORDS, WORDS), :] = values

        @pl.when(rank >= EARLY)
        def _():
            late[pl.ds((tile * (CAP - EARLY) + rank - EARLY) * WORDS, WORDS), :] = values

        return carry

    lax.fori_loop(0, count[0], place, 0)


def pack(owner, count, innovation, error, offset, cell, tiles):
    blocks = innovation.shape[0]
    return pl.pallas_call(
        pack_kernel,
        out_shape=(
            jax.ShapeDtypeStruct((tiles * EARLY * WORDS, 128), F32),
            jax.ShapeDtypeStruct((tiles * (CAP - EARLY) * WORDS, 128), F32),
        ),
        in_specs=[smem(), smem(), vmem(), vmem(), vmem(), vmem()],
        out_specs=(vmem(), vmem()),
        scratch_shapes=[pltpu.VMEM((blocks * WORDS, 128), F32), pltpu.SMEM((tiles,), jnp.int32)],
        name="pack",
    )(owner, count, innovation, error, offset, cell)


def rows_of(count):
    return (count + 1 + 7) // 8 * 8


def deposit_step(arrived, sofar, tile_rows, tile_cols, last):
    slots = arrived.shape[0] // WORDS
    width = tile_cols // GROUPS
    m_one = GROUPS * tile_rows
    m_all = 2 * (2 * m_one + EDGE)
    steps = slots // CHUNK
    half_m = m_one // 2
    half_n = width // 2
    low_at = 2 * m_one + EDGE
    row_pad = rows_of(tile_rows)

    def kernel(*refs):
        if sofar is None:
            src, out, left_a, left_b, right_a, right_b, acc = refs
        else:
            src, before_ref, out, left_a, left_b, right_a, right_b, acc = refs
        m_index = (lax.broadcasted_iota(jnp.int32, (m_one, 128), 0) - half_m).astype(F32).astype(BF16)
        n_index = (lax.broadcasted_iota(jnp.int32, (width, 128), 0) - half_n).astype(F32).astype(BF16)
        e_index = lax.broadcasted_iota(jnp.int32, (EDGE, 128), 0).astype(F32).astype(BF16)
        n_one = jnp.ones((width, 128), BF16)
        n_zero = jnp.zeros((width, 128), BF16)
        m_zero = jnp.zeros((m_one, 128), BF16)
        e_zero = jnp.zeros((EDGE, 128), BF16)

        def spread(x, j, n):
            row = jnp.broadcast_to(x[j : j + 1, :], (16, 128)).astype(BF16)
            return jnp.broadcast_to(row[None], (n // 16, 16, 128)).reshape(n, 128)

        def build(chunk, left, right):
            base = chunk * (CHUNK * WORDS)
            amount = src[pl.ds(base, CHUNK, stride=WORDS), :]
            north = src[pl.ds(base + 1, CHUNK, stride=WORDS), :]
            east = src[pl.ds(base + 2, CHUNK, stride=WORDS), :]
            cell = src[pl.ds(base + 3, CHUNK, stride=WORDS), :].astype(jnp.int32)
            row = cell // tile_cols
            col = cell % tile_cols
            group = col // width
            at_edge = row == tile_rows - 1
            m_here = (group * tile_rows + row - half_m).astype(F32)
            m_next = jnp.where(at_edge, 1.0e4, m_here + 1.0)
            n_here = (col % width - half_n).astype(F32)
            e_here = jnp.where(at_edge, group, 4 * EDGE).astype(F32)
            pieces = []
            for value in (amount, amount * east):
                low = value * (1.0 - north)
                high = value * north
                low_top = low.astype(BF16).astype(F32)
                high_top = high.astype(BF16).astype(F32)
                pieces.append(((low_top, high_top), (low - low_top, high - high_top)))
            for j in range(CHUNK):
                at_row = m_index == spread(m_here, j, m_one)
                at_next = m_index == spread(m_next, j, m_one)
                whole_edge = e_index == spread(e_here, j, EDGE)
                part_edge = e_index == spread(e_here + GROUPS, j, EDGE)
                for k in range(2):
                    start = k * low_at
                    for field in range(2):
                        low, high = pieces[field][k]
                        left[j, start + field * m_one : start + (field + 1) * m_one] = jnp.where(
                            at_row,
                            spread(low, j, m_one),
                            jnp.where(at_next, spread(high, j, m_one), m_zero),
                        )
                    left[j, start + 2 * m_one : start + low_at] = jnp.where(
                        whole_edge,
                        spread(pieces[0][k][1], j, EDGE),
                        jnp.where(part_edge, spread(pieces[1][k][1], j, EDGE), e_zero),
                    )
                right[j] = jnp.where(n_index == spread(n_here, j, width), n_one, n_zero)

        def joined(ref):
            return jnp.concatenate([ref[j] for j in range(CHUNK)], axis=1)

        def add(left, right):
            acc[...] += lax.dot_general(
                joined(left), joined(right), (((1,), (1,)), ((), ())), preferred_element_type=F32
            )

        if sofar is None:
            acc[...] = jnp.zeros((m_all, width), F32)
        else:
            acc[...] = before_ref[...]
        build(0, left_a, right_a)

        def turn(i, carry):
            build(2 * i + 1, left_b, right_b)
            add(left_a, right_a)
            build(jnp.minimum(2 * i + 2, steps - 1), left_a, right_a)
            add(left_b, right_b)
            return carry

        lax.fori_loop(0, steps // 2, turn, 0)
        if not last:
            out[...] = acc[...]
            return
        acc[0:low_at] = acc[0:low_at] + acc[low_at:m_all]
        lane = lax.broadcasted_iota(jnp.int32, (row_pad, width), 1)
        before = jnp.zeros((row_pad, 1), F32)
        blank = jnp.zeros((row_pad - tile_rows - 1, width), F32)

        def field_of(g, field):
            top = field * m_one + g * tile_rows
            edge = 2 * m_one + field * GROUPS + g
            return jnp.concatenate([acc[top : top + tile_rows], acc[edge : edge + 1], blank], 0)

        for g in range(GROUPS):
            whole = field_of(g, 0)
            part = field_of(g, 1)
            moved = pltpu.roll(part, 1, 1)
            moved = jnp.where(lane == 0, jnp.broadcast_to(before, (row_pad, width)), moved)
            out[:, g * width : (g + 1) * width] = whole - part + moved
            before = part[:, width - 1 : width]
        edge = lax.broadcasted_iota(jnp.int32, (row_pad, 128), 1)
        out[:, tile_cols : tile_cols + 128] = jnp.where(
            edge == 0, jnp.broadcast_to(before, (row_pad, 128)), 0.0
        )

    shape = (row_pad, tile_cols + 128) if last else (m_all, width)
    operands = (arrived,) if sofar is None else (arrived, sofar)
    return pl.pallas_call(
        kernel,
        out_shape=jax.ShapeDtypeStruct(shape, F32),
        in_specs=[vmem()] * len(operands),
        out_specs=vmem(),
        scratch_shapes=[
            pltpu.VMEM((CHUNK, m_all, 128), BF16),
            pltpu.VMEM((CHUNK, m_all, 128), BF16),
            pltpu.VMEM((CHUNK, width, 128), BF16),
            pltpu.VMEM((CHUNK, width, 128), BF16),
            pltpu.VMEM((m_all, width), F32),
        ],
        name="deposit_last" if last else "deposit_first",
    )(*operands)


def two_sum(a, b):
    s = a + b
    t = s - a
    return s, (a - (s - t)) + (b - t)


def quick_sum(a, b):
    s = a + b
    return s, b - (s - a)


def halves(a):
    t = a * 4097.0
    top = t - (t - a)
    return top, a - top


def two_prod(a, b, a_halves, b_halves):
    p = a * b
    a1, a2 = a_halves
    b1, b2 = b_halves
    return p, ((a1 * b1 - p) + a1 * b2 + a2 * b1) + a2 * b2


def pair_add(a, b):
    s, e = two_sum(a[0], b[0])
    return quick_sum(s, e + (a[1] + b[1]))


def pair_mul(a, b):
    p, e = two_prod(a[0], b[0], halves(a[0]), halves(b[0]))
    return quick_sum(p, e + (a[0] * b[1] + a[1] * b[0]))


def pair_neg(a):
    return -a[0], -a[1]


def pair_div(a, b):
    q1 = a[0] / b[0]
    zero = jnp.zeros_like(q1)
    rest = pair_add(a, pair_neg(pair_mul((q1, zero), b)))
    q2 = rest[0] / b[0]
    rest = pair_add(rest, pair_neg(pair_mul((q2, zero), b)))
    q3 = rest[0] / b[0]
    s, e = quick_sum(q1, q2)
    return quick_sum(s, e + q3)


def roll_to(x, step, axis):
    return pltpu.roll(x, step % x.shape[axis], axis)


def apply_pair(v, inertia, east, south):
    h, l = v
    h_cut = halves(h)
    total, e = two_prod(inertia[0], h, inertia[1], h_cut)
    rest = e + inertia[0] * l
    for axis, (face, face_cut) in ((1, east), (0, south)):
        other = roll_to(h, -1, axis)
        d = h - other
        t = d - h
        err = (h - (d - t)) - (other + t)
        low = (l - roll_to(l, -1, axis)) + err
        p, e = two_prod(face, d, face_cut, halves(d))
        low = e + face * low
        total, e = two_sum(total, p)
        rest = rest + (e + low)
        total, e = two_sum(total, -roll_to(p, 1, axis))
        rest = rest + (e - roll_to(low, 1, axis))
    return quick_sum(total, rest)


def apply_plain(v, inertia, east, south):
    total = inertia * v
    for axis, face in ((1, east), (0, south)):
        flow = face * (v - roll_to(v, -1, axis))
        total = total + (flow - roll_to(flow, 1, axis))
    return total


def pair_fold(a):
    while a[0].shape[0] > 8:
        n = a[0].shape[0] // 2
        a = pair_add((a[0][:n], a[1][:n]), (a[0][n:], a[1][n:]))
    while a[0].shape[1] > 128:
        n = a[0].shape[1] // 2
        a = pair_add((a[0][:, :n], a[1][:, :n]), (a[0][:, n:], a[1][:, n:]))
    for step in (4, 2, 1):
        a = pair_add(a, (pltpu.roll(a[0], step, 0), pltpu.roll(a[1], step, 0)))
    return a


def basis_kernel(side, tile, other, ocean, inertia, east, south, forcing, sums):
    rows, cols = inertia.shape[0] - 16, inertia.shape[1] - 128
    first = side[0] == 0
    middle = tile[pl.ds(pl.multiple_of(side[0] * rows, 8), rows), :]
    corner = jnp.where(first, other[8:16, :], 0.0)
    top = jnp.where(first, other[0:8, :], tile[rows - 8 : rows, :])
    bottom = jnp.where(
        first, tile[rows : rows + 8, :], other[0:8, :] + tile[2 * rows : 2 * rows + 8, :]
    )
    start = jnp.concatenate([top, middle[0:8] + corner, middle[8:], bottom], axis=0) * ocean[...]
    forcing[...] = start
    weights = [(w[...], halves(w[...])) for w in (inertia, east, south)]
    vectors = [(start, jnp.zeros_like(start))]
    for k in range(ITERS):
        vectors.append(apply_pair(vectors[-1], *weights))
    inner = [(h[8 : 8 + rows, :cols], l[8 : 8 + rows, :cols]) for h, l in vectors]
    cuts = [halves(h) for h, l in inner]
    lane = lax.broadcasted_iota(jnp.int32, (8, 128), 1)
    tops, lows = [], []
    for k in range(MOMENTS):
        i, j = k // 2, (k + 1) // 2
        a, b = inner[i], inner[j]
        p, e = two_prod(a[0], b[0], cuts[i], cuts[j])
        total = pair_fold((p, e + (a[0] * b[1] + a[1] * b[0])))
        tops.append(total[0][0:1])
        lows.append(total[1][0:1])
    blank = [jnp.zeros((16 - MOMENTS, 128), F32)]
    pair = (jnp.concatenate(tops + blank, 0), jnp.concatenate(lows + blank, 0))
    for step in (64, 32, 16, 8, 4, 2, 1):
        pair = pair_add(pair, (pltpu.roll(pair[0], step, 1), pltpu.roll(pair[1], step, 1)))
    lane = lax.broadcasted_iota(jnp.int32, (16, 128), 1)
    slot = lax.broadcasted_iota(jnp.int32, (16, 128), 0)
    row = jnp.sum(
        jnp.where(lane == slot, pair[0], jnp.where(lane == slot + 64, pair[1], 0.0)),
        axis=0,
        keepdims=True,
    )
    sums[...] = jnp.broadcast_to(row, sums.shape)


def basis(side, tile, other, ocean, inertia, east, south, devices):
    return pl.pallas_call(
        basis_kernel,
        out_shape=(
            jax.ShapeDtypeStruct(inertia.shape, F32),
            jax.ShapeDtypeStruct((devices, 128), F32),
        ),
        in_specs=[smem()] + [vmem()] * 6,
        out_specs=(vmem(), vmem()),
        name="basis",
    )(side, tile, other, ocean, inertia, east, south)


def solve_kernel(sums, forcing, inertia, east, south, field, residual):
    rows, cols = field.shape
    s = sums[...]
    pair = (s, jnp.zeros_like(s))
    while pair[0].shape[0] > 8:
        n = pair[0].shape[0] // 2
        pair = pair_add((pair[0][:n], pair[1][:n]), (pair[0][n:], pair[1][n:]))
    for step in (4, 2, 1):
        pair = pair_add(pair, (pltpu.roll(pair[0], step, 0), pltpu.roll(pair[1], step, 0)))
    pair = quick_sum(pair[0], pair[1] + pltpu.roll(pair[0], 64, 1))

    def entry(k):
        return tuple(jnp.broadcast_to(x[0:1, k : k + 1], (8, 128)) for x in pair)

    right = [entry(k) for k in range(MOMENTS)]
    ahead = list(right)
    steps, ratios = [], []
    for k in range(ITERS):
        step = pair_div(right[k], ahead[k + 1])
        steps.append(step[0])
        if k + 1 < ITERS:
            last = MOMENTS - 1 - k
            new = list(right)
            for m in range(k + 1, last):
                new[m] = pair_add(right[m], pair_neg(pair_mul(step, ahead[m + 1])))
            ratio = pair_neg(pair_mul(step, pair_div(new[k + 1], right[k])))
            for m in range(k + 1, last):
                ahead[m] = pair_add(new[m], pair_mul(ratio, ahead[m]))
            right = new
            ratios.append(ratio[0])
    weights = (inertia[...], east[...], south[...])
    left = forcing[...]
    heading = left
    total = None
    for k in range(ITERS):
        step = steps[k][0:1, 0:1]
        total = step * heading if total is None else total + step * heading
        left = left - step * apply_plain(heading, *weights)
        if k + 1 < ITERS:
            heading = left + ratios[k][0:1, 0:1] * heading
    field[...] = total[8 : 8 + rows, :cols]
    residual[...] = left[8 : 8 + rows, :cols]


def solve(sums, forcing, inertia, east, south, rows, cols):
    shape = jax.ShapeDtypeStruct((rows, cols), F32)
    return pl.pallas_call(
        solve_kernel,
        out_shape=(shape, shape),
        in_specs=[vmem()] * 5,
        out_specs=(vmem(), vmem()),
        name="solve",
    )(sums, forcing, inertia, east, south)


def around(value, axis, steps):
    count = lax.axis_size(axis)
    return lax.ppermute(value, axis, [(i, (i + steps) % count) for i in range(count)])


def body(
    innovation,
    obs_error,
    obs_offset,
    obs_cell,
    obs_owner,
    block_count,
    land_mask,
    inertia,
    sea_depth,
):
    n_lat = lax.axis_size("lat")
    n_lon = lax.axis_size(LON)
    n_obs = lax.axis_size("obs")
    tiles = n_lat * n_lon
    rows, cols = land_mask.shape
    sent = pack(obs_owner, block_count, innovation, obs_error, obs_offset, obs_cell, tiles)
    arrived = [
        lax.all_to_all(
            part.reshape(tiles, -1, 1, 128), LAT_LON, split_axis=0, concat_axis=0, tiled=True
        ).reshape(-1, 128)
        for part in sent
    ]

    conduct = land_mask.astype(F32) * sea_depth
    lane = lax.broadcasted_iota(jnp.int32, (1, 128), 1)
    stacked = jnp.stack([conduct, inertia])
    from_west = around(stacked[:, :, cols - 128 :], LON, 1)
    from_east = around(stacked[:, :, :128], LON, -1)
    wide = jnp.concatenate([stacked, jnp.where(lane < 64, from_east, from_west)], axis=2)
    above = around(wide[:, rows - 8 :], LAT_OBS, 1)
    below = around(wide[:, :8], LAT_OBS, -1)
    conduct, inertia = jnp.concatenate([above, wide, below], axis=1)
    ocean = (conduct > 0.0).astype(F32)
    east = jnp.sqrt(conduct * jnp.roll(conduct, -1, 1))
    south = jnp.sqrt(conduct * jnp.roll(conduct, -1, 0))

    part = deposit_step(arrived[0], None, rows * n_obs, cols, False)
    part = deposit_step(arrived[1], part, rows * n_obs, cols, True)
    tile = part + around(part, "obs", 1)
    spill = tile[:, cols:]
    from_west = around(jnp.where(lane == 0, spill[:, :1], tile[:, cols - 128 : cols]), LON, 1)
    from_east = around(tile[:, :128], LON, -1)
    tile = jnp.concatenate(
        [
            tile[:, :128] + jnp.where(lane == 0, from_west, 0.0),
            tile[:, 128:cols],
            jnp.where(lane < 64, from_east, from_west) + spill,
        ],
        axis=1,
    )
    side = lax.axis_index("obs").astype(jnp.int32)
    outer = jnp.where(side == 0, tile[:16], tile[2 * rows - 8 : 2 * rows + 8])
    swap = []
    for i in range(n_lat):
        swap.append((2 * i + 1, (2 * i + 2) % (2 * n_lat)))
        swap.append((2 * i, (2 * i - 1) % (2 * n_lat)))
    other = lax.ppermute(outer, LAT_OBS, swap)
    forcing, sums = basis(
        side.reshape(1), tile, other, ocean, inertia, east, south, tiles * n_obs
    )
    sums = lax.all_to_all(
        sums.reshape(tiles * n_obs, 1, 128), LAT_LON_OBS, split_axis=0, concat_axis=0, tiled=True
    ).reshape(tiles * n_obs, 128)
    return solve(sums, forcing, inertia, east, south, rows, cols)


def solution(mesh):
    split = Mesh(
        mesh.devices.reshape(mesh.shape["lat"], 4, 4, mesh.shape["obs"]),
        ("lat", "lon_0", "lon_1", "obs"),
    )
    return jax.shard_map(
        body,
        mesh=split,
        in_specs=(
            P(LAT_LON_OBS, None),
            P(LAT_LON_OBS, None),
            P(None, LAT_LON_OBS, None),
            P(LAT_LON_OBS, None),
            P(LAT_LON_OBS, None),
            P(LAT_LON_OBS),
            P(LAT_OBS, LON),
            P(LAT_OBS, LON),
            P(LAT_OBS, LON),
        ),
        out_specs=(P(LAT_OBS, LON), P(LAT_OBS, LON)),
        check_vma=False,
    )
```

```python
import jax
import jax.numpy as jnp
from jax import lax
from jax.experimental import pallas as pl
from jax.experimental.pallas import tpu as pltpu
from jax.sharding import Mesh
from jax.sharding import PartitionSpec as P

ITERS = 5
MOMENTS = 2 * ITERS
CAP = 3
WORDS = 4
LON = ("lon_0", "lon_1")
LAT_OBS = ("lat", "obs")
LAT_LON_OBS = ("lat", "lon_0", "lon_1", "obs")
LAT_LON = ("lat", "lon_0", "lon_1")
F32 = jnp.float32
BF16 = jnp.bfloat16
GROUPS = 4
WINDOW = 24
STEP = 16


def vmem():
    return pl.BlockSpec(memory_space=pltpu.VMEM)


def smem():
    return pl.BlockSpec(memory_space=pltpu.SMEM)


def pack_kernel(owner, count, innovation, error, offset, cell, out, rows, seen):
    blocks = innovation.shape[0]
    tiles = out.shape[0] // (CAP * WORDS)
    err = error[...]
    rows[pl.ds(0, blocks, stride=WORDS), :] = innovation[...] / (err * err)
    rows[pl.ds(1, blocks, stride=WORDS), :] = offset[0]
    rows[pl.ds(2, blocks, stride=WORDS), :] = offset[1]
    rows[pl.ds(3, blocks, stride=WORDS), :] = cell[...].astype(F32)
    out[...] = jnp.zeros(out.shape, F32)

    def clear(tile, carry):
        seen[tile] = 0
        return carry

    lax.fori_loop(0, tiles, clear, 0)

    def place(block, carry):
        tile = owner[0, block]
        rank = seen[tile]
        seen[tile] = rank + 1
        slot = tile * CAP + rank
        out[pl.ds(slot * WORDS, WORDS), :] = rows[pl.ds(block * WORDS, WORDS), :]
        return carry

    lax.fori_loop(0, count[0], place, 0)


def pack(owner, count, innovation, error, offset, cell, tiles):
    blocks = innovation.shape[0]
    return pl.pallas_call(
        pack_kernel,
        out_shape=jax.ShapeDtypeStruct((tiles * CAP * WORDS, 128), F32),
        in_specs=[smem(), smem(), vmem(), vmem(), vmem(), vmem()],
        out_specs=vmem(),
        scratch_shapes=[pltpu.VMEM((blocks * WORDS, 128), F32), pltpu.SMEM((tiles,), jnp.int32)],
        name="pack",
    )(owner, count, innovation, error, offset, cell)


SORT_8 = (
    (0, 1), (2, 3), (4, 5), (6, 7), (0, 2), (1, 3), (4, 6), (5, 7), (1, 2), (5, 6),
    (0, 4), (1, 5), (2, 6), (3, 7), (2, 4), (3, 5), (1, 2), (3, 4), (5, 6),
)
CLEAN_8 = (
    (0, 4), (1, 5), (2, 6), (3, 7), (0, 2), (1, 3), (4, 6), (5, 7), (0, 1), (2, 3), (4, 5), (6, 7),
)


def quotient(x, n):
    return x >> (n.bit_length() - 1) if n & (n - 1) == 0 else x // n


def remainder(x, n):
    return x & (n - 1) if n & (n - 1) == 0 else x % n


def deposit(arrived, tile_rows, tile_cols):
    slots = arrived.shape[0] // WORDS
    width = tile_cols // GROUPS
    m_one = GROUPS * WINDOW
    m_all = 4 * m_one
    depth = tile_rows + WINDOW - 8
    filled = -(-slots // 8)
    regs = 8
    while regs < filled:
        regs *= 2
    total = -(-slots // 8)
    row_pad = (tile_rows + 1 + 7) // 8 * 8
    index_rows = max(m_one, width)
    middle = index_rows // 2
    last_cell = float(tile_rows * tile_cols - 1)
    parts = regs // 8
    entries = total * (tile_rows // STEP + 1) + 8

    def kernel(src, out, held, left_a, left_b, right_a, right_b, acc, index, span_v, span_s, at, row_of, room, sem):
        index[...] = (lax.broadcasted_iota(jnp.int32, index.shape, 0) - middle).astype(F32).astype(BF16)
        acc[...] = jnp.zeros(acc.shape, F32)
        sub = lax.broadcasted_iota(jnp.int32, (8, 128), 0)

        def load(p):
            return [held[w, p] for w in range(WORDS)]

        def store(p, x):
            for w in range(WORDS):
                held[w, p] = x[w]

        def ordered(a, b):
            m = a[3] <= b[3]
            return (
                [jnp.where(m, x, y) for x, y in zip(a, b)],
                [jnp.where(m, y, x) for x, y in zip(a, b)],
            )

        def network(places, pairs):
            xs = [load(p) for p in places]
            for a, b in pairs:
                xs[a], xs[b] = ordered(xs[a], xs[b])
            for p, x in zip(places, xs):
                store(p, x)

        def first(g, carry):
            xs = []
            for i in range(8):
                base = pl.multiple_of((g * 8 + i) * 8 * WORDS, 8 * WORDS)
                xs.append([src[pl.ds(base + w, 8, stride=WORDS), :] for w in range(WORDS)])
            for a, b in SORT_8:
                xs[a], xs[b] = ordered(xs[a], xs[b])
            for i in range(8):
                store(g * 8 + i, xs[i])
            return carry

        lax.fori_loop(0, filled // 8, first, 0)
        for p in range(filled, regs):
            for w in range(WORDS):
                held[w, p] = jnp.full((8, 128), 1.0e9 if w == 3 else 0.0, F32)

        def near(g, carry):
            network([g * 8 + i for i in range(8)], CLEAN_8)
            return carry

        def several(pairs):
            for p, q in pairs:
                x, y = ordered(load(p), load(q))
                store(p, x)
                store(q, y)

        size = 16
        while size <= regs:
            h = size // 2
            several([(t // h * size + t % h, t // h * size + size - 1 - t % h) for t in range(regs // 2)])
            d = h // 2
            while d >= 8:
                several([(t // d * 2 * d + t % d, t // d * 2 * d + t % d + d) for t in range(regs // 2)])
                d //= 2
            lax.fori_loop(0, regs // 8, near, 0)
            size *= 2

        def turned(x, mask):
            return jnp.take_along_axis(x, sub ^ mask, axis=0, mode="promise_in_bounds")

        for k in range(3):
            mask = (2 << k) - 1
            low = (sub & (1 << k)) == 0
            for p in range(regs // 2):
                a = load(p)
                b = [turned(x, mask) for x in load(regs - 1 - p)]
                m = (a[3] <= b[3]) == low
                store(p, [jnp.where(m, x, y) for x, y in zip(a, b)])
                store(regs - 1 - p, [turned(jnp.where(m, y, x), mask) for x, y in zip(a, b)])
            for bit in range(k - 1, -1, -1):
                low_bit = (sub & (1 << bit)) == 0
                for p in range(regs):
                    a = load(p)
                    c = [turned(x, 1 << bit) for x in a]
                    m = jnp.where(low_bit, a[3], c[3]) <= jnp.where(low_bit, c[3], a[3])
                    store(p, [jnp.where(m, x, y) for x, y in zip(a, c)])
            d = regs // 2
            while d >= 8:
                if d == 32:

                    def far(g, carry):
                        network([g + 8 * i for i in range(8)], CLEAN_8)
                        return carry

                    lax.fori_loop(0, 8, far, 0)
                    d = 4
                else:
                    several([(t // d * 2 * d + t % d, t // d * 2 * d + t % d + d) for t in range(regs // 2)])
                    d //= 2
            lax.fori_loop(0, regs // 8, near, 0)

        lane = lax.broadcasted_iota(jnp.int32, (8, 128), 1)
        spans = jnp.zeros((8, 128), jnp.int32)
        for i in range(parts):
            low = jnp.min(jnp.minimum(held[3, 8 * i], last_cell), axis=1, keepdims=True)
            high = jnp.max(jnp.minimum(held[3, 8 * i + 7], last_cell), axis=1, keepdims=True)
            low = quotient(low.astype(jnp.int32), tile_cols)
            high = quotient(high.astype(jnp.int32), tile_cols)
            spans = jnp.where(lane == i, low, jnp.where(lane == 64 + i, high, spans))
        span_v[...] = spans
        copy = pltpu.make_async_copy(span_v, span_s, sem)
        copy.start()
        copy.wait()

        def plan(c, t):
            s = c // parts
            i = c % parts
            low = span_s[s, i]
            high = span_s[s, 64 + i]

            def note(t, row, rows):
                at[t] = c
                row_of[t] = row
                room[t] = rows

            def further(x):
                note(x[1], x[0], STEP)
                return x[0] + STEP, x[1] + 1

            row, t = lax.while_loop(lambda x: high - x[0] >= WINDOW - 1, further, (low // 8 * 8, t))
            note(t, row, WINDOW - 1)
            return t + 1

        count = lax.fori_loop(0, -(-slots // regs) * parts, plan, jnp.int32(0))
        for e in range(3):
            at[count + e] = 0
            row_of[count + e] = 0
            room[count + e] = 0

        def spread(x, j):
            pair = jnp.concatenate([x[2 * j : 2 * j + 1], x[2 * j + 1 : 2 * j + 2]], axis=1)
            return jnp.broadcast_to(pair, (16, 256)).astype(BF16)

        def build(t, left, right):
            c = at[t]
            s = c // parts
            i = c % parts
            amount, north, east, cell = [held[w, pl.ds(i * 8, 8), s, :] for w in range(WORDS)]
            cell = cell.astype(jnp.int32)
            row = quotient(cell, tile_cols) - row_of[t]
            col = remainder(cell, tile_cols)
            inside = (row >= 0) & (row < room[t])
            place = quotient(col, width) * WINDOW + row - middle
            m_here = jnp.where(inside, place, 8 * index_rows).astype(F32)
            m_next = m_here + 1.0
            n_here = (remainder(col, width) - middle).astype(F32)
            pieces = []
            for value in (amount, amount * east):
                low = value * (1.0 - north)
                high = value * north
                low_top = low.astype(BF16).astype(F32)
                high_top = high.astype(BF16).astype(F32)
                pieces += [(low_top, high_top), (low - low_top, high - high_top)]
            zero = jnp.zeros((16, 256), BF16)
            one = jnp.ones((16, 256), BF16)
            for j in range(4):
                here = spread(m_here, j)
                after = spread(m_next, j)
                column = spread(n_here, j)
                values = [(spread(x, j), spread(y, j)) for x, y in pieces]
                for q in range(m_one // 16):
                    own = index[q * 16 : (q + 1) * 16]
                    at_row = own == here
                    at_next = own == after
                    for f, (low, high) in enumerate(values):
                        left[j, f * m_one + q * 16 : f * m_one + (q + 1) * 16] = jnp.where(
                            at_row, low, jnp.where(at_next, high, zero)
                        )
                for q in range(width // 16):
                    right[j, q * 16 : (q + 1) * 16] = jnp.where(
                        index[q * 16 : (q + 1) * 16] == column, one, zero
                    )

        def joined(ref):
            return jnp.concatenate([ref[j] for j in range(4)], axis=1)

        def add(t, left, right):
            row = pl.multiple_of(row_of[t], 8)
            product = lax.dot_general(
                joined(left), joined(right), (((1,), (1,)), ((), ())), preferred_element_type=F32
            )
            for q in range(4 * GROUPS):
                acc[q, pl.ds(row, WINDOW), :] += product[q * WINDOW : (q + 1) * WINDOW]

        build(0, left_a, right_a)

        def turn(i, carry):
            build(2 * i + 1, left_b, right_b)
            add(2 * i, left_a, right_a)
            build(2 * i + 2, left_a, right_a)
            add(2 * i + 1, left_b, right_b)
            return carry

        lax.fori_loop(0, (count + 1) // 2, turn, 0)
        lane = lax.broadcasted_iota(jnp.int32, (row_pad, width), 1)
        before = jnp.zeros((row_pad, 1), F32)
        for g in range(GROUPS):
            whole = acc[g, 0:row_pad] + acc[GROUPS + g, 0:row_pad]
            part = acc[2 * GROUPS + g, 0:row_pad] + acc[3 * GROUPS + g, 0:row_pad]
            moved = pltpu.roll(part, 1, 1)
            moved = jnp.where(lane == 0, jnp.broadcast_to(before, (row_pad, width)), moved)
            out[:, g * width : (g + 1) * width] = whole - part + moved
            before = part[:, width - 1 : width]
        edge = lax.broadcasted_iota(jnp.int32, (row_pad, 128), 1)
        out[:, tile_cols : tile_cols + 128] = jnp.where(
            edge == 0, jnp.broadcast_to(before, (row_pad, 128)), 0.0
        )

    return pl.pallas_call(
        kernel,
        out_shape=jax.ShapeDtypeStruct((row_pad, tile_cols + 128), F32),
        in_specs=[vmem()],
        out_specs=vmem(),
        scratch_shapes=[
            pltpu.VMEM((WORDS, regs, 8, 128), F32),
            pltpu.VMEM((4, m_all, 256), BF16),
            pltpu.VMEM((4, m_all, 256), BF16),
            pltpu.VMEM((4, width, 256), BF16),
            pltpu.VMEM((4, width, 256), BF16),
            pltpu.VMEM((4 * GROUPS, depth, width), F32),
            pltpu.VMEM((index_rows, 256), BF16),
            pltpu.VMEM((8, 128), jnp.int32),
            pltpu.SMEM((8, 128), jnp.int32),
            pltpu.SMEM((entries,), jnp.int32),
            pltpu.SMEM((entries,), jnp.int32),
            pltpu.SMEM((entries,), jnp.int32),
            pltpu.SemaphoreType.DMA,
        ],
        name="deposit",
    )(arrived)


def two_sum(a, b):
    s = a + b
    t = s - a
    return s, (a - (s - t)) + (b - t)


def quick_sum(a, b):
    s = a + b
    return s, b - (s - a)


def halves(a):
    t = a * 4097.0
    top = t - (t - a)
    return top, a - top


def two_prod(a, b, a_halves, b_halves):
    p = a * b
    a1, a2 = a_halves
    b1, b2 = b_halves
    return p, ((a1 * b1 - p) + a1 * b2 + a2 * b1) + a2 * b2


def pair_add(a, b):
    s, e = two_sum(a[0], b[0])
    return quick_sum(s, e + (a[1] + b[1]))


def pair_mul(a, b):
    p, e = two_prod(a[0], b[0], halves(a[0]), halves(b[0]))
    return quick_sum(p, e + (a[0] * b[1] + a[1] * b[0]))


def pair_neg(a):
    return -a[0], -a[1]


def pair_div(a, b):
    q1 = a[0] / b[0]
    zero = jnp.zeros_like(q1)
    rest = pair_add(a, pair_neg(pair_mul((q1, zero), b)))
    q2 = rest[0] / b[0]
    rest = pair_add(rest, pair_neg(pair_mul((q2, zero), b)))
    q3 = rest[0] / b[0]
    s, e = quick_sum(q1, q2)
    return quick_sum(s, e + q3)


def roll_to(x, step, axis):
    return pltpu.roll(x, step % x.shape[axis], axis)


def apply_pair(v, inertia, east, south):
    h, l = v
    h_cut = halves(h)
    total, e = two_prod(inertia[0], h, inertia[1], h_cut)
    rest = e + inertia[0] * l
    for axis, (face, face_cut) in ((1, east), (0, south)):
        other = roll_to(h, -1, axis)
        d = h - other
        t = d - h
        err = (h - (d - t)) - (other + t)
        low = (l - roll_to(l, -1, axis)) + err
        p, e = two_prod(face, d, face_cut, halves(d))
        low = e + face * low
        total, e = two_sum(total, p)
        rest = rest + (e + low)
        total, e = two_sum(total, -roll_to(p, 1, axis))
        rest = rest + (e - roll_to(low, 1, axis))
    return quick_sum(total, rest)


def apply_plain(v, inertia, east, south):
    total = inertia * v
    for axis, face in ((1, east), (0, south)):
        flow = face * (v - roll_to(v, -1, axis))
        total = total + (flow - roll_to(flow, 1, axis))
    return total


def pair_fold(a):
    while a[0].shape[0] > 8:
        n = a[0].shape[0] // 2
        a = pair_add((a[0][:n], a[1][:n]), (a[0][n:], a[1][n:]))
    while a[0].shape[1] > 128:
        n = a[0].shape[1] // 2
        a = pair_add((a[0][:, :n], a[1][:, :n]), (a[0][:, n:], a[1][:, n:]))
    for step in (4, 2, 1):
        a = pair_add(a, (pltpu.roll(a[0], step, 0), pltpu.roll(a[1], step, 0)))
    return a


def basis_kernel(side, tile, other, ocean, inertia, east, south, forcing, sums, high, low, cut, tops, lows):
    rows, cols = inertia.shape[0] - 16, inertia.shape[1] - 128
    first = side[0] == 0
    middle = tile[pl.ds(pl.multiple_of(side[0] * rows, 8), rows), :]
    corner = jnp.where(first, other[8:16, :], 0.0)
    top = jnp.where(first, other[0:8, :], tile[rows - 8 : rows, :])
    bottom = jnp.where(
        first, tile[rows : rows + 8, :], other[0:8, :] + tile[2 * rows : 2 * rows + 8, :]
    )
    start = jnp.concatenate([top, middle[0:8] + corner, middle[8:], bottom], axis=0) * ocean[...]
    forcing[...] = start
    high[...] = start
    low[...] = jnp.zeros_like(start)
    fields = (inertia, east, south)
    for k, w in enumerate(fields):
        cut[2 * k], cut[2 * k + 1] = halves(w[...])
    tops[...] = jnp.zeros(tops.shape, F32)
    lows[...] = jnp.zeros(lows.shape, F32)

    def inner(v):
        return v[0][8 : 8 + rows, :cols], v[1][8 : 8 + rows, :cols]

    def product(a, b, a_cut, b_cut):
        p, e = two_prod(a[0], b[0], a_cut, b_cut)
        return pair_fold((p, e + (a[0] * b[1] + a[1] * b[0])))

    def turn(k, carry):
        old = (high[...], low[...])
        weights = [(w[...], (cut[2 * i], cut[2 * i + 1])) for i, w in enumerate(fields)]
        new = apply_pair(old, *weights)
        high[...], low[...] = new
        a, b = inner(old), inner(new)
        a_cut, b_cut = halves(a[0]), halves(b[0])
        for place, total in ((2 * k, product(a, a, a_cut, a_cut)), (2 * k + 1, product(a, b, a_cut, b_cut))):
            tops[pl.ds(place, 1), :] = total[0][0:1]
            lows[pl.ds(place, 1), :] = total[1][0:1]
        return carry

    lax.fori_loop(0, ITERS, turn, 0)
    pair = (tops[...], lows[...])
    for step in (64, 32, 16, 8, 4, 2, 1):
        pair = pair_add(pair, (pltpu.roll(pair[0], step, 1), pltpu.roll(pair[1], step, 1)))
    lane = lax.broadcasted_iota(jnp.int32, (16, 128), 1)
    slot = lax.broadcasted_iota(jnp.int32, (16, 128), 0)
    row = jnp.sum(
        jnp.where(lane == slot, pair[0], jnp.where(lane == slot + 64, pair[1], 0.0)),
        axis=0,
        keepdims=True,
    )
    sums[...] = jnp.broadcast_to(row, sums.shape)


def basis(side, tile, other, ocean, inertia, east, south, devices):
    return pl.pallas_call(
        basis_kernel,
        out_shape=(
            jax.ShapeDtypeStruct(inertia.shape, F32),
            jax.ShapeDtypeStruct((devices, 128), F32),
        ),
        in_specs=[smem()] + [vmem()] * 6,
        out_specs=(vmem(), vmem()),
        scratch_shapes=[
            pltpu.VMEM(inertia.shape, F32),
            pltpu.VMEM(inertia.shape, F32),
            pltpu.VMEM((6,) + inertia.shape, F32),
            pltpu.VMEM((16, 128), F32),
            pltpu.VMEM((16, 128), F32),
        ],
        name="basis",
    )(side, tile, other, ocean, inertia, east, south)


def solve_kernel(sums, forcing, inertia, east, south, field, residual, total, left, heading, coefs):
    rows, cols = field.shape
    s = sums[...]
    pair = (s, jnp.zeros_like(s))
    while pair[0].shape[0] > 8:
        n = pair[0].shape[0] // 2
        pair = pair_add((pair[0][:n], pair[1][:n]), (pair[0][n:], pair[1][n:]))
    for step in (4, 2, 1):
        pair = pair_add(pair, (pltpu.roll(pair[0], step, 0), pltpu.roll(pair[1], step, 0)))
    pair = quick_sum(pair[0], pair[1] + pltpu.roll(pair[0], 64, 1))

    def entry(k):
        return tuple(jnp.broadcast_to(x[0:1, k : k + 1], (8, 128)) for x in pair)

    right = [entry(k) for k in range(MOMENTS)]
    ahead = list(right)
    steps, ratios = [], []
    for k in range(ITERS):
        step = pair_div(right[k], ahead[k + 1])
        steps.append(step[0])
        if k + 1 < ITERS:
            last = MOMENTS - 1 - k
            new = list(right)
            for m in range(k + 1, last):
                new[m] = pair_add(right[m], pair_neg(pair_mul(step, ahead[m + 1])))
            ratio = pair_neg(pair_mul(step, pair_div(new[k + 1], right[k])))
            for m in range(k + 1, last):
                ahead[m] = pair_add(new[m], pair_mul(ratio, ahead[m]))
            right = new
            ratios.append(ratio[0])
    for k in range(ITERS):
        coefs[k : k + 1, :] = steps[k][0:1]
        coefs[8 + k : 9 + k, :] = ratios[k][0:1] if k + 1 < ITERS else jnp.zeros((1, 128), F32)
    left[...] = forcing[...]
    heading[...] = forcing[...]
    total[...] = jnp.zeros(total.shape, F32)

    def turn(k, carry):
        step = coefs[pl.ds(k, 1), 0:1]
        ratio = coefs[pl.ds(8 + k, 1), 0:1]
        p = heading[...]
        total[...] += step * p
        r = left[...] - step * apply_plain(p, inertia[...], east[...], south[...])
        left[...] = r
        heading[...] = r + ratio * p
        return carry

    lax.fori_loop(0, ITERS, turn, 0)
    field[...] = total[8 : 8 + rows, :cols]
    residual[...] = left[8 : 8 + rows, :cols]


def solve(sums, forcing, inertia, east, south, rows, cols):
    shape = jax.ShapeDtypeStruct((rows, cols), F32)
    return pl.pallas_call(
        solve_kernel,
        out_shape=(shape, shape),
        in_specs=[vmem()] * 5,
        out_specs=(vmem(), vmem()),
        scratch_shapes=[pltpu.VMEM(inertia.shape, F32)] * 3 + [pltpu.VMEM((16, 128), F32)],
        name="solve",
    )(sums, forcing, inertia, east, south)


def around(value, axis, steps):
    count = lax.axis_size(axis)
    return lax.ppermute(value, axis, [(i, (i + steps) % count) for i in range(count)])


def body(
    innovation,
    obs_error,
    obs_offset,
    obs_cell,
    obs_owner,
    block_count,
    land_mask,
    inertia,
    sea_depth,
):
    n_lat = lax.axis_size("lat")
    n_lon = lax.axis_size(LON)
    n_obs = lax.axis_size("obs")
    tiles = n_lat * n_lon
    rows, cols = land_mask.shape
    sent = pack(obs_owner, block_count, innovation, obs_error, obs_offset, obs_cell, tiles)
    arrived = lax.all_to_all(
        sent.reshape(tiles, CAP * WORDS, 1, 128), LAT_LON, split_axis=0, concat_axis=0, tiled=True
    ).reshape(tiles * CAP * WORDS, 128)

    conduct = land_mask.astype(F32) * sea_depth
    lane = lax.broadcasted_iota(jnp.int32, (1, 128), 1)
    stacked = jnp.stack([conduct, inertia])
    from_west = around(stacked[:, :, cols - 128 :], LON, 1)
    from_east = around(stacked[:, :, :128], LON, -1)
    wide = jnp.concatenate([stacked, jnp.where(lane < 64, from_east, from_west)], axis=2)
    above = around(wide[:, rows - 8 :], LAT_OBS, 1)
    below = around(wide[:, :8], LAT_OBS, -1)
    conduct, inertia = jnp.concatenate([above, wide, below], axis=1)
    ocean = (conduct > 0.0).astype(F32)
    east = jnp.sqrt(conduct * jnp.roll(conduct, -1, 1))
    south = jnp.sqrt(conduct * jnp.roll(conduct, -1, 0))

    part = deposit(arrived, rows * n_obs, cols)
    tile = part + around(part, "obs", 1)
    spill = tile[:, cols:]
    from_west = around(jnp.where(lane == 0, spill[:, :1], tile[:, cols - 128 : cols]), LON, 1)
    from_east = around(tile[:, :128], LON, -1)
    tile = jnp.concatenate(
        [
            tile[:, :128] + jnp.where(lane == 0, from_west, 0.0),
            tile[:, 128:cols],
            jnp.where(lane < 64, from_east, from_west) + spill,
        ],
        axis=1,
    )
    side = lax.axis_index("obs").astype(jnp.int32)
    outer = jnp.where(side == 0, tile[:16], tile[2 * rows - 8 : 2 * rows + 8])
    swap = []
    for i in range(n_lat):
        swap.append((2 * i + 1, (2 * i + 2) % (2 * n_lat)))
        swap.append((2 * i, (2 * i - 1) % (2 * n_lat)))
    other = lax.ppermute(outer, LAT_OBS, swap)
    forcing, sums = basis(
        side.reshape(1), tile, other, ocean, inertia, east, south, tiles * n_obs
    )
    sums = lax.all_to_all(
        sums.reshape(tiles * n_obs, 1, 128), LAT_LON_OBS, split_axis=0, concat_axis=0, tiled=True
    ).reshape(tiles * n_obs, 128)
    return solve(sums, forcing, inertia, east, south, rows, cols)


def solution(mesh):
    split = Mesh(
        mesh.devices.reshape(mesh.shape["lat"], 4, 4, mesh.shape["obs"]),
        ("lat", "lon_0", "lon_1", "obs"),
    )
    return jax.shard_map(
        body,
        mesh=split,
        in_specs=(
            P(LAT_LON_OBS, None),
            P(LAT_LON_OBS, None),
            P(None, LAT_LON_OBS, None),
            P(LAT_LON_OBS, None),
            P(LAT_LON_OBS, None),
            P(LAT_LON_OBS),
            P(LAT_OBS, LON),
            P(LAT_OBS, LON),
            P(LAT_OBS, LON),
        ),
        out_specs=(P(LAT_OBS, LON), P(LAT_OBS, LON)),
        check_vma=False,
    )
```

```python
import jax
import jax.numpy as jnp
from jax import lax
from jax.experimental import pallas as pl
from jax.experimental.pallas import tpu as pltpu
from jax.sharding import Mesh
from jax.sharding import PartitionSpec as P

ITERS = 5
MOMENTS = 2 * ITERS
CAP = 3
WORDS = 4
LON = ("lon_0", "lon_1")
LAT_OBS = ("lat", "obs")
LAT_LON_OBS = ("lat", "lon_0", "lon_1", "obs")
LAT_LON = ("lat", "lon_0", "lon_1")
F32 = jnp.float32
BF16 = jnp.bfloat16
GROUPS = 4
WINDOW = 24
STEP = 16


def vmem():
    return pl.BlockSpec(memory_space=pltpu.VMEM)


def smem():
    return pl.BlockSpec(memory_space=pltpu.SMEM)


def on_chip(*values):
    return [pltpu.with_memory_space_constraint(v, pltpu.MemorySpace.VMEM) for v in values]


def limit(mib):
    return pltpu.CompilerParams(vmem_limit_bytes=mib * 2**20)


def pack_kernel(owner, count, innovation, error, offset, cell, out, rows, seen):
    blocks = innovation.shape[0]
    tiles = out.shape[0] // (CAP * WORDS)
    err = error[...]
    rows[pl.ds(0, blocks, stride=WORDS), :] = innovation[...] / (err * err)
    rows[pl.ds(1, blocks, stride=WORDS), :] = offset[0]
    rows[pl.ds(2, blocks, stride=WORDS), :] = offset[1]
    rows[pl.ds(3, blocks, stride=WORDS), :] = cell[...].astype(F32)
    out[...] = jnp.zeros(out.shape, F32)

    def clear(tile, carry):
        seen[tile] = 0
        return carry

    lax.fori_loop(0, tiles, clear, 0)

    def place(block, carry):
        tile = owner[0, block]
        rank = seen[tile]
        seen[tile] = rank + 1
        slot = tile * CAP + rank
        out[pl.ds(slot * WORDS, WORDS), :] = rows[pl.ds(block * WORDS, WORDS), :]
        return carry

    lax.fori_loop(0, count[0], place, 0)


def pack(owner, count, innovation, error, offset, cell, tiles):
    blocks = innovation.shape[0]
    return pl.pallas_call(
        pack_kernel,
        out_shape=jax.ShapeDtypeStruct((tiles * CAP * WORDS, 128), F32),
        in_specs=[smem(), smem(), vmem(), vmem(), vmem(), vmem()],
        out_specs=vmem(),
        scratch_shapes=[pltpu.VMEM((blocks * WORDS, 128), F32), pltpu.SMEM((tiles,), jnp.int32)],
        name="pack",
    )(owner, count, innovation, error, offset, cell)


SORT_8 = (
    (0, 1), (2, 3), (4, 5), (6, 7), (0, 2), (1, 3), (4, 6), (5, 7), (1, 2), (5, 6),
    (0, 4), (1, 5), (2, 6), (3, 7), (2, 4), (3, 5), (1, 2), (3, 4), (5, 6),
)
CLEAN_8 = (
    (0, 4), (1, 5), (2, 6), (3, 7), (0, 2), (1, 3), (4, 6), (5, 7), (0, 1), (2, 3), (4, 5), (6, 7),
)


def quotient(x, n):
    return x >> (n.bit_length() - 1) if n & (n - 1) == 0 else x // n


def remainder(x, n):
    return x & (n - 1) if n & (n - 1) == 0 else x % n


def deposit(arrived, tile_rows, tile_cols):
    slots = arrived.shape[0] // WORDS
    width = tile_cols // GROUPS
    m_one = GROUPS * WINDOW
    m_all = 4 * m_one
    depth = tile_rows + WINDOW - 8
    filled = -(-slots // 8)
    regs = 8
    while regs < filled:
        regs *= 2
    total = -(-slots // 8)
    row_pad = (tile_rows + 1 + 7) // 8 * 8
    index_rows = max(m_one, width)
    middle = index_rows // 2
    last_cell = float(tile_rows * tile_cols - 1)
    parts = regs // 8
    entries = total * (tile_rows // STEP + 1) + 8

    def kernel(src, out, held, left_a, left_b, right_a, right_b, acc, index, span_v, span_s, at, row_of, room, sem):
        index[...] = (lax.broadcasted_iota(jnp.int32, index.shape, 0) - middle).astype(F32).astype(BF16)
        acc[...] = jnp.zeros(acc.shape, F32)
        sub = lax.broadcasted_iota(jnp.int32, (8, 128), 0)

        def load(p):
            return [held[w, p] for w in range(WORDS)]

        def store(p, x):
            for w in range(WORDS):
                held[w, p] = x[w]

        def ordered(a, b):
            m = a[3] <= b[3]
            return (
                [jnp.where(m, x, y) for x, y in zip(a, b)],
                [jnp.where(m, y, x) for x, y in zip(a, b)],
            )

        def network(places, pairs):
            xs = [load(p) for p in places]
            for a, b in pairs:
                xs[a], xs[b] = ordered(xs[a], xs[b])
            for p, x in zip(places, xs):
                store(p, x)

        def first(g, carry):
            xs = []
            for i in range(8):
                base = pl.multiple_of((g * 8 + i) * 8 * WORDS, 8 * WORDS)
                xs.append([src[pl.ds(base + w, 8, stride=WORDS), :] for w in range(WORDS)])
            for a, b in SORT_8:
                xs[a], xs[b] = ordered(xs[a], xs[b])
            for i in range(8):
                store(g * 8 + i, xs[i])
            return carry

        lax.fori_loop(0, filled // 8, first, 0)
        for p in range(filled, regs):
            for w in range(WORDS):
                held[w, p] = jnp.full((8, 128), 1.0e9 if w == 3 else 0.0, F32)

        def near(g, carry):
            network([g * 8 + i for i in range(8)], CLEAN_8)
            return carry

        def several(pairs):
            for p, q in pairs:
                x, y = ordered(load(p), load(q))
                store(p, x)
                store(q, y)

        size = 16
        while size <= regs:
            h = size // 2
            several([(t // h * size + t % h, t // h * size + size - 1 - t % h) for t in range(regs // 2)])
            d = h // 2
            while d >= 8:
                several([(t // d * 2 * d + t % d, t // d * 2 * d + t % d + d) for t in range(regs // 2)])
                d //= 2
            lax.fori_loop(0, regs // 8, near, 0)
            size *= 2

        def turned(x, mask):
            return jnp.take_along_axis(x, sub ^ mask, axis=0, mode="promise_in_bounds")

        for k in range(3):
            mask = (2 << k) - 1
            low = (sub & (1 << k)) == 0
            for p in range(regs // 2):
                a = load(p)
                b = [turned(x, mask) for x in load(regs - 1 - p)]
                m = (a[3] <= b[3]) == low
                store(p, [jnp.where(m, x, y) for x, y in zip(a, b)])
                store(regs - 1 - p, [turned(jnp.where(m, y, x), mask) for x, y in zip(a, b)])
            for bit in range(k - 1, -1, -1):
                low_bit = (sub & (1 << bit)) == 0
                for p in range(regs):
                    a = load(p)
                    c = [turned(x, 1 << bit) for x in a]
                    m = jnp.where(low_bit, a[3], c[3]) <= jnp.where(low_bit, c[3], a[3])
                    store(p, [jnp.where(m, x, y) for x, y in zip(a, c)])
            d = regs // 2
            while d >= 8:
                if d == 32:

                    def far(g, carry):
                        network([g + 8 * i for i in range(8)], CLEAN_8)
                        return carry

                    lax.fori_loop(0, 8, far, 0)
                    d = 4
                else:
                    several([(t // d * 2 * d + t % d, t // d * 2 * d + t % d + d) for t in range(regs // 2)])
                    d //= 2
            lax.fori_loop(0, regs // 8, near, 0)

        lane = lax.broadcasted_iota(jnp.int32, (8, 128), 1)
        spans = jnp.zeros((8, 128), jnp.int32)
        for i in range(parts):
            low = jnp.min(jnp.minimum(held[3, 8 * i], last_cell), axis=1, keepdims=True)
            high = jnp.max(jnp.minimum(held[3, 8 * i + 7], last_cell), axis=1, keepdims=True)
            low = quotient(low.astype(jnp.int32), tile_cols)
            high = quotient(high.astype(jnp.int32), tile_cols)
            spans = jnp.where(lane == i, low, jnp.where(lane == 64 + i, high, spans))
        span_v[...] = spans
        copy = pltpu.make_async_copy(span_v, span_s, sem)
        copy.start()
        copy.wait()

        def plan(c, t):
            s = c // parts
            i = c % parts
            low = span_s[s, i]
            high = span_s[s, 64 + i]

            def note(t, row, rows):
                at[t] = c
                row_of[t] = row
                room[t] = rows

            def further(x):
                note(x[1], x[0], STEP)
                return x[0] + STEP, x[1] + 1

            row, t = lax.while_loop(lambda x: high - x[0] >= WINDOW - 1, further, (low // 8 * 8, t))
            note(t, row, WINDOW - 1)
            return t + 1

        count = lax.fori_loop(0, -(-slots // regs) * parts, plan, jnp.int32(0))
        for e in range(3):
            at[count + e] = 0
            row_of[count + e] = 0
            room[count + e] = 0

        def spread(x, j):
            pair = jnp.concatenate([x[2 * j : 2 * j + 1], x[2 * j + 1 : 2 * j + 2]], axis=1)
            return jnp.broadcast_to(pair, (16, 256)).astype(BF16)

        def build(t, left, right):
            c = at[t]
            s = c // parts
            i = c % parts
            amount, north, east, cell = [held[w, pl.ds(i * 8, 8), s, :] for w in range(WORDS)]
            cell = cell.astype(jnp.int32)
            row = quotient(cell, tile_cols) - row_of[t]
            col = remainder(cell, tile_cols)
            inside = (row >= 0) & (row < room[t])
            place = quotient(col, width) * WINDOW + row - middle
            m_here = jnp.where(inside, place, 8 * index_rows).astype(F32)
            m_next = m_here + 1.0
            n_here = (remainder(col, width) - middle).astype(F32)
            pieces = []
            for value in (amount, amount * east):
                low = value * (1.0 - north)
                high = value * north
                low_top = low.astype(BF16).astype(F32)
                high_top = high.astype(BF16).astype(F32)
                pieces += [(low_top, high_top), (low - low_top, high - high_top)]
            zero = jnp.zeros((16, 256), BF16)
            one = jnp.ones((16, 256), BF16)
            for j in range(4):
                here = spread(m_here, j)
                after = spread(m_next, j)
                column = spread(n_here, j)
                values = [(spread(x, j), spread(y, j)) for x, y in pieces]
                for q in range(m_one // 16):
                    own = index[q * 16 : (q + 1) * 16]
                    at_row = own == here
                    at_next = own == after
                    for f, (low, high) in enumerate(values):
                        left[j, f * m_one + q * 16 : f * m_one + (q + 1) * 16] = jnp.where(
                            at_row, low, jnp.where(at_next, high, zero)
                        )
                for q in range(width // 16):
                    right[j, q * 16 : (q + 1) * 16] = jnp.where(
                        index[q * 16 : (q + 1) * 16] == column, one, zero
                    )

        def joined(ref):
            return jnp.concatenate([ref[j] for j in range(4)], axis=1)

        def add(t, left, right):
            row = pl.multiple_of(row_of[t], 8)
            product = lax.dot_general(
                joined(left), joined(right), (((1,), (1,)), ((), ())), preferred_element_type=F32
            )
            for q in range(4 * GROUPS):
                acc[q, pl.ds(row, WINDOW), :] += product[q * WINDOW : (q + 1) * WINDOW]

        build(0, left_a, right_a)

        def turn(i, carry):
            build(2 * i + 1, left_b, right_b)
            add(2 * i, left_a, right_a)
            build(2 * i + 2, left_a, right_a)
            add(2 * i + 1, left_b, right_b)
            return carry

        lax.fori_loop(0, (count + 1) // 2, turn, 0)
        lane = lax.broadcasted_iota(jnp.int32, (row_pad, width), 1)
        before = jnp.zeros((row_pad, 1), F32)
        for g in range(GROUPS):
            whole = acc[g, 0:row_pad] + acc[GROUPS + g, 0:row_pad]
            part = acc[2 * GROUPS + g, 0:row_pad] + acc[3 * GROUPS + g, 0:row_pad]
            moved = pltpu.roll(part, 1, 1)
            moved = jnp.where(lane == 0, jnp.broadcast_to(before, (row_pad, width)), moved)
            out[:, g * width : (g + 1) * width] = whole - part + moved
            before = part[:, width - 1 : width]
        edge = lax.broadcasted_iota(jnp.int32, (row_pad, 128), 1)
        out[:, tile_cols : tile_cols + 128] = jnp.where(
            edge == 0, jnp.broadcast_to(before, (row_pad, 128)), 0.0
        )

    return pl.pallas_call(
        kernel,
        out_shape=pltpu.VMEM((row_pad, tile_cols + 128), F32),
        compiler_params=limit(24),
        in_specs=[vmem()],
        out_specs=vmem(),
        scratch_shapes=[
            pltpu.VMEM((WORDS, regs, 8, 128), F32),
            pltpu.VMEM((4, m_all, 256), BF16),
            pltpu.VMEM((4, m_all, 256), BF16),
            pltpu.VMEM((4, width, 256), BF16),
            pltpu.VMEM((4, width, 256), BF16),
            pltpu.VMEM((4 * GROUPS, depth, width), F32),
            pltpu.VMEM((index_rows, 256), BF16),
            pltpu.VMEM((8, 128), jnp.int32),
            pltpu.SMEM((8, 128), jnp.int32),
            pltpu.SMEM((entries,), jnp.int32),
            pltpu.SMEM((entries,), jnp.int32),
            pltpu.SMEM((entries,), jnp.int32),
            pltpu.SemaphoreType.DMA,
        ],
        name="deposit",
    )(*on_chip(arrived))


def two_sum(a, b):
    s = a + b
    t = s - a
    return s, (a - (s - t)) + (b - t)


def quick_sum(a, b):
    s = a + b
    return s, b - (s - a)


def halves(a):
    t = a * 4097.0
    top = t - (t - a)
    return top, a - top


def two_prod(a, b, a_halves, b_halves):
    p = a * b
    a1, a2 = a_halves
    b1, b2 = b_halves
    return p, ((a1 * b1 - p) + a1 * b2 + a2 * b1) + a2 * b2


def pair_add(a, b):
    s, e = two_sum(a[0], b[0])
    return quick_sum(s, e + (a[1] + b[1]))


def pair_mul(a, b):
    p, e = two_prod(a[0], b[0], halves(a[0]), halves(b[0]))
    return quick_sum(p, e + (a[0] * b[1] + a[1] * b[0]))


def pair_neg(a):
    return -a[0], -a[1]


def pair_div(a, b):
    q1 = a[0] / b[0]
    zero = jnp.zeros_like(q1)
    rest = pair_add(a, pair_neg(pair_mul((q1, zero), b)))
    q2 = rest[0] / b[0]
    rest = pair_add(rest, pair_neg(pair_mul((q2, zero), b)))
    q3 = rest[0] / b[0]
    s, e = quick_sum(q1, q2)
    return quick_sum(s, e + q3)


def roll_to(x, step, axis):
    return pltpu.roll(x, step % x.shape[axis], axis)


def apply_pair(v, inertia, east, south):
    h, l = v
    h_cut = halves(h)
    total, e = two_prod(inertia[0], h, inertia[1], h_cut)
    rest = e + inertia[0] * l
    for axis, (face, face_cut) in ((1, east), (0, south)):
        other = roll_to(h, -1, axis)
        d = h - other
        t = d - h
        err = (h - (d - t)) - (other + t)
        low = (l - roll_to(l, -1, axis)) + err
        p, e = two_prod(face, d, face_cut, halves(d))
        low = e + face * low
        total, e = two_sum(total, p)
        rest = rest + (e + low)
        total, e = two_sum(total, -roll_to(p, 1, axis))
        rest = rest + (e - roll_to(low, 1, axis))
    return quick_sum(total, rest)


def apply_plain(v, inertia, east, south):
    total = inertia * v
    for axis, face in ((1, east), (0, south)):
        flow = face * (v - roll_to(v, -1, axis))
        total = total + (flow - roll_to(flow, 1, axis))
    return total


def pair_fold(a):
    while a[0].shape[0] > 8:
        n = a[0].shape[0] // 2
        a = pair_add((a[0][:n], a[1][:n]), (a[0][n:], a[1][n:]))
    while a[0].shape[1] > 128:
        n = a[0].shape[1] // 2
        a = pair_add((a[0][:, :n], a[1][:, :n]), (a[0][:, n:], a[1][:, n:]))
    for step in (4, 2, 1):
        a = pair_add(a, (pltpu.roll(a[0], step, 0), pltpu.roll(a[1], step, 0)))
    return a


def basis_kernel(side, tile, other, ocean, inertia, east, south, forcing, sums):
    rows, cols = inertia.shape[0] - 16, inertia.shape[1] - 128
    first = side[0] == 0
    middle = tile[pl.ds(pl.multiple_of(side[0] * rows, 8), rows), :]
    corner = jnp.where(first, other[8:16, :], 0.0)
    top = jnp.where(first, other[0:8, :], tile[rows - 8 : rows, :])
    bottom = jnp.where(
        first, tile[rows : rows + 8, :], other[0:8, :] + tile[2 * rows : 2 * rows + 8, :]
    )
    start = jnp.concatenate([top, middle[0:8] + corner, middle[8:], bottom], axis=0) * ocean[...]
    forcing[...] = start
    weights = [(w[...], halves(w[...])) for w in (inertia, east, south)]
    vectors = [(start, jnp.zeros_like(start))]
    for k in range(ITERS):
        vectors.append(apply_pair(vectors[-1], *weights))
    inner = [(h[8 : 8 + rows, :cols], l[8 : 8 + rows, :cols]) for h, l in vectors]
    cuts = [halves(h) for h, l in inner]
    lane = lax.broadcasted_iota(jnp.int32, (8, 128), 1)
    tops, lows = [], []
    for k in range(MOMENTS):
        i, j = k // 2, (k + 1) // 2
        a, b = inner[i], inner[j]
        p, e = two_prod(a[0], b[0], cuts[i], cuts[j])
        total = pair_fold((p, e + (a[0] * b[1] + a[1] * b[0])))
        tops.append(total[0][0:1])
        lows.append(total[1][0:1])
    blank = [jnp.zeros((16 - MOMENTS, 128), F32)]
    pair = (jnp.concatenate(tops + blank, 0), jnp.concatenate(lows + blank, 0))
    for step in (64, 32, 16, 8, 4, 2, 1):
        pair = pair_add(pair, (pltpu.roll(pair[0], step, 1), pltpu.roll(pair[1], step, 1)))
    lane = lax.broadcasted_iota(jnp.int32, (16, 128), 1)
    slot = lax.broadcasted_iota(jnp.int32, (16, 128), 0)
    row = jnp.sum(
        jnp.where(lane == slot, pair[0], jnp.where(lane == slot + 64, pair[1], 0.0)),
        axis=0,
        keepdims=True,
    )
    sums[...] = jnp.broadcast_to(row, sums.shape)


def basis(side, tile, other, ocean, inertia, east, south, devices):
    return pl.pallas_call(
        basis_kernel,
        out_shape=(
            pltpu.VMEM(inertia.shape, F32),
            pltpu.VMEM((devices, 128), F32),
        ),
        compiler_params=limit(24),
        in_specs=[smem()] + [vmem()] * 6,
        out_specs=(vmem(), vmem()),
        name="basis",
    )(side, *on_chip(tile, other, ocean, inertia, east, south))


def solve_kernel(sums, forcing, inertia, east, south, field, residual):
    rows, cols = field.shape
    s = sums[...]
    pair = (s, jnp.zeros_like(s))
    while pair[0].shape[0] > 8:
        n = pair[0].shape[0] // 2
        pair = pair_add((pair[0][:n], pair[1][:n]), (pair[0][n:], pair[1][n:]))
    for step in (4, 2, 1):
        pair = pair_add(pair, (pltpu.roll(pair[0], step, 0), pltpu.roll(pair[1], step, 0)))
    pair = quick_sum(pair[0], pair[1] + pltpu.roll(pair[0], 64, 1))

    def entry(k):
        return tuple(jnp.broadcast_to(x[0:1, k : k + 1], (8, 128)) for x in pair)

    right = [entry(k) for k in range(MOMENTS)]
    ahead = list(right)
    steps, ratios = [], []
    for k in range(ITERS):
        step = pair_div(right[k], ahead[k + 1])
        steps.append(step[0])
        if k + 1 < ITERS:
            last = MOMENTS - 1 - k
            new = list(right)
            for m in range(k + 1, last):
                new[m] = pair_add(right[m], pair_neg(pair_mul(step, ahead[m + 1])))
            ratio = pair_neg(pair_mul(step, pair_div(new[k + 1], right[k])))
            for m in range(k + 1, last):
                ahead[m] = pair_add(new[m], pair_mul(ratio, ahead[m]))
            right = new
            ratios.append(ratio[0])
    weights = (inertia[...], east[...], south[...])
    left = forcing[...]
    heading = left
    total = None
    for k in range(ITERS):
        step = steps[k][0:1, 0:1]
        total = step * heading if total is None else total + step * heading
        left = left - step * apply_plain(heading, *weights)
        if k + 1 < ITERS:
            heading = left + ratios[k][0:1, 0:1] * heading
    field[...] = total[8 : 8 + rows, :cols]
    residual[...] = left[8 : 8 + rows, :cols]


def solve(sums, forcing, inertia, east, south, rows, cols):
    shape = jax.ShapeDtypeStruct((rows, cols), F32)
    return pl.pallas_call(
        solve_kernel,
        out_shape=(shape, shape),
        compiler_params=limit(16),
        in_specs=[vmem()] * 5,
        out_specs=(vmem(), vmem()),
        name="solve",
    )(*on_chip(sums, forcing, inertia, east, south))


def around(value, axis, steps):
    count = lax.axis_size(axis)
    return lax.ppermute(value, axis, [(i, (i + steps) % count) for i in range(count)])


def body(
    innovation,
    obs_error,
    obs_offset,
    obs_cell,
    obs_owner,
    block_count,
    land_mask,
    inertia,
    sea_depth,
):
    n_lat = lax.axis_size("lat")
    n_lon = lax.axis_size(LON)
    n_obs = lax.axis_size("obs")
    tiles = n_lat * n_lon
    rows, cols = land_mask.shape
    sent = pack(obs_owner, block_count, innovation, obs_error, obs_offset, obs_cell, tiles)
    arrived = lax.all_to_all(
        sent.reshape(tiles, CAP * WORDS, 1, 128), LAT_LON, split_axis=0, concat_axis=0, tiled=True
    ).reshape(tiles * CAP * WORDS, 128)

    conduct = land_mask.astype(F32) * sea_depth
    lane = lax.broadcasted_iota(jnp.int32, (1, 128), 1)
    stacked = jnp.stack([conduct, inertia])
    from_west = around(stacked[:, :, cols - 128 :], LON, 1)
    from_east = around(stacked[:, :, :128], LON, -1)
    wide = jnp.concatenate([stacked, jnp.where(lane < 64, from_east, from_west)], axis=2)
    above = around(wide[:, rows - 8 :], LAT_OBS, 1)
    below = around(wide[:, :8], LAT_OBS, -1)
    conduct, inertia = jnp.concatenate([above, wide, below], axis=1)
    ocean = (conduct > 0.0).astype(F32)
    east = jnp.sqrt(conduct * jnp.roll(conduct, -1, 1))
    south = jnp.sqrt(conduct * jnp.roll(conduct, -1, 0))

    part = deposit(arrived, rows * n_obs, cols)
    tile = part + around(part, "obs", 1)
    spill = tile[:, cols:]
    from_west = around(jnp.where(lane == 0, spill[:, :1], tile[:, cols - 128 : cols]), LON, 1)
    from_east = around(tile[:, :128], LON, -1)
    tile = jnp.concatenate(
        [
            tile[:, :128] + jnp.where(lane == 0, from_west, 0.0),
            tile[:, 128:cols],
            jnp.where(lane < 64, from_east, from_west) + spill,
        ],
        axis=1,
    )
    side = lax.axis_index("obs").astype(jnp.int32)
    outer = jnp.where(side == 0, tile[:16], tile[2 * rows - 8 : 2 * rows + 8])
    swap = []
    for i in range(n_lat):
        swap.append((2 * i + 1, (2 * i + 2) % (2 * n_lat)))
        swap.append((2 * i, (2 * i - 1) % (2 * n_lat)))
    other = lax.ppermute(outer, LAT_OBS, swap)
    forcing, sums = basis(
        side.reshape(1), tile, other, ocean, inertia, east, south, tiles * n_obs
    )
    sums = lax.all_to_all(
        sums.reshape(tiles * n_obs, 1, 128), LAT_LON_OBS, split_axis=0, concat_axis=0, tiled=True
    ).reshape(tiles * n_obs, 128)
    return solve(sums, forcing, inertia, east, south, rows, cols)


def solution(mesh):
    split = Mesh(
        mesh.devices.reshape(mesh.shape["lat"], 4, 4, mesh.shape["obs"]),
        ("lat", "lon_0", "lon_1", "obs"),
    )
    return jax.shard_map(
        body,
        mesh=split,
        in_specs=(
            P(LAT_LON_OBS, None),
            P(LAT_LON_OBS, None),
            P(None, LAT_LON_OBS, None),
            P(LAT_LON_OBS, None),
            P(LAT_LON_OBS, None),
            P(LAT_LON_OBS),
            P(LAT_OBS, LON),
            P(LAT_OBS, LON),
            P(LAT_OBS, LON),
        ),
        out_specs=(P(LAT_OBS, LON), P(LAT_OBS, LON)),
        check_vma=False,
    )
```

```python
import jax
import jax.numpy as jnp
from jax import lax
from jax.experimental import pallas as pl
from jax.experimental.pallas import tpu as pltpu
from jax.sharding import Mesh
from jax.sharding import PartitionSpec as P

ITERS = 5
MOMENTS = 2 * ITERS
CAP = 3
WORDS = 4
LON = ("lon_0", "lon_1")
LAT_OBS = ("lat", "obs")
LAT_LON_OBS = ("lat", "lon_0", "lon_1", "obs")
LAT_LON = ("lat", "lon_0", "lon_1")
F32 = jnp.float32
BF16 = jnp.bfloat16
GROUPS = 4
WINDOW = 24
STEP = 16


def vmem():
    return pl.BlockSpec(memory_space=pltpu.VMEM)


def smem():
    return pl.BlockSpec(memory_space=pltpu.SMEM)


def on_chip(*values):
    return [pltpu.with_memory_space_constraint(v, pltpu.MemorySpace.VMEM) for v in values]


def limit(mib):
    return pltpu.CompilerParams(vmem_limit_bytes=mib * 2**20)


def pack_kernel(owner, count, innovation, error, offset, cell, out, rows, seen):
    blocks = innovation.shape[0]
    tiles = out.shape[0] // (CAP * WORDS)
    err = error[...]
    rows[pl.ds(0, blocks, stride=WORDS), :] = innovation[...] / (err * err)
    rows[pl.ds(1, blocks, stride=WORDS), :] = offset[0]
    rows[pl.ds(2, blocks, stride=WORDS), :] = offset[1]
    rows[pl.ds(3, blocks, stride=WORDS), :] = cell[...].astype(F32)
    out[...] = jnp.zeros(out.shape, F32)

    def clear(tile, carry):
        seen[tile] = 0
        return carry

    lax.fori_loop(0, tiles, clear, 0, unroll=8)

    live_total = count[0]

    def place(block, carry):
        live = block < live_total
        tile = owner[0, block]
        rank = seen[tile]
        seen[tile] = rank + live.astype(jnp.int32)
        source = jnp.where(live, block, 0)
        slot = jnp.where(live, tile * CAP + rank, owner[0, 0] * CAP)
        out[pl.ds(slot * WORDS, WORDS), :] = rows[pl.ds(source * WORDS, WORDS), :]
        return carry

    lax.fori_loop(0, blocks, place, 0, unroll=8)


def pack(owner, count, innovation, error, offset, cell, tiles):
    blocks = innovation.shape[0]
    return pl.pallas_call(
        pack_kernel,
        out_shape=jax.ShapeDtypeStruct((tiles * CAP * WORDS, 128), F32),
        in_specs=[smem(), smem(), vmem(), vmem(), vmem(), vmem()],
        out_specs=vmem(),
        scratch_shapes=[pltpu.VMEM((blocks * WORDS, 128), F32), pltpu.SMEM((tiles,), jnp.int32)],
        name="pack",
    )(owner, count, innovation, error, offset, cell)


SORT_8 = (
    (0, 1), (2, 3), (4, 5), (6, 7), (0, 2), (1, 3), (4, 6), (5, 7), (1, 2), (5, 6),
    (0, 4), (1, 5), (2, 6), (3, 7), (2, 4), (3, 5), (1, 2), (3, 4), (5, 6),
)
CLEAN_8 = (
    (0, 4), (1, 5), (2, 6), (3, 7), (0, 2), (1, 3), (4, 6), (5, 7), (0, 1), (2, 3), (4, 5), (6, 7),
)


def quotient(x, n):
    return x >> (n.bit_length() - 1) if n & (n - 1) == 0 else x // n


def remainder(x, n):
    return x & (n - 1) if n & (n - 1) == 0 else x % n


def deposit(arrived, tile_rows, tile_cols):
    slots = arrived.shape[0] // WORDS
    width = tile_cols // GROUPS
    m_one = GROUPS * WINDOW
    m_all = 4 * m_one
    depth = tile_rows + WINDOW - 8
    filled = -(-slots // 8)
    regs = 8
    while regs < filled:
        regs *= 2
    total = -(-slots // 8)
    row_pad = (tile_rows + 1 + 7) // 8 * 8
    index_rows = max(m_one, width)
    middle = index_rows // 2
    last_cell = float(tile_rows * tile_cols - 1)
    parts = regs // 8
    entries = total * (tile_rows // STEP + 1) + 8

    def kernel(src, out, held, left_a, left_b, right_a, right_b, acc, index, span_v, span_s, at, row_of, room, sem):
        index[...] = (lax.broadcasted_iota(jnp.int32, index.shape, 0) - middle).astype(F32).astype(BF16)
        acc[...] = jnp.zeros(acc.shape, F32)
        sub = lax.broadcasted_iota(jnp.int32, (8, 128), 0)

        def load(p):
            return [held[w, p] for w in range(WORDS)]

        def store(p, x):
            for w in range(WORDS):
                held[w, p] = x[w]

        def ordered(a, b):
            m = a[3] <= b[3]
            return (
                [jnp.where(m, x, y) for x, y in zip(a, b)],
                [jnp.where(m, y, x) for x, y in zip(a, b)],
            )

        def network(places, pairs):
            xs = [load(p) for p in places]
            for a, b in pairs:
                xs[a], xs[b] = ordered(xs[a], xs[b])
            for p, x in zip(places, xs):
                store(p, x)

        def first(g, carry):
            xs = []
            for i in range(8):
                base = pl.multiple_of((g * 8 + i) * 8 * WORDS, 8 * WORDS)
                xs.append([src[pl.ds(base + w, 8, stride=WORDS), :] for w in range(WORDS)])
            for a, b in SORT_8:
                xs[a], xs[b] = ordered(xs[a], xs[b])
            for i in range(8):
                store(g * 8 + i, xs[i])
            return carry

        lax.fori_loop(0, filled // 8, first, 0)
        for p in range(filled, regs):
            for w in range(WORDS):
                held[w, p] = jnp.full((8, 128), 1.0e9 if w == 3 else 0.0, F32)

        def near(g, carry):
            network([g * 8 + i for i in range(8)], CLEAN_8)
            return carry

        def several(pairs):
            for p, q in pairs:
                x, y = ordered(load(p), load(q))
                store(p, x)
                store(q, y)

        size = 16
        while size <= regs:
            h = size // 2
            several([(t // h * size + t % h, t // h * size + size - 1 - t % h) for t in range(regs // 2)])
            d = h // 2
            while d >= 8:
                several([(t // d * 2 * d + t % d, t // d * 2 * d + t % d + d) for t in range(regs // 2)])
                d //= 2
            lax.fori_loop(0, regs // 8, near, 0)
            size *= 2

        def turned(x, mask):
            return jnp.take_along_axis(x, sub ^ mask, axis=0, mode="promise_in_bounds")

        for k in range(3):
            mask = (2 << k) - 1
            low = (sub & (1 << k)) == 0
            for p in range(regs // 2):
                a = load(p)
                b = [turned(x, mask) for x in load(regs - 1 - p)]
                m = (a[3] <= b[3]) == low
                store(p, [jnp.where(m, x, y) for x, y in zip(a, b)])
                store(regs - 1 - p, [turned(jnp.where(m, y, x), mask) for x, y in zip(a, b)])
            for bit in range(k - 1, -1, -1):
                low_bit = (sub & (1 << bit)) == 0
                for p in range(regs):
                    a = load(p)
                    c = [turned(x, 1 << bit) for x in a]
                    m = jnp.where(low_bit, a[3], c[3]) <= jnp.where(low_bit, c[3], a[3])
                    store(p, [jnp.where(m, x, y) for x, y in zip(a, c)])
            d = regs // 2
            while d >= 8:
                if d == 32:

                    def far(g, carry):
                        network([g + 8 * i for i in range(8)], CLEAN_8)
                        return carry

                    lax.fori_loop(0, 8, far, 0)
                    d = 4
                else:
                    several([(t // d * 2 * d + t % d, t // d * 2 * d + t % d + d) for t in range(regs // 2)])
                    d //= 2
            lax.fori_loop(0, regs // 8, near, 0)

        lane = lax.broadcasted_iota(jnp.int32, (8, 128), 1)
        spans = jnp.zeros((8, 128), jnp.int32)
        for i in range(parts):
            low = jnp.min(jnp.minimum(held[3, 8 * i], last_cell), axis=1, keepdims=True)
            high = jnp.max(jnp.minimum(held[3, 8 * i + 7], last_cell), axis=1, keepdims=True)
            low = quotient(low.astype(jnp.int32), tile_cols)
            high = quotient(high.astype(jnp.int32), tile_cols)
            spans = jnp.where(lane == i, low, jnp.where(lane == 64 + i, high, spans))
        span_v[...] = spans
        copy = pltpu.make_async_copy(span_v, span_s, sem)
        copy.start()
        copy.wait()

        def plan(c, t):
            s = c // parts
            i = c % parts
            low = span_s[s, i]
            high = span_s[s, 64 + i]

            def note(t, row, rows):
                at[t] = c
                row_of[t] = row
                room[t] = rows

            def further(x):
                note(x[1], x[0], STEP)
                return x[0] + STEP, x[1] + 1

            row, t = lax.while_loop(lambda x: high - x[0] >= WINDOW - 1, further, (low // 8 * 8, t))
            note(t, row, WINDOW - 1)
            return t + 1

        count = lax.fori_loop(0, -(-slots // regs) * parts, plan, jnp.int32(0))
        for e in range(3):
            at[count + e] = 0
            row_of[count + e] = 0
            room[count + e] = 0

        def spread(x, j):
            pair = jnp.concatenate([x[2 * j : 2 * j + 1], x[2 * j + 1 : 2 * j + 2]], axis=1)
            return jnp.broadcast_to(pair, (16, 256)).astype(BF16)

        def build(t, left, right):
            c = at[t]
            s = c // parts
            i = c % parts
            amount, north, east, cell = [held[w, pl.ds(i * 8, 8), s, :] for w in range(WORDS)]
            cell = cell.astype(jnp.int32)
            row = quotient(cell, tile_cols) - row_of[t]
            col = remainder(cell, tile_cols)
            inside = (row >= 0) & (row < room[t])
            place = quotient(col, width) * WINDOW + row - middle
            m_here = jnp.where(inside, place, 8 * index_rows).astype(F32)
            m_next = m_here + 1.0
            n_here = (remainder(col, width) - middle).astype(F32)
            pieces = []
            for value in (amount, amount * east):
                low = value * (1.0 - north)
                high = value * north
                low_top = low.astype(BF16).astype(F32)
                high_top = high.astype(BF16).astype(F32)
                pieces += [(low_top, high_top), (low - low_top, high - high_top)]
            zero = jnp.zeros((16, 256), BF16)
            one = jnp.ones((16, 256), BF16)
            for j in range(4):
                here = spread(m_here, j)
                after = spread(m_next, j)
                column = spread(n_here, j)
                values = [(spread(x, j), spread(y, j)) for x, y in pieces]
                for q in range(m_one // 16):
                    own = index[q * 16 : (q + 1) * 16]
                    at_row = own == here
                    at_next = own == after
                    for f, (low, high) in enumerate(values):
                        left[j, f * m_one + q * 16 : f * m_one + (q + 1) * 16] = jnp.where(
                            at_row, low, jnp.where(at_next, high, zero)
                        )
                for q in range(width // 16):
                    right[j, q * 16 : (q + 1) * 16] = jnp.where(
                        index[q * 16 : (q + 1) * 16] == column, one, zero
                    )

        def joined(ref):
            return jnp.concatenate([ref[j] for j in range(4)], axis=1)

        def add(t, left, right):
            row = pl.multiple_of(row_of[t], 8)
            product = lax.dot_general(
                joined(left), joined(right), (((1,), (1,)), ((), ())), preferred_element_type=F32
            )
            for q in range(4 * GROUPS):
                acc[q, pl.ds(row, WINDOW), :] += product[q * WINDOW : (q + 1) * WINDOW]

        build(0, left_a, right_a)

        def turn(i, carry):
            build(2 * i + 1, left_b, right_b)
            add(2 * i, left_a, right_a)
            build(2 * i + 2, left_a, right_a)
            add(2 * i + 1, left_b, right_b)
            return carry

        lax.fori_loop(0, (count + 1) // 2, turn, 0)
        lane = lax.broadcasted_iota(jnp.int32, (row_pad, width), 1)
        before = jnp.zeros((row_pad, 1), F32)
        for g in range(GROUPS):
            whole = acc[g, 0:row_pad] + acc[GROUPS + g, 0:row_pad]
            part = acc[2 * GROUPS + g, 0:row_pad] + acc[3 * GROUPS + g, 0:row_pad]
            moved = pltpu.roll(part, 1, 1)
            moved = jnp.where(lane == 0, jnp.broadcast_to(before, (row_pad, width)), moved)
            out[:, g * width : (g + 1) * width] = whole - part + moved
            before = part[:, width - 1 : width]
        edge = lax.broadcasted_iota(jnp.int32, (row_pad, 128), 1)
        out[:, tile_cols : tile_cols + 128] = jnp.where(
            edge == 0, jnp.broadcast_to(before, (row_pad, 128)), 0.0
        )

    return pl.pallas_call(
        kernel,
        out_shape=pltpu.VMEM((row_pad, tile_cols + 128), F32),
        compiler_params=limit(24),
        in_specs=[vmem()],
        out_specs=vmem(),
        scratch_shapes=[
            pltpu.VMEM((WORDS, regs, 8, 128), F32),
            pltpu.VMEM((4, m_all, 256), BF16),
            pltpu.VMEM((4, m_all, 256), BF16),
            pltpu.VMEM((4, width, 256), BF16),
            pltpu.VMEM((4, width, 256), BF16),
            pltpu.VMEM((4 * GROUPS, depth, width), F32),
            pltpu.VMEM((index_rows, 256), BF16),
            pltpu.VMEM((8, 128), jnp.int32),
            pltpu.SMEM((8, 128), jnp.int32),
            pltpu.SMEM((entries,), jnp.int32),
            pltpu.SMEM((entries,), jnp.int32),
            pltpu.SMEM((entries,), jnp.int32),
            pltpu.SemaphoreType.DMA,
        ],
        name="deposit",
    )(*on_chip(arrived))


def two_sum(a, b):
    s = a + b
    t = s - a
    return s, (a - (s - t)) + (b - t)


def quick_sum(a, b):
    s = a + b
    return s, b - (s - a)


def halves(a):
    t = a * 4097.0
    top = t - (t - a)
    return top, a - top


def two_prod(a, b, a_halves, b_halves):
    p = a * b
    a1, a2 = a_halves
    b1, b2 = b_halves
    return p, ((a1 * b1 - p) + a1 * b2 + a2 * b1) + a2 * b2


def pair_add(a, b):
    s, e = two_sum(a[0], b[0])
    return quick_sum(s, e + (a[1] + b[1]))


def pair_mul(a, b):
    p, e = two_prod(a[0], b[0], halves(a[0]), halves(b[0]))
    return quick_sum(p, e + (a[0] * b[1] + a[1] * b[0]))


def pair_neg(a):
    return -a[0], -a[1]


def pair_div(a, b):
    q1 = a[0] / b[0]
    zero = jnp.zeros_like(q1)
    rest = pair_add(a, pair_neg(pair_mul((q1, zero), b)))
    q2 = rest[0] / b[0]
    rest = pair_add(rest, pair_neg(pair_mul((q2, zero), b)))
    q3 = rest[0] / b[0]
    s, e = quick_sum(q1, q2)
    return quick_sum(s, e + q3)


def roll_to(x, step, axis):
    return pltpu.roll(x, step % x.shape[axis], axis)


def apply_pair(v, inertia, east, south):
    h, l = v
    h_cut = halves(h)
    total, e = two_prod(inertia[0], h, inertia[1], h_cut)
    rest = e + inertia[0] * l
    for axis, (face, face_cut) in ((1, east), (0, south)):
        other = roll_to(h, -1, axis)
        d = h - other
        t = d - h
        err = (h - (d - t)) - (other + t)
        low = (l - roll_to(l, -1, axis)) + err
        p, e = two_prod(face, d, face_cut, halves(d))
        low = e + face * low
        total, e = two_sum(total, p)
        rest = rest + (e + low)
        total, e = two_sum(total, -roll_to(p, 1, axis))
        rest = rest + (e - roll_to(low, 1, axis))
    return quick_sum(total, rest)


def apply_plain(v, inertia, east, south):
    total = inertia * v
    for axis, face in ((1, east), (0, south)):
        flow = face * (v - roll_to(v, -1, axis))
        total = total + (flow - roll_to(flow, 1, axis))
    return total


def pair_fold(a):
    while a[0].shape[0] > 8:
        n = a[0].shape[0] // 2
        a = pair_add((a[0][:n], a[1][:n]), (a[0][n:], a[1][n:]))
    while a[0].shape[1] > 128:
        n = a[0].shape[1] // 2
        a = pair_add((a[0][:, :n], a[1][:, :n]), (a[0][:, n:], a[1][:, n:]))
    for step in (4, 2, 1):
        a = pair_add(a, (pltpu.roll(a[0], step, 0), pltpu.roll(a[1], step, 0)))
    return a


def basis_kernel(side, tile, other, ocean, inertia, east, south, forcing, sums):
    rows, cols = inertia.shape[0] - 16, inertia.shape[1] - 128
    first = side[0] == 0
    middle = tile[pl.ds(pl.multiple_of(side[0] * rows, 8), rows), :]
    corner = jnp.where(first, other[8:16, :], 0.0)
    top = jnp.where(first, other[0:8, :], tile[rows - 8 : rows, :])
    bottom = jnp.where(
        first, tile[rows : rows + 8, :], other[0:8, :] + tile[2 * rows : 2 * rows + 8, :]
    )
    start = jnp.concatenate([top, middle[0:8] + corner, middle[8:], bottom], axis=0) * ocean[...]
    forcing[...] = start
    weights = [(w[...], halves(w[...])) for w in (inertia, east, south)]
    vectors = [(start, jnp.zeros_like(start))]
    for k in range(ITERS):
        vectors.append(apply_pair(vectors[-1], *weights))
    inner = [(h[8 : 8 + rows, :cols], l[8 : 8 + rows, :cols]) for h, l in vectors]
    cuts = [halves(h) for h, l in inner]
    lane = lax.broadcasted_iota(jnp.int32, (8, 128), 1)
    tops, lows = [], []
    for k in range(MOMENTS):
        i, j = k // 2, (k + 1) // 2
        a, b = inner[i], inner[j]
        p, e = two_prod(a[0], b[0], cuts[i], cuts[j])
        total = pair_fold((p, e + (a[0] * b[1] + a[1] * b[0])))
        tops.append(total[0][0:1])
        lows.append(total[1][0:1])
    blank = [jnp.zeros((16 - MOMENTS, 128), F32)]
    pair = (jnp.concatenate(tops + blank, 0), jnp.concatenate(lows + blank, 0))
    for step in (64, 32, 16, 8, 4, 2, 1):
        pair = pair_add(pair, (pltpu.roll(pair[0], step, 1), pltpu.roll(pair[1], step, 1)))
    lane = lax.broadcasted_iota(jnp.int32, (16, 128), 1)
    slot = lax.broadcasted_iota(jnp.int32, (16, 128), 0)
    row = jnp.sum(
        jnp.where(lane == slot, pair[0], jnp.where(lane == slot + 64, pair[1], 0.0)),
        axis=0,
        keepdims=True,
    )
    sums[...] = jnp.broadcast_to(row, sums.shape)


def basis(side, tile, other, ocean, inertia, east, south, devices):
    return pl.pallas_call(
        basis_kernel,
        out_shape=(
            pltpu.VMEM(inertia.shape, F32),
            pltpu.VMEM((devices, 128), F32),
        ),
        compiler_params=limit(24),
        in_specs=[smem()] + [vmem()] * 6,
        out_specs=(vmem(), vmem()),
        name="basis",
    )(side, *on_chip(tile, other, ocean, inertia, east, south))


def solve_kernel(sums, forcing, inertia, east, south, field, residual):
    rows, cols = field.shape
    s = sums[...]
    pair = (s, jnp.zeros_like(s))
    while pair[0].shape[0] > 8:
        n = pair[0].shape[0] // 2
        pair = pair_add((pair[0][:n], pair[1][:n]), (pair[0][n:], pair[1][n:]))
    for step in (4, 2, 1):
        pair = pair_add(pair, (pltpu.roll(pair[0], step, 0), pltpu.roll(pair[1], step, 0)))
    pair = quick_sum(pair[0], pair[1] + pltpu.roll(pair[0], 64, 1))

    def entry(k):
        return tuple(jnp.broadcast_to(x[0:1, k : k + 1], (8, 128)) for x in pair)

    right = [entry(k) for k in range(MOMENTS)]
    ahead = list(right)
    steps, ratios = [], []
    for k in range(ITERS):
        step = pair_div(right[k], ahead[k + 1])
        steps.append(step[0])
        if k + 1 < ITERS:
            last = MOMENTS - 1 - k
            new = list(right)
            for m in range(k + 1, last):
                new[m] = pair_add(right[m], pair_neg(pair_mul(step, ahead[m + 1])))
            ratio = pair_neg(pair_mul(step, pair_div(new[k + 1], right[k])))
            for m in range(k + 1, last):
                ahead[m] = pair_add(new[m], pair_mul(ratio, ahead[m]))
            right = new
            ratios.append(ratio[0])
    weights = (inertia[...], east[...], south[...])
    left = forcing[...]
    heading = left
    total = None
    for k in range(ITERS):
        step = steps[k][0:1, 0:1]
        total = step * heading if total is None else total + step * heading
        left = left - step * apply_plain(heading, *weights)
        if k + 1 < ITERS:
            heading = left + ratios[k][0:1, 0:1] * heading
    field[...] = total[8 : 8 + rows, :cols]
    residual[...] = left[8 : 8 + rows, :cols]


def solve(sums, forcing, inertia, east, south, rows, cols):
    shape = jax.ShapeDtypeStruct((rows, cols), F32)
    return pl.pallas_call(
        solve_kernel,
        out_shape=(shape, shape),
        compiler_params=limit(16),
        in_specs=[vmem()] * 5,
        out_specs=(vmem(), vmem()),
        name="solve",
    )(*on_chip(sums, forcing, inertia, east, south))


def around(value, axis, steps):
    count = lax.axis_size(axis)
    return lax.ppermute(value, axis, [(i, (i + steps) % count) for i in range(count)])


def body(
    innovation,
    obs_error,
    obs_offset,
    obs_cell,
    obs_owner,
    block_count,
    land_mask,
    inertia,
    sea_depth,
):
    n_lat = lax.axis_size("lat")
    n_lon = lax.axis_size(LON)
    n_obs = lax.axis_size("obs")
    tiles = n_lat * n_lon
    rows, cols = land_mask.shape
    sent = pack(obs_owner, block_count, innovation, obs_error, obs_offset, obs_cell, tiles)
    arrived = lax.all_to_all(
        sent.reshape(tiles, CAP * WORDS, 1, 128), LAT_LON, split_axis=0, concat_axis=0, tiled=True
    ).reshape(tiles * CAP * WORDS, 128)

    conduct = land_mask.astype(F32) * sea_depth
    lane = lax.broadcasted_iota(jnp.int32, (1, 128), 1)
    stacked = jnp.stack([conduct, inertia])
    from_west = around(stacked[:, :, cols - 128 :], LON, 1)
    from_east = around(stacked[:, :, :128], LON, -1)
    wide = jnp.concatenate([stacked, jnp.where(lane < 64, from_east, from_west)], axis=2)
    above = around(wide[:, rows - 8 :], LAT_OBS, 1)
    below = around(wide[:, :8], LAT_OBS, -1)
    part = deposit(arrived, rows * n_obs, cols)
    tile = part + around(part, "obs", 1)
    tile, above, below = lax.optimization_barrier((tile, above, below))
    conduct, inertia = jnp.concatenate([above, wide, below], axis=1)
    ocean = (conduct > 0.0).astype(F32)
    east = jnp.sqrt(conduct * jnp.roll(conduct, -1, 1))
    south = jnp.sqrt(conduct * jnp.roll(conduct, -1, 0))
    spill = tile[:, cols:]
    from_west = around(jnp.where(lane == 0, spill[:, :1], tile[:, cols - 128 : cols]), LON, 1)
    from_east = around(tile[:, :128], LON, -1)
    tile = jnp.concatenate(
        [
            tile[:, :128] + jnp.where(lane == 0, from_west, 0.0),
            tile[:, 128:cols],
            jnp.where(lane < 64, from_east, from_west) + spill,
        ],
        axis=1,
    )
    side = lax.axis_index("obs").astype(jnp.int32)
    outer = jnp.where(side == 0, tile[:16], tile[2 * rows - 8 : 2 * rows + 8])
    swap = []
    for i in range(n_lat):
        swap.append((2 * i + 1, (2 * i + 2) % (2 * n_lat)))
        swap.append((2 * i, (2 * i - 1) % (2 * n_lat)))
    other = lax.ppermute(outer, LAT_OBS, swap)
    forcing, sums = basis(
        side.reshape(1), tile, other, ocean, inertia, east, south, tiles * n_obs
    )
    sums = lax.all_to_all(
        sums.reshape(tiles * n_obs, 1, 128), LAT_LON_OBS, split_axis=0, concat_axis=0, tiled=True
    ).reshape(tiles * n_obs, 128)
    return solve(sums, forcing, inertia, east, south, rows, cols)


def solution(mesh):
    split = Mesh(
        mesh.devices.reshape(mesh.shape["lat"], 4, 4, mesh.shape["obs"]),
        ("lat", "lon_0", "lon_1", "obs"),
    )
    return jax.shard_map(
        body,
        mesh=split,
        in_specs=(
            P(LAT_LON_OBS, None),
            P(LAT_LON_OBS, None),
            P(None, LAT_LON_OBS, None),
            P(LAT_LON_OBS, None),
            P(LAT_LON_OBS, None),
            P(LAT_LON_OBS),
            P(LAT_OBS, LON),
            P(LAT_OBS, LON),
            P(LAT_OBS, LON),
        ),
        out_specs=(P(LAT_OBS, LON), P(LAT_OBS, LON)),
        check_vma=False,
    )
```

```python
import jax
import jax.numpy as jnp
from jax import lax
from jax.experimental import pallas as pl
from jax.experimental.pallas import tpu as pltpu
from jax.sharding import Mesh
from jax.sharding import PartitionSpec as P

ITERS = 5
MOMENTS = 2 * ITERS
CAP = 3
WORDS = 4
LON = ("lon_0", "lon_1")
LAT_OBS = ("lat", "obs")
LAT_LON_OBS = ("lat", "lon_0", "lon_1", "obs")
LAT_LON = ("lat", "lon_0", "lon_1")
F32 = jnp.float32
BF16 = jnp.bfloat16
GROUPS = 4
WINDOW = 24
STEP = 16


def vmem():
    return pl.BlockSpec(memory_space=pltpu.VMEM)


def smem():
    return pl.BlockSpec(memory_space=pltpu.SMEM)


def on_chip(*values):
    return [pltpu.with_memory_space_constraint(v, pltpu.MemorySpace.VMEM) for v in values]


def limit(mib):
    return pltpu.CompilerParams(vmem_limit_bytes=mib * 2**20)


def pack_kernel(owner, count, innovation, error, offset, cell, out, rows, seen):
    blocks = innovation.shape[0]
    tiles = out.shape[0] // (CAP * WORDS)
    err = error[...]
    rows[pl.ds(0, blocks, stride=WORDS), :] = innovation[...] / (err * err)
    rows[pl.ds(1, blocks, stride=WORDS), :] = offset[0]
    rows[pl.ds(2, blocks, stride=WORDS), :] = offset[1]
    rows[pl.ds(3, blocks, stride=WORDS), :] = cell[...].astype(F32)
    out[...] = jnp.zeros(out.shape, F32)

    def clear(tile, carry):
        seen[tile] = 0
        return carry

    lax.fori_loop(0, tiles, clear, 0, unroll=8)

    live_total = count[0]

    def place(block, carry):
        live = block < live_total
        tile = owner[0, block]
        rank = seen[tile]
        seen[tile] = rank + live.astype(jnp.int32)
        source = jnp.where(live, block, 0)
        slot = jnp.where(live, tile * CAP + rank, owner[0, 0] * CAP)
        out[pl.ds(slot * WORDS, WORDS), :] = rows[pl.ds(source * WORDS, WORDS), :]
        return carry

    lax.fori_loop(0, blocks, place, 0, unroll=8)


def pack(owner, count, innovation, error, offset, cell, tiles):
    blocks = innovation.shape[0]
    return pl.pallas_call(
        pack_kernel,
        out_shape=jax.ShapeDtypeStruct((tiles * CAP * WORDS, 128), F32),
        in_specs=[smem(), smem(), vmem(), vmem(), vmem(), vmem()],
        out_specs=vmem(),
        scratch_shapes=[pltpu.VMEM((blocks * WORDS, 128), F32), pltpu.SMEM((tiles,), jnp.int32)],
        name="pack",
    )(owner, count, innovation, error, offset, cell)


SORT_8 = (
    (0, 1), (2, 3), (4, 5), (6, 7), (0, 2), (1, 3), (4, 6), (5, 7), (1, 2), (5, 6),
    (0, 4), (1, 5), (2, 6), (3, 7), (2, 4), (3, 5), (1, 2), (3, 4), (5, 6),
)
CLEAN_8 = (
    (0, 4), (1, 5), (2, 6), (3, 7), (0, 2), (1, 3), (4, 6), (5, 7), (0, 1), (2, 3), (4, 5), (6, 7),
)


def quotient(x, n):
    return x >> (n.bit_length() - 1) if n & (n - 1) == 0 else x // n


def remainder(x, n):
    return x & (n - 1) if n & (n - 1) == 0 else x % n


def deposit(arrived, tile_rows, tile_cols):
    slots = arrived.shape[0] // WORDS
    width = tile_cols // GROUPS
    m_one = GROUPS * WINDOW
    m_all = 4 * m_one
    depth = tile_rows + WINDOW - 8
    filled = -(-slots // 8)
    regs = 8
    while regs < filled:
        regs *= 2
    total = -(-slots // 8)
    row_pad = (tile_rows + 1 + 7) // 8 * 8
    index_rows = max(m_one, width)
    middle = index_rows // 2
    last_cell = float(tile_rows * tile_cols - 1)
    parts = regs // 8
    entries = total * (tile_rows // STEP + 1) + 8

    def kernel(src, out, held, left_a, left_b, right_a, right_b, acc, index, span_v, span_s, at, row_of, room, sem):
        index[...] = (lax.broadcasted_iota(jnp.int32, index.shape, 0) - middle).astype(F32).astype(BF16)
        acc[...] = jnp.zeros(acc.shape, F32)
        sub = lax.broadcasted_iota(jnp.int32, (8, 128), 0)

        def load(p):
            return [held[w, p] for w in range(WORDS)]

        def store(p, x):
            for w in range(WORDS):
                held[w, p] = x[w]

        def ordered(a, b):
            m = a[3] <= b[3]
            return (
                [jnp.where(m, x, y) for x, y in zip(a, b)],
                [jnp.where(m, y, x) for x, y in zip(a, b)],
            )

        def network(places, pairs):
            xs = [load(p) for p in places]
            for a, b in pairs:
                xs[a], xs[b] = ordered(xs[a], xs[b])
            for p, x in zip(places, xs):
                store(p, x)

        def first(g, carry):
            xs = []
            for i in range(8):
                base = pl.multiple_of((g * 8 + i) * 8 * WORDS, 8 * WORDS)
                xs.append([src[pl.ds(base + w, 8, stride=WORDS), :] for w in range(WORDS)])
            for a, b in SORT_8:
                xs[a], xs[b] = ordered(xs[a], xs[b])
            for i in range(8):
                store(g * 8 + i, xs[i])
            return carry

        lax.fori_loop(0, filled // 8, first, 0)
        for p in range(filled, regs):
            for w in range(WORDS):
                held[w, p] = jnp.full((8, 128), 1.0e9 if w == 3 else 0.0, F32)

        def near(g, carry):
            network([g * 8 + i for i in range(8)], CLEAN_8)
            return carry

        def several(pairs):
            for p, q in pairs:
                x, y = ordered(load(p), load(q))
                store(p, x)
                store(q, y)

        size = 16
        while size <= regs:
            h = size // 2
            several([(t // h * size + t % h, t // h * size + size - 1 - t % h) for t in range(regs // 2)])
            d = h // 2
            while d >= 8:
                several([(t // d * 2 * d + t % d, t // d * 2 * d + t % d + d) for t in range(regs // 2)])
                d //= 2
            lax.fori_loop(0, regs // 8, near, 0)
            size *= 2

        def turned(x, mask):
            return jnp.take_along_axis(x, sub ^ mask, axis=0, mode="promise_in_bounds")

        for k in range(3):
            mask = (2 << k) - 1
            low = (sub & (1 << k)) == 0
            for p in range(regs // 2):
                a = load(p)
                b = [turned(x, mask) for x in load(regs - 1 - p)]
                m = (a[3] <= b[3]) == low
                store(p, [jnp.where(m, x, y) for x, y in zip(a, b)])
                store(regs - 1 - p, [turned(jnp.where(m, y, x), mask) for x, y in zip(a, b)])
            for bit in range(k - 1, -1, -1):
                low_bit = (sub & (1 << bit)) == 0
                for p in range(regs):
                    a = load(p)
                    c = [turned(x, 1 << bit) for x in a]
                    m = jnp.where(low_bit, a[3], c[3]) <= jnp.where(low_bit, c[3], a[3])
                    store(p, [jnp.where(m, x, y) for x, y in zip(a, c)])
            d = regs // 2
            while d >= 8:
                if d == 32:

                    def far(g, carry):
                        network([g + 8 * i for i in range(8)], CLEAN_8)
                        return carry

                    lax.fori_loop(0, 8, far, 0)
                    d = 4
                else:
                    several([(t // d * 2 * d + t % d, t // d * 2 * d + t % d + d) for t in range(regs // 2)])
                    d //= 2
            lax.fori_loop(0, regs // 8, near, 0)

        lane = lax.broadcasted_iota(jnp.int32, (8, 128), 1)
        spans = jnp.zeros((8, 128), jnp.int32)
        for i in range(parts):
            low = jnp.min(jnp.minimum(held[3, 8 * i], last_cell), axis=1, keepdims=True)
            high = jnp.max(jnp.minimum(held[3, 8 * i + 7], last_cell), axis=1, keepdims=True)
            low = quotient(low.astype(jnp.int32), tile_cols)
            high = quotient(high.astype(jnp.int32), tile_cols)
            spans = jnp.where(lane == i, low, jnp.where(lane == 64 + i, high, spans))
        span_v[...] = spans
        copy = pltpu.make_async_copy(span_v, span_s, sem)
        copy.start()
        copy.wait()

        def plan(c, t):
            s = c // parts
            i = c % parts
            low = span_s[s, i]
            high = span_s[s, 64 + i]

            def note(t, row, rows):
                at[t] = c
                row_of[t] = row
                room[t] = rows

            def further(x):
                note(x[1], x[0], STEP)
                return x[0] + STEP, x[1] + 1

            row, t = lax.while_loop(lambda x: high - x[0] >= WINDOW - 1, further, (low // 8 * 8, t))
            note(t, row, WINDOW - 1)
            return t + 1

        count = lax.fori_loop(0, -(-slots // regs) * parts, plan, jnp.int32(0))
        for e in range(3):
            at[count + e] = 0
            row_of[count + e] = 0
            room[count + e] = 0

        def spread(x, j):
            pair = jnp.concatenate([x[2 * j : 2 * j + 1], x[2 * j + 1 : 2 * j + 2]], axis=1)
            return jnp.broadcast_to(pair, (16, 256)).astype(BF16)

        def build(t, left, right):
            c = at[t]
            s = c // parts
            i = c % parts
            amount, north, east, cell = [held[w, pl.ds(i * 8, 8), s, :] for w in range(WORDS)]
            cell = cell.astype(jnp.int32)
            row = quotient(cell, tile_cols) - row_of[t]
            col = remainder(cell, tile_cols)
            inside = (row >= 0) & (row < room[t])
            place = quotient(col, width) * WINDOW + row - middle
            m_here = jnp.where(inside, place, 8 * index_rows).astype(F32)
            m_next = m_here + 1.0
            n_here = (remainder(col, width) - middle).astype(F32)
            pieces = []
            for value in (amount, amount * east):
                low = value * (1.0 - north)
                high = value * north
                low_top = low.astype(BF16).astype(F32)
                high_top = high.astype(BF16).astype(F32)
                pieces += [(low_top, high_top), (low - low_top, high - high_top)]
            zero = jnp.zeros((16, 256), BF16)
            one = jnp.ones((16, 256), BF16)
            for j in range(4):
                here = spread(m_here, j)
                after = spread(m_next, j)
                column = spread(n_here, j)
                values = [(spread(x, j), spread(y, j)) for x, y in pieces]
                for q in range(m_one // 16):
                    own = index[q * 16 : (q + 1) * 16]
                    at_row = own == here
                    at_next = own == after
                    for f, (low, high) in enumerate(values):
                        left[j, f * m_one + q * 16 : f * m_one + (q + 1) * 16] = jnp.where(
                            at_row, low, jnp.where(at_next, high, zero)
                        )
                for q in range(width // 16):
                    right[j, q * 16 : (q + 1) * 16] = jnp.where(
                        index[q * 16 : (q + 1) * 16] == column, one, zero
                    )

        def joined(ref):
            return jnp.concatenate([ref[j] for j in range(4)], axis=1)

        def add(t, left, right):
            row = pl.multiple_of(row_of[t], 8)
            product = lax.dot_general(
                joined(left), joined(right), (((1,), (1,)), ((), ())), preferred_element_type=F32
            )
            for q in range(4 * GROUPS):
                acc[q, pl.ds(row, WINDOW), :] += product[q * WINDOW : (q + 1) * WINDOW]

        build(0, left_a, right_a)

        def turn(i, carry):
            build(2 * i + 1, left_b, right_b)
            add(2 * i, left_a, right_a)
            build(2 * i + 2, left_a, right_a)
            add(2 * i + 1, left_b, right_b)
            return carry

        lax.fori_loop(0, (count + 1) // 2, turn, 0)
        lane = lax.broadcasted_iota(jnp.int32, (row_pad, width), 1)
        before = jnp.zeros((row_pad, 1), F32)
        for g in range(GROUPS):
            whole = acc[g, 0:row_pad] + acc[GROUPS + g, 0:row_pad]
            part = acc[2 * GROUPS + g, 0:row_pad] + acc[3 * GROUPS + g, 0:row_pad]
            moved = pltpu.roll(part, 1, 1)
            moved = jnp.where(lane == 0, jnp.broadcast_to(before, (row_pad, width)), moved)
            out[:, g * width : (g + 1) * width] = whole - part + moved
            before = part[:, width - 1 : width]
        edge = lax.broadcasted_iota(jnp.int32, (row_pad, 128), 1)
        out[:, tile_cols : tile_cols + 128] = jnp.where(
            edge == 0, jnp.broadcast_to(before, (row_pad, 128)), 0.0
        )

    return pl.pallas_call(
        kernel,
        out_shape=pltpu.VMEM((row_pad, tile_cols + 128), F32),
        compiler_params=limit(24),
        in_specs=[vmem()],
        out_specs=vmem(),
        scratch_shapes=[
            pltpu.VMEM((WORDS, regs, 8, 128), F32),
            pltpu.VMEM((4, m_all, 256), BF16),
            pltpu.VMEM((4, m_all, 256), BF16),
            pltpu.VMEM((4, width, 256), BF16),
            pltpu.VMEM((4, width, 256), BF16),
            pltpu.VMEM((4 * GROUPS, depth, width), F32),
            pltpu.VMEM((index_rows, 256), BF16),
            pltpu.VMEM((8, 128), jnp.int32),
            pltpu.SMEM((8, 128), jnp.int32),
            pltpu.SMEM((entries,), jnp.int32),
            pltpu.SMEM((entries,), jnp.int32),
            pltpu.SMEM((entries,), jnp.int32),
            pltpu.SemaphoreType.DMA,
        ],
        name="deposit",
    )(*on_chip(arrived))


def two_sum(a, b):
    s = a + b
    t = s - a
    return s, (a - (s - t)) + (b - t)


def quick_sum(a, b):
    s = a + b
    return s, b - (s - a)


def halves(a):
    t = a * 4097.0
    top = t - (t - a)
    return top, a - top


def two_prod(a, b, a_halves, b_halves):
    p = a * b
    a1, a2 = a_halves
    b1, b2 = b_halves
    return p, ((a1 * b1 - p) + a1 * b2 + a2 * b1) + a2 * b2


def pair_add(a, b):
    s, e = two_sum(a[0], b[0])
    return quick_sum(s, e + (a[1] + b[1]))


def pair_mul(a, b):
    p, e = two_prod(a[0], b[0], halves(a[0]), halves(b[0]))
    return quick_sum(p, e + (a[0] * b[1] + a[1] * b[0]))


def pair_neg(a):
    return -a[0], -a[1]


def pair_div(a, b):
    q1 = a[0] / b[0]
    zero = jnp.zeros_like(q1)
    rest = pair_add(a, pair_neg(pair_mul((q1, zero), b)))
    q2 = rest[0] / b[0]
    rest = pair_add(rest, pair_neg(pair_mul((q2, zero), b)))
    q3 = rest[0] / b[0]
    s, e = quick_sum(q1, q2)
    return quick_sum(s, e + q3)


def roll_to(x, step, axis):
    return pltpu.roll(x, step % x.shape[axis], axis)


def apply_pair(v, inertia, east, south):
    h, l = v
    h_cut = halves(h)
    total, e = two_prod(inertia[0], h, inertia[1], h_cut)
    rest = e + inertia[0] * l
    for axis, (face, face_cut) in ((1, east), (0, south)):
        other = roll_to(h, -1, axis)
        d = h - other
        t = d - h
        err = (h - (d - t)) - (other + t)
        low = (l - roll_to(l, -1, axis)) + err
        p, e = two_prod(face, d, face_cut, halves(d))
        low = e + face * low
        total, e = two_sum(total, p)
        rest = rest + (e + low)
        total, e = two_sum(total, -roll_to(p, 1, axis))
        rest = rest + (e - roll_to(low, 1, axis))
    return quick_sum(total, rest)


def apply_plain(v, inertia, east, south):
    total = inertia * v
    for axis, face in ((1, east), (0, south)):
        flow = face * (v - roll_to(v, -1, axis))
        total = total + (flow - roll_to(flow, 1, axis))
    return total


def pair_fold(a):
    while a[0].shape[0] > 8:
        n = a[0].shape[0] // 2
        a = pair_add((a[0][:n], a[1][:n]), (a[0][n:], a[1][n:]))
    while a[0].shape[1] > 128:
        n = a[0].shape[1] // 2
        a = pair_add((a[0][:, :n], a[1][:, :n]), (a[0][:, n:], a[1][:, n:]))
    for step in (4, 2, 1):
        a = pair_add(a, (pltpu.roll(a[0], step, 0), pltpu.roll(a[1], step, 0)))
    return a


def basis_kernel(side, tile, other, ocean, inertia, east, south, forcing, sums):
    rows, cols = inertia.shape[0] - 16, inertia.shape[1] - 128
    first = side[0] == 0
    middle = tile[pl.ds(pl.multiple_of(side[0] * rows, 8), rows), :]
    corner = jnp.where(first, other[8:16, :], 0.0)
    top = jnp.where(first, other[0:8, :], tile[rows - 8 : rows, :])
    bottom = jnp.where(
        first, tile[rows : rows + 8, :], other[0:8, :] + tile[2 * rows : 2 * rows + 8, :]
    )
    start = jnp.concatenate([top, middle[0:8] + corner, middle[8:], bottom], axis=0) * ocean[...]
    forcing[...] = start
    weights = [(w[...], halves(w[...])) for w in (inertia, east, south)]
    vectors = [(start, jnp.zeros_like(start))]
    for k in range(ITERS):
        vectors.append(apply_pair(vectors[-1], *weights))
    inner = [(h[8 : 8 + rows, :cols], l[8 : 8 + rows, :cols]) for h, l in vectors]
    cuts = [halves(h) for h, l in inner]
    lane = lax.broadcasted_iota(jnp.int32, (8, 128), 1)
    tops, lows = [], []
    for k in range(MOMENTS):
        i, j = k // 2, (k + 1) // 2
        a, b = inner[i], inner[j]
        p, e = two_prod(a[0], b[0], cuts[i], cuts[j])
        total = pair_fold((p, e + (a[0] * b[1] + a[1] * b[0])))
        tops.append(total[0][0:1])
        lows.append(total[1][0:1])
    blank = [jnp.zeros((16 - MOMENTS, 128), F32)]
    pair = (jnp.concatenate(tops + blank, 0), jnp.concatenate(lows + blank, 0))
    for step in (64, 32, 16, 8, 4, 2, 1):
        pair = pair_add(pair, (pltpu.roll(pair[0], step, 1), pltpu.roll(pair[1], step, 1)))
    lane = lax.broadcasted_iota(jnp.int32, (16, 128), 1)
    slot = lax.broadcasted_iota(jnp.int32, (16, 128), 0)
    row = jnp.sum(
        jnp.where(lane == slot, pair[0], jnp.where(lane == slot + 64, pair[1], 0.0)),
        axis=0,
        keepdims=True,
    )
    sums[...] = jnp.broadcast_to(row, sums.shape)


def basis(side, tile, other, ocean, inertia, east, south, devices):
    return pl.pallas_call(
        basis_kernel,
        out_shape=(
            pltpu.VMEM(inertia.shape, F32),
            pltpu.VMEM((devices, 128), F32),
        ),
        compiler_params=limit(24),
        in_specs=[smem()] + [vmem()] * 6,
        out_specs=(vmem(), vmem()),
        name="basis",
    )(side, *on_chip(tile, other, ocean, inertia, east, south))


def solve_kernel(sums, forcing, inertia, east, south, field, residual):
    rows, cols = field.shape
    s = sums[...]
    pair = (s, jnp.zeros_like(s))
    while pair[0].shape[0] > 8:
        n = pair[0].shape[0] // 2
        pair = pair_add((pair[0][:n], pair[1][:n]), (pair[0][n:], pair[1][n:]))
    for step in (4, 2, 1):
        pair = pair_add(pair, (pltpu.roll(pair[0], step, 0), pltpu.roll(pair[1], step, 0)))
    pair = quick_sum(pair[0], pair[1] + pltpu.roll(pair[0], 64, 1))

    def entry(k):
        return tuple(jnp.broadcast_to(x[0:1, k : k + 1], (8, 128)) for x in pair)

    right = [entry(k) for k in range(MOMENTS)]
    ahead = list(right)
    steps, ratios = [], []
    for k in range(ITERS):
        step = pair_div(right[k], ahead[k + 1])
        steps.append(step[0])
        if k + 1 < ITERS:
            last = MOMENTS - 1 - k
            new = list(right)
            for m in range(k + 1, last):
                new[m] = pair_add(right[m], pair_neg(pair_mul(step, ahead[m + 1])))
            ratio = pair_neg(pair_mul(step, pair_div(new[k + 1], right[k])))
            for m in range(k + 1, last):
                ahead[m] = pair_add(new[m], pair_mul(ratio, ahead[m]))
            right = new
            ratios.append(ratio[0])
    weights = (inertia[...], east[...], south[...])
    left = forcing[...]
    heading = left
    total = None
    for k in range(ITERS):
        step = steps[k][0:1, 0:1]
        total = step * heading if total is None else total + step * heading
        left = left - step * apply_plain(heading, *weights)
        if k + 1 < ITERS:
            heading = left + ratios[k][0:1, 0:1] * heading
    field[...] = total[8 : 8 + rows, :cols]
    residual[...] = left[8 : 8 + rows, :cols]


def solve(sums, forcing, inertia, east, south, rows, cols):
    shape = jax.ShapeDtypeStruct((rows, cols), F32)
    return pl.pallas_call(
        solve_kernel,
        out_shape=(shape, shape),
        compiler_params=limit(16),
        in_specs=[vmem()] * 5,
        out_specs=(vmem(), vmem()),
        name="solve",
    )(*on_chip(sums, forcing, inertia, east, south))


def around(value, axis, steps):
    count = lax.axis_size(axis)
    return lax.ppermute(value, axis, [(i, (i + steps) % count) for i in range(count)])


def body(
    innovation,
    obs_error,
    obs_offset,
    obs_cell,
    obs_owner,
    block_count,
    land_mask,
    inertia,
    sea_depth,
):
    n_lat = lax.axis_size("lat")
    n_lon = lax.axis_size(LON)
    n_obs = lax.axis_size("obs")
    tiles = n_lat * n_lon
    rows, cols = land_mask.shape
    sent = pack(obs_owner, block_count, innovation, obs_error, obs_offset, obs_cell, tiles)
    arrived = lax.all_to_all(
        sent.reshape(tiles, CAP * WORDS, 1, 128), LAT_LON, split_axis=0, concat_axis=0, tiled=True
    ).reshape(tiles * CAP * WORDS, 128)

    conduct = land_mask.astype(F32) * sea_depth
    lane = lax.broadcasted_iota(jnp.int32, (1, 128), 1)
    stacked = jnp.stack([conduct, inertia])
    from_west = around(stacked[:, :, cols - 128 :], LON, 1)
    from_east = around(stacked[:, :, :128], LON, -1)
    wide = jnp.concatenate([stacked, jnp.where(lane < 64, from_east, from_west)], axis=2)
    above = around(wide[:, rows - 8 :], LAT_OBS, 1)
    below = around(wide[:, :8], LAT_OBS, -1)
    part = deposit(arrived, rows * n_obs, cols)
    part, above, below = lax.optimization_barrier((part, above, below))
    tile = part + around(part, "obs", 1)
    tile, above, below = lax.optimization_barrier((tile, above, below))
    conduct, inertia = jnp.concatenate([above, wide, below], axis=1)
    ocean = (conduct > 0.0).astype(F32)
    east = jnp.sqrt(conduct * jnp.roll(conduct, -1, 1))
    south = jnp.sqrt(conduct * jnp.roll(conduct, -1, 0))
    spill = tile[:, cols:]
    side = lax.axis_index("obs").astype(jnp.int32)
    leaving = jnp.where(
        side == 0, jnp.where(lane == 0, spill[:, :1], tile[:, cols - 128 : cols]), tile[:, :128]
    )
    split = []
    for i in range(n_lon):
        split.append((2 * i, 2 * ((i + 1) % n_lon)))
        split.append((2 * i + 1, 2 * ((i - 1) % n_lon) + 1))
    came = lax.ppermute(leaving, LON + ("obs",), split)
    swapped = around(came, "obs", 1)
    from_west = jnp.where(side == 0, came, swapped)
    from_east = jnp.where(side == 0, swapped, came)
    tile = jnp.concatenate(
        [
            tile[:, :128] + jnp.where(lane == 0, from_west, 0.0),
            tile[:, 128:cols],
            jnp.where(lane < 64, from_east, from_west) + spill,
        ],
        axis=1,
    )
    outer = jnp.where(side == 0, tile[:16], tile[2 * rows - 8 : 2 * rows + 8])
    swap = []
    for i in range(n_lat):
        swap.append((2 * i + 1, (2 * i + 2) % (2 * n_lat)))
        swap.append((2 * i, (2 * i - 1) % (2 * n_lat)))
    other = lax.ppermute(outer, LAT_OBS, swap)
    forcing, sums = basis(
        side.reshape(1), tile, other, ocean, inertia, east, south, tiles * n_obs
    )
    sums = lax.all_to_all(
        sums.reshape(tiles * n_obs, 1, 128), LAT_LON_OBS, split_axis=0, concat_axis=0, tiled=True
    ).reshape(tiles * n_obs, 128)
    return solve(sums, forcing, inertia, east, south, rows, cols)


def solution(mesh):
    split = Mesh(
        mesh.devices.reshape(mesh.shape["lat"], 4, 4, mesh.shape["obs"]),
        ("lat", "lon_0", "lon_1", "obs"),
    )
    return jax.shard_map(
        body,
        mesh=split,
        in_specs=(
            P(LAT_LON_OBS, None),
            P(LAT_LON_OBS, None),
            P(None, LAT_LON_OBS, None),
            P(LAT_LON_OBS, None),
            P(LAT_LON_OBS, None),
            P(LAT_LON_OBS),
            P(LAT_OBS, LON),
            P(LAT_OBS, LON),
            P(LAT_OBS, LON),
        ),
        out_specs=(P(LAT_OBS, LON), P(LAT_OBS, LON)),
        check_vma=False,
    )
```

```python
import jax
import jax.numpy as jnp
from jax import lax
from jax.experimental import pallas as pl
from jax.experimental.pallas import tpu as pltpu
from jax.sharding import Mesh
from jax.sharding import PartitionSpec as P

ITERS = 5
MOMENTS = 2 * ITERS
CAP = 3
WORDS = 4
LON = ("lon_0", "lon_1")
LAT_OBS = ("lat", "obs")
LAT_LON_OBS = ("lat", "lon_0", "lon_1", "obs")
LAT_LON = ("lat", "lon_0", "lon_1")
F32 = jnp.float32
BF16 = jnp.bfloat16
GROUPS = 4
WINDOW = 24
STEP = 16
RUN = 32


def vmem():
    return pl.BlockSpec(memory_space=pltpu.VMEM)


def smem():
    return pl.BlockSpec(memory_space=pltpu.SMEM)


def on_chip(*values):
    return [pltpu.with_memory_space_constraint(v, pltpu.MemorySpace.VMEM) for v in values]


def limit(mib):
    return pltpu.CompilerParams(vmem_limit_bytes=mib * 2**20)


def pack_kernel(owner, count, innovation, error, offset, cell, out, rows, seen):
    blocks = innovation.shape[0]
    tiles = out.shape[0] // (CAP * WORDS)
    err = error[...]
    rows[pl.ds(0, blocks, stride=WORDS), :] = innovation[...] / (err * err)
    rows[pl.ds(1, blocks, stride=WORDS), :] = offset[0]
    rows[pl.ds(2, blocks, stride=WORDS), :] = offset[1]
    rows[pl.ds(3, blocks, stride=WORDS), :] = cell[...].astype(F32)
    out[...] = jnp.zeros(out.shape, F32)

    def clear(tile, carry):
        seen[tile] = 0
        return carry

    lax.fori_loop(0, tiles, clear, 0, unroll=8)

    live_total = count[0]

    def place(block, carry):
        live = block < live_total
        tile = owner[0, block]
        rank = seen[tile]
        seen[tile] = rank + live.astype(jnp.int32)
        source = jnp.where(live, block, 0)
        slot = jnp.where(live, tile * CAP + rank, owner[0, 0] * CAP)
        out[pl.ds(slot * WORDS, WORDS), :] = rows[pl.ds(source * WORDS, WORDS), :]
        return carry

    lax.fori_loop(0, blocks, place, 0, unroll=8)


def pack(owner, count, innovation, error, offset, cell, tiles):
    blocks = innovation.shape[0]
    return pl.pallas_call(
        pack_kernel,
        out_shape=jax.ShapeDtypeStruct((tiles * CAP * WORDS, 128), F32),
        in_specs=[smem(), smem(), vmem(), vmem(), vmem(), vmem()],
        out_specs=vmem(),
        scratch_shapes=[pltpu.VMEM((blocks * WORDS, 128), F32), pltpu.SMEM((tiles,), jnp.int32)],
        name="pack",
    )(owner, count, innovation, error, offset, cell)


SORT_8 = (
    (0, 1), (2, 3), (4, 5), (6, 7), (0, 2), (1, 3), (4, 6), (5, 7), (1, 2), (5, 6),
    (0, 4), (1, 5), (2, 6), (3, 7), (2, 4), (3, 5), (1, 2), (3, 4), (5, 6),
)
CLEAN_8 = (
    (0, 4), (1, 5), (2, 6), (3, 7), (0, 2), (1, 3), (4, 6), (5, 7), (0, 1), (2, 3), (4, 5), (6, 7),
)


def quotient(x, n):
    return x >> (n.bit_length() - 1) if n & (n - 1) == 0 else x // n


def remainder(x, n):
    return x & (n - 1) if n & (n - 1) == 0 else x % n


def deposit(arrived, tile_rows, tile_cols):
    slots = arrived.shape[0] // WORDS
    width = tile_cols // GROUPS
    m_one = GROUPS * WINDOW
    m_all = 4 * m_one
    depth = tile_rows + WINDOW - 8
    filled = -(-slots // 8)
    regs = 8
    while regs < filled:
        regs *= 2
    total = -(-slots // 8)
    row_pad = (tile_rows + 1 + 7) // 8 * 8
    index_rows = max(m_one, width)
    middle = index_rows // 2
    last_cell = float(tile_rows * tile_cols - 1)
    parts = regs // RUN
    pairs = RUN // 2
    entries = total * (tile_rows // STEP + 1) + 8

    def kernel(src, out, held, left_a, left_b, right_a, right_b, acc, index, span_v, span_s, at, row_of, room, sem):
        index[...] = (lax.broadcasted_iota(jnp.int32, index.shape, 0) - middle).astype(F32).astype(BF16)
        acc[...] = jnp.zeros(acc.shape, F32)
        sub = lax.broadcasted_iota(jnp.int32, (8, 128), 0)

        def load(p):
            return [held[w, p] for w in range(WORDS)]

        def store(p, x):
            for w in range(WORDS):
                held[w, p] = x[w]

        def ordered(a, b):
            m = a[3] <= b[3]
            return (
                [jnp.where(m, x, y) for x, y in zip(a, b)],
                [jnp.where(m, y, x) for x, y in zip(a, b)],
            )

        def network(places, pairs):
            xs = [load(p) for p in places]
            for a, b in pairs:
                xs[a], xs[b] = ordered(xs[a], xs[b])
            for p, x in zip(places, xs):
                store(p, x)

        def first(g, carry):
            xs = []
            for i in range(8):
                base = pl.multiple_of((g * 8 + i) * 8 * WORDS, 8 * WORDS)
                xs.append([src[pl.ds(base + w, 8, stride=WORDS), :] for w in range(WORDS)])
            for a, b in SORT_8:
                xs[a], xs[b] = ordered(xs[a], xs[b])
            for i in range(8):
                store(g * 8 + i, xs[i])
            return carry

        lax.fori_loop(0, filled // 8, first, 0)
        for p in range(filled, regs):
            for w in range(WORDS):
                held[w, p] = jnp.full((8, 128), 1.0e9 if w == 3 else 0.0, F32)

        def near(g, carry):
            network([g * 8 + i for i in range(8)], CLEAN_8)
            return carry

        def several(pairs):
            for p, q in pairs:
                x, y = ordered(load(p), load(q))
                store(p, x)
                store(q, y)

        size = 16
        while size <= regs:
            h = size // 2
            several([(t // h * size + t % h, t // h * size + size - 1 - t % h) for t in range(regs // 2)])
            d = h // 2
            while d >= 8:
                several([(t // d * 2 * d + t % d, t // d * 2 * d + t % d + d) for t in range(regs // 2)])
                d //= 2
            lax.fori_loop(0, regs // 8, near, 0)
            size *= 2

        def turned(x, mask):
            return jnp.take_along_axis(x, sub ^ mask, axis=0, mode="promise_in_bounds")

        for k in range(3):
            mask = (2 << k) - 1
            low = (sub & (1 << k)) == 0
            for p in range(regs // 2):
                a = load(p)
                b = [turned(x, mask) for x in load(regs - 1 - p)]
                m = (a[3] <= b[3]) == low
                store(p, [jnp.where(m, x, y) for x, y in zip(a, b)])
                store(regs - 1 - p, [turned(jnp.where(m, y, x), mask) for x, y in zip(a, b)])
            for bit in range(k - 1, -1, -1):
                low_bit = (sub & (1 << bit)) == 0
                for p in range(regs):
                    a = load(p)
                    c = [turned(x, 1 << bit) for x in a]
                    m = jnp.where(low_bit, a[3], c[3]) <= jnp.where(low_bit, c[3], a[3])
                    store(p, [jnp.where(m, x, y) for x, y in zip(a, c)])
            d = regs // 2
            while d >= 8:
                if d == 32:

                    def far(g, carry):
                        network([g + 8 * i for i in range(8)], CLEAN_8)
                        return carry

                    lax.fori_loop(0, 8, far, 0)
                    d = 4
                else:
                    several([(t // d * 2 * d + t % d, t // d * 2 * d + t % d + d) for t in range(regs // 2)])
                    d //= 2
            lax.fori_loop(0, regs // 8, near, 0)

        lane = lax.broadcasted_iota(jnp.int32, (8, 128), 1)
        spans = jnp.zeros((8, 128), jnp.int32)
        for i in range(parts):
            low = jnp.min(jnp.minimum(held[3, RUN * i], last_cell), axis=1, keepdims=True)
            high = jnp.max(jnp.minimum(held[3, RUN * i + RUN - 1], last_cell), axis=1, keepdims=True)
            low = quotient(low.astype(jnp.int32), tile_cols)
            high = quotient(high.astype(jnp.int32), tile_cols)
            spans = jnp.where(lane == i, low, jnp.where(lane == 64 + i, high, spans))
        span_v[...] = spans
        copy = pltpu.make_async_copy(span_v, span_s, sem)
        copy.start()
        copy.wait()

        def plan(c, t):
            s = c // parts
            i = c % parts
            low = span_s[s, i]
            high = span_s[s, 64 + i]

            def note(t, row, rows):
                at[t] = c
                row_of[t] = row
                room[t] = rows

            def further(x):
                note(x[1], x[0], STEP)
                return x[0] + STEP, x[1] + 1

            row, t = lax.while_loop(lambda x: high - x[0] >= WINDOW - 1, further, (low // 8 * 8, t))
            note(t, row, WINDOW - 1)
            return t + 1

        count = lax.fori_loop(0, -(-slots // regs) * parts, plan, jnp.int32(0))
        for e in range(3):
            at[count + e] = 0
            row_of[count + e] = 0
            room[count + e] = 0

        def spread(x, j):
            pair = jnp.concatenate([x[2 * j : 2 * j + 1], x[2 * j + 1 : 2 * j + 2]], axis=1)
            return jnp.broadcast_to(pair, (16, 256)).astype(BF16)

        def build(t, left, right):
            c = at[t]
            s = c // parts
            i = c % parts
            amount, north, east, cell = [
                held[w, pl.ds(i * RUN, RUN), s, :] for w in range(WORDS)
            ]
            cell = cell.astype(jnp.int32)
            row = quotient(cell, tile_cols) - row_of[t]
            col = remainder(cell, tile_cols)
            inside = (row >= 0) & (row < room[t])
            place = quotient(col, width) * WINDOW + row - middle
            m_here = jnp.where(inside, place, 8 * index_rows).astype(F32)
            n_here = (remainder(col, width) - middle).astype(F32)
            pieces = []
            for value in (amount, amount * east):
                low = value * (1.0 - north)
                high = value * north
                low_top = low.astype(BF16).astype(F32)
                high_top = high.astype(BF16).astype(F32)
                pieces += [(low_top, high_top), (low - low_top, high - high_top)]
            zero = jnp.zeros((16, 256), BF16)
            one = jnp.ones((16, 256), BF16)
            for j in range(pairs):
                here = spread(m_here, j)
                after = here + one
                column = spread(n_here, j)
                values = [(spread(x, j), spread(y, j)) for x, y in pieces]
                for q in range(m_one // 16):
                    own = index[q * 16 : (q + 1) * 16]
                    at_row = jnp.where(own == here, one, zero)
                    at_next = jnp.where(own == after, one, zero)
                    for f, (low, high) in enumerate(values):
                        left[j, f * m_one + q * 16 : f * m_one + (q + 1) * 16] = (
                            at_row * low + at_next * high
                        )
                for q in range(width // 16):
                    right[j, q * 16 : (q + 1) * 16] = jnp.where(
                        index[q * 16 : (q + 1) * 16] == column, one, zero
                    )

        def joined(ref):
            return jnp.concatenate([ref[j] for j in range(pairs)], axis=1)

        def add(t, left, right):
            row = pl.multiple_of(row_of[t], 8)
            product = lax.dot_general(
                joined(left), joined(right), (((1,), (1,)), ((), ())), preferred_element_type=F32
            )
            for q in range(4 * GROUPS):
                acc[q, pl.ds(row, WINDOW), :] += product[q * WINDOW : (q + 1) * WINDOW]

        build(0, left_a, right_a)

        def turn(i, carry):
            build(2 * i + 1, left_b, right_b)
            add(2 * i, left_a, right_a)
            build(2 * i + 2, left_a, right_a)
            add(2 * i + 1, left_b, right_b)
            return carry

        lax.fori_loop(0, (count + 1) // 2, turn, 0)
        lane = lax.broadcasted_iota(jnp.int32, (row_pad, width), 1)
        before = jnp.zeros((row_pad, 1), F32)
        for g in range(GROUPS):
            whole = acc[g, 0:row_pad] + acc[GROUPS + g, 0:row_pad]
            part = acc[2 * GROUPS + g, 0:row_pad] + acc[3 * GROUPS + g, 0:row_pad]
            moved = pltpu.roll(part, 1, 1)
            moved = jnp.where(lane == 0, jnp.broadcast_to(before, (row_pad, width)), moved)
            out[:, g * width : (g + 1) * width] = whole - part + moved
            before = part[:, width - 1 : width]
        edge = lax.broadcasted_iota(jnp.int32, (row_pad, 128), 1)
        out[:, tile_cols : tile_cols + 128] = jnp.where(
            edge == 0, jnp.broadcast_to(before, (row_pad, 128)), 0.0
        )

    return pl.pallas_call(
        kernel,
        out_shape=pltpu.VMEM((row_pad, tile_cols + 128), F32),
        compiler_params=limit(32),
        in_specs=[vmem()],
        out_specs=vmem(),
        scratch_shapes=[
            pltpu.VMEM((WORDS, regs, 8, 128), F32),
            pltpu.VMEM((pairs, m_all, 256), BF16),
            pltpu.VMEM((pairs, m_all, 256), BF16),
            pltpu.VMEM((pairs, width, 256), BF16),
            pltpu.VMEM((pairs, width, 256), BF16),
            pltpu.VMEM((4 * GROUPS, depth, width), F32),
            pltpu.VMEM((index_rows, 256), BF16),
            pltpu.VMEM((8, 128), jnp.int32),
            pltpu.SMEM((8, 128), jnp.int32),
            pltpu.SMEM((entries,), jnp.int32),
            pltpu.SMEM((entries,), jnp.int32),
            pltpu.SMEM((entries,), jnp.int32),
            pltpu.SemaphoreType.DMA,
        ],
        name="deposit",
    )(*on_chip(arrived))


def two_sum(a, b):
    s = a + b
    t = s - a
    return s, (a - (s - t)) + (b - t)


def quick_sum(a, b):
    s = a + b
    return s, b - (s - a)


def halves(a):
    t = a * 4097.0
    top = t - (t - a)
    return top, a - top


def two_prod(a, b, a_halves, b_halves):
    p = a * b
    a1, a2 = a_halves
    b1, b2 = b_halves
    return p, ((a1 * b1 - p) + a1 * b2 + a2 * b1) + a2 * b2


def pair_add(a, b):
    s, e = two_sum(a[0], b[0])
    return quick_sum(s, e + (a[1] + b[1]))


def pair_mul(a, b):
    p, e = two_prod(a[0], b[0], halves(a[0]), halves(b[0]))
    return quick_sum(p, e + (a[0] * b[1] + a[1] * b[0]))


def pair_neg(a):
    return -a[0], -a[1]


def pair_div(a, b):
    q1 = a[0] / b[0]
    zero = jnp.zeros_like(q1)
    rest = pair_add(a, pair_neg(pair_mul((q1, zero), b)))
    q2 = rest[0] / b[0]
    rest = pair_add(rest, pair_neg(pair_mul((q2, zero), b)))
    q3 = rest[0] / b[0]
    s, e = quick_sum(q1, q2)
    return quick_sum(s, e + q3)


def roll_to(x, step, axis):
    return pltpu.roll(x, step % x.shape[axis], axis)


def apply_pair(v, inertia, east, south):
    h, l = v
    h_cut = halves(h)
    total, e = two_prod(inertia[0], h, inertia[1], h_cut)
    rest = e + inertia[0] * l
    for axis, (face, face_cut) in ((1, east), (0, south)):
        other = roll_to(h, -1, axis)
        d = h - other
        t = d - h
        err = (h - (d - t)) - (other + t)
        low = (l - roll_to(l, -1, axis)) + err
        p, e = two_prod(face, d, face_cut, halves(d))
        low = e + face * low
        total, e = two_sum(total, p)
        rest = rest + (e + low)
        total, e = two_sum(total, -roll_to(p, 1, axis))
        rest = rest + (e - roll_to(low, 1, axis))
    return quick_sum(total, rest)


def apply_plain(v, inertia, east, south):
    total = inertia * v
    for axis, face in ((1, east), (0, south)):
        flow = face * (v - roll_to(v, -1, axis))
        total = total + (flow - roll_to(flow, 1, axis))
    return total


def pair_fold(a):
    while a[0].shape[0] > 8:
        n = a[0].shape[0] // 2
        a = pair_add((a[0][:n], a[1][:n]), (a[0][n:], a[1][n:]))
    while a[0].shape[1] > 128:
        n = a[0].shape[1] // 2
        a = pair_add((a[0][:, :n], a[1][:, :n]), (a[0][:, n:], a[1][:, n:]))
    for step in (4, 2, 1):
        a = pair_add(a, (pltpu.roll(a[0], step, 0), pltpu.roll(a[1], step, 0)))
    return a


def basis_kernel(side, tile, other, ocean, inertia, east, south, forcing, sums):
    rows, cols = inertia.shape[0] - 16, inertia.shape[1] - 128
    first = side[0] == 0
    middle = tile[pl.ds(pl.multiple_of(side[0] * rows, 8), rows), :]
    corner = jnp.where(first, other[8:16, :], 0.0)
    top = jnp.where(first, other[0:8, :], tile[rows - 8 : rows, :])
    bottom = jnp.where(
        first, tile[rows : rows + 8, :], other[0:8, :] + tile[2 * rows : 2 * rows + 8, :]
    )
    start = jnp.concatenate([top, middle[0:8] + corner, middle[8:], bottom], axis=0) * ocean[...]
    forcing[...] = start
    weights = [(w[...], halves(w[...])) for w in (inertia, east, south)]
    vectors = [(start, jnp.zeros_like(start))]
    for k in range(ITERS):
        vectors.append(apply_pair(vectors[-1], *weights))
    inner = [(h[8 : 8 + rows, :cols], l[8 : 8 + rows, :cols]) for h, l in vectors]
    cuts = [halves(h) for h, l in inner]
    lane = lax.broadcasted_iota(jnp.int32, (8, 128), 1)
    tops, lows = [], []
    for k in range(MOMENTS):
        i, j = k // 2, (k + 1) // 2
        a, b = inner[i], inner[j]
        p, e = two_prod(a[0], b[0], cuts[i], cuts[j])
        total = pair_fold((p, e + (a[0] * b[1] + a[1] * b[0])))
        tops.append(total[0][0:1])
        lows.append(total[1][0:1])
    blank = [jnp.zeros((16 - MOMENTS, 128), F32)]
    pair = (jnp.concatenate(tops + blank, 0), jnp.concatenate(lows + blank, 0))
    for step in (64, 32, 16, 8, 4, 2, 1):
        pair = pair_add(pair, (pltpu.roll(pair[0], step, 1), pltpu.roll(pair[1], step, 1)))
    lane = lax.broadcasted_iota(jnp.int32, (16, 128), 1)
    slot = lax.broadcasted_iota(jnp.int32, (16, 128), 0)
    row = jnp.sum(
        jnp.where(lane == slot, pair[0], jnp.where(lane == slot + 64, pair[1], 0.0)),
        axis=0,
        keepdims=True,
    )
    sums[...] = jnp.broadcast_to(row, sums.shape)


def basis(side, tile, other, ocean, inertia, east, south, devices):
    return pl.pallas_call(
        basis_kernel,
        out_shape=(
            pltpu.VMEM(inertia.shape, F32),
            pltpu.VMEM((devices, 128), F32),
        ),
        compiler_params=limit(24),
        in_specs=[smem()] + [vmem()] * 6,
        out_specs=(vmem(), vmem()),
        name="basis",
    )(side, *on_chip(tile, other, ocean, inertia, east, south))


def solve_kernel(sums, forcing, inertia, east, south, field, residual):
    rows, cols = field.shape
    s = sums[...]
    pair = (s, jnp.zeros_like(s))
    while pair[0].shape[0] > 8:
        n = pair[0].shape[0] // 2
        pair = pair_add((pair[0][:n], pair[1][:n]), (pair[0][n:], pair[1][n:]))
    for step in (4, 2, 1):
        pair = pair_add(pair, (pltpu.roll(pair[0], step, 0), pltpu.roll(pair[1], step, 0)))
    pair = quick_sum(pair[0], pair[1] + pltpu.roll(pair[0], 64, 1))

    def entry(k):
        return tuple(jnp.broadcast_to(x[0:1, k : k + 1], (8, 128)) for x in pair)

    right = [entry(k) for k in range(MOMENTS)]
    ahead = list(right)
    steps, ratios = [], []
    for k in range(ITERS):
        step = pair_div(right[k], ahead[k + 1])
        steps.append(step[0])
        if k + 1 < ITERS:
            last = MOMENTS - 1 - k
            new = list(right)
            for m in range(k + 1, last):
                new[m] = pair_add(right[m], pair_neg(pair_mul(step, ahead[m + 1])))
            ratio = pair_neg(pair_mul(step, pair_div(new[k + 1], right[k])))
            for m in range(k + 1, last):
                ahead[m] = pair_add(new[m], pair_mul(ratio, ahead[m]))
            right = new
            ratios.append(ratio[0])
    weights = (inertia[...], east[...], south[...])
    left = forcing[...]
    heading = left
    total = None
    for k in range(ITERS):
        step = steps[k][0:1, 0:1]
        total = step * heading if total is None else total + step * heading
        left = left - step * apply_plain(heading, *weights)
        if k + 1 < ITERS:
            heading = left + ratios[k][0:1, 0:1] * heading
    field[...] = total[8 : 8 + rows, :cols]
    residual[...] = left[8 : 8 + rows, :cols]


def solve(sums, forcing, inertia, east, south, rows, cols):
    shape = jax.ShapeDtypeStruct((rows, cols), F32)
    return pl.pallas_call(
        solve_kernel,
        out_shape=(shape, shape),
        compiler_params=limit(16),
        in_specs=[vmem()] * 5,
        out_specs=(vmem(), vmem()),
        name="solve",
    )(*on_chip(sums, forcing, inertia, east, south))


def around(value, axis, steps):
    count = lax.axis_size(axis)
    return lax.ppermute(value, axis, [(i, (i + steps) % count) for i in range(count)])


def body(
    innovation,
    obs_error,
    obs_offset,
    obs_cell,
    obs_owner,
    block_count,
    land_mask,
    inertia,
    sea_depth,
):
    n_lat = lax.axis_size("lat")
    n_lon = lax.axis_size(LON)
    n_obs = lax.axis_size("obs")
    tiles = n_lat * n_lon
    rows, cols = land_mask.shape
    sent = pack(obs_owner, block_count, innovation, obs_error, obs_offset, obs_cell, tiles)
    arrived = lax.all_to_all(
        sent.reshape(tiles, CAP * WORDS, 1, 128), LAT_LON, split_axis=0, concat_axis=0, tiled=True
    ).reshape(tiles * CAP * WORDS, 128)

    conduct = land_mask.astype(F32) * sea_depth
    lane = lax.broadcasted_iota(jnp.int32, (1, 128), 1)
    stacked = jnp.stack([conduct, inertia])
    from_west = around(stacked[:, :, cols - 128 :], LON, 1)
    from_east = around(stacked[:, :, :128], LON, -1)
    wide = jnp.concatenate([stacked, jnp.where(lane < 64, from_east, from_west)], axis=2)
    above = around(wide[:, rows - 8 :], LAT_OBS, 1)
    below = around(wide[:, :8], LAT_OBS, -1)
    part = deposit(arrived, rows * n_obs, cols)
    part, above, below = lax.optimization_barrier((part, above, below))
    tile = part + around(part, "obs", 1)
    tile, above, below = lax.optimization_barrier((tile, above, below))
    conduct, inertia = jnp.concatenate([above, wide, below], axis=1)
    ocean = (conduct > 0.0).astype(F32)
    east = jnp.sqrt(conduct * jnp.roll(conduct, -1, 1))
    south = jnp.sqrt(conduct * jnp.roll(conduct, -1, 0))
    spill = tile[:, cols:]
    side = lax.axis_index("obs").astype(jnp.int32)
    leaving = jnp.where(
        side == 0, jnp.where(lane == 0, spill[:, :1], tile[:, cols - 128 : cols]), tile[:, :128]
    )
    split = []
    for i in range(n_lon):
        split.append((2 * i, 2 * ((i + 1) % n_lon)))
        split.append((2 * i + 1, 2 * ((i - 1) % n_lon) + 1))
    came = lax.ppermute(leaving, LON + ("obs",), split)
    swapped = around(came, "obs", 1)
    from_west = jnp.where(side == 0, came, swapped)
    from_east = jnp.where(side == 0, swapped, came)
    tile = jnp.concatenate(
        [
            tile[:, :128] + jnp.where(lane == 0, from_west, 0.0),
            tile[:, 128:cols],
            jnp.where(lane < 64, from_east, from_west) + spill,
        ],
        axis=1,
    )
    outer = jnp.where(side == 0, tile[:16], tile[2 * rows - 8 : 2 * rows + 8])
    swap = []
    for i in range(n_lat):
        swap.append((2 * i + 1, (2 * i + 2) % (2 * n_lat)))
        swap.append((2 * i, (2 * i - 1) % (2 * n_lat)))
    other = lax.ppermute(outer, LAT_OBS, swap)
    forcing, sums = basis(
        side.reshape(1), tile, other, ocean, inertia, east, south, tiles * n_obs
    )
    sums = lax.all_to_all(
        sums.reshape(tiles * n_obs, 1, 128), LAT_LON_OBS, split_axis=0, concat_axis=0, tiled=True
    ).reshape(tiles * n_obs, 128)
    return solve(sums, forcing, inertia, east, south, rows, cols)


def solution(mesh):
    split = Mesh(
        mesh.devices.reshape(mesh.shape["lat"], 4, 4, mesh.shape["obs"]),
        ("lat", "lon_0", "lon_1", "obs"),
    )
    return jax.shard_map(
        body,
        mesh=split,
        in_specs=(
            P(LAT_LON_OBS, None),
            P(LAT_LON_OBS, None),
            P(None, LAT_LON_OBS, None),
            P(LAT_LON_OBS, None),
            P(LAT_LON_OBS, None),
            P(LAT_LON_OBS),
            P(LAT_OBS, LON),
            P(LAT_OBS, LON),
            P(LAT_OBS, LON),
        ),
        out_specs=(P(LAT_OBS, LON), P(LAT_OBS, LON)),
        check_vma=False,
    )
```

```python
import jax
import jax.numpy as jnp
from jax import lax
from jax.experimental import pallas as pl
from jax.experimental.pallas import tpu as pltpu
from jax.sharding import Mesh
from jax.sharding import PartitionSpec as P

ITERS = 5
MOMENTS = 2 * ITERS
CAP = 3
WORDS = 4
LON = ("lon_0", "lon_1")
LAT_OBS = ("lat", "obs")
LAT_LON_OBS = ("lat", "lon_0", "lon_1", "obs")
LAT_LON = ("lat", "lon_0", "lon_1")
F32 = jnp.float32
BF16 = jnp.bfloat16
GROUPS = 4
WINDOW = 24
STEP = 16
RUN = 32


def vmem():
    return pl.BlockSpec(memory_space=pltpu.VMEM)


def smem():
    return pl.BlockSpec(memory_space=pltpu.SMEM)


def on_chip(*values):
    return [pltpu.with_memory_space_constraint(v, pltpu.MemorySpace.VMEM) for v in values]


def limit(mib):
    return pltpu.CompilerParams(vmem_limit_bytes=mib * 2**20)


def pack_kernel(owner, count, innovation, error, offset, cell, out, rows, seen):
    blocks = innovation.shape[0]
    tiles = out.shape[0] // (CAP * WORDS)
    err = error[...]
    rows[pl.ds(0, blocks, stride=WORDS), :] = innovation[...] / (err * err)
    rows[pl.ds(1, blocks, stride=WORDS), :] = offset[0]
    rows[pl.ds(2, blocks, stride=WORDS), :] = offset[1]
    rows[pl.ds(3, blocks, stride=WORDS), :] = cell[...].astype(F32)
    out[...] = jnp.zeros(out.shape, F32)

    def clear(tile, carry):
        seen[tile] = 0
        return carry

    lax.fori_loop(0, tiles, clear, 0, unroll=8)

    live_total = count[0]

    def place(block, carry):
        live = block < live_total
        tile = owner[0, block]
        rank = seen[tile]
        seen[tile] = rank + live.astype(jnp.int32)
        source = jnp.where(live, block, 0)
        slot = jnp.where(live, tile * CAP + rank, owner[0, 0] * CAP)
        out[pl.ds(slot * WORDS, WORDS), :] = rows[pl.ds(source * WORDS, WORDS), :]
        return carry

    lax.fori_loop(0, blocks, place, 0, unroll=8)


def pack(owner, count, innovation, error, offset, cell, tiles):
    blocks = innovation.shape[0]
    return pl.pallas_call(
        pack_kernel,
        out_shape=jax.ShapeDtypeStruct((tiles * CAP * WORDS, 128), F32),
        in_specs=[smem(), smem(), vmem(), vmem(), vmem(), vmem()],
        out_specs=vmem(),
        scratch_shapes=[pltpu.VMEM((blocks * WORDS, 128), F32), pltpu.SMEM((tiles,), jnp.int32)],
        name="pack",
    )(owner, count, innovation, error, offset, cell)


SORT_8 = (
    (0, 1), (2, 3), (4, 5), (6, 7), (0, 2), (1, 3), (4, 6), (5, 7), (1, 2), (5, 6),
    (0, 4), (1, 5), (2, 6), (3, 7), (2, 4), (3, 5), (1, 2), (3, 4), (5, 6),
)
CLEAN_8 = (
    (0, 4), (1, 5), (2, 6), (3, 7), (0, 2), (1, 3), (4, 6), (5, 7), (0, 1), (2, 3), (4, 5), (6, 7),
)


def quotient(x, n):
    return x >> (n.bit_length() - 1) if n & (n - 1) == 0 else x // n


def remainder(x, n):
    return x & (n - 1) if n & (n - 1) == 0 else x % n


def deposit(arrived, tile_rows, tile_cols):
    slots = arrived.shape[0] // WORDS
    width = tile_cols // GROUPS
    m_one = GROUPS * WINDOW
    m_all = 4 * m_one
    depth = tile_rows + WINDOW - 8
    filled = -(-slots // 8)
    regs = 8
    while regs < filled:
        regs *= 2
    total = -(-slots // 8)
    row_pad = (tile_rows + 1 + 7) // 8 * 8
    index_rows = max(m_one, width)
    middle = index_rows // 2
    last_cell = float(tile_rows * tile_cols - 1)
    parts = regs // RUN
    pairs = RUN // 2
    entries = total * (tile_rows // STEP + 1) + 8

    def kernel(src, out, held, left_a, left_b, right_a, right_b, acc, index, span_v, span_s, at, row_of, room, sem):
        index[...] = (lax.broadcasted_iota(jnp.int32, index.shape, 0) - middle).astype(F32).astype(BF16)
        acc[...] = jnp.zeros(acc.shape, F32)
        sub = lax.broadcasted_iota(jnp.int32, (8, 128), 0)

        def load(p):
            return [held[w, p] for w in range(WORDS)]

        def store(p, x):
            for w in range(WORDS):
                held[w, p] = x[w]

        def ordered(a, b):
            m = a[3] <= b[3]
            return (
                [jnp.where(m, x, y) for x, y in zip(a, b)],
                [jnp.where(m, y, x) for x, y in zip(a, b)],
            )

        def network(places, pairs):
            xs = [load(p) for p in places]
            for a, b in pairs:
                xs[a], xs[b] = ordered(xs[a], xs[b])
            for p, x in zip(places, xs):
                store(p, x)

        def first(g, carry):
            xs = []
            for i in range(8):
                base = pl.multiple_of((g * 8 + i) * 8 * WORDS, 8 * WORDS)
                xs.append([src[pl.ds(base + w, 8, stride=WORDS), :] for w in range(WORDS)])
            for a, b in SORT_8:
                xs[a], xs[b] = ordered(xs[a], xs[b])
            for i in range(8):
                store(g * 8 + i, xs[i])
            return carry

        lax.fori_loop(0, filled // 8, first, 0)
        for p in range(filled, regs):
            for w in range(WORDS):
                held[w, p] = jnp.full((8, 128), 1.0e9 if w == 3 else 0.0, F32)

        def near(g, carry):
            network([g * 8 + i for i in range(8)], CLEAN_8)
            return carry

        def several(pairs):
            for p, q in pairs:
                x, y = ordered(load(p), load(q))
                store(p, x)
                store(q, y)

        size = 16
        while size <= regs:
            h = size // 2
            several([(t // h * size + t % h, t // h * size + size - 1 - t % h) for t in range(regs // 2)])
            d = h // 2
            while d >= 8:
                several([(t // d * 2 * d + t % d, t // d * 2 * d + t % d + d) for t in range(regs // 2)])
                d //= 2
            lax.fori_loop(0, regs // 8, near, 0)
            size *= 2

        def turned(x, mask):
            return jnp.take_along_axis(x, sub ^ mask, axis=0, mode="promise_in_bounds")

        for k in range(3):
            mask = (2 << k) - 1
            low = (sub & (1 << k)) == 0
            for p in range(regs // 2):
                a = load(p)
                b = [turned(x, mask) for x in load(regs - 1 - p)]
                m = (a[3] <= b[3]) == low
                store(p, [jnp.where(m, x, y) for x, y in zip(a, b)])
                store(regs - 1 - p, [turned(jnp.where(m, y, x), mask) for x, y in zip(a, b)])
            for bit in range(k - 1, -1, -1):
                low_bit = (sub & (1 << bit)) == 0
                for p in range(regs):
                    a = load(p)
                    c = [turned(x, 1 << bit) for x in a]
                    m = jnp.where(low_bit, a[3], c[3]) <= jnp.where(low_bit, c[3], a[3])
                    store(p, [jnp.where(m, x, y) for x, y in zip(a, c)])
            d = regs // 2
            while d >= 8:
                if d == 32:

                    def far(g, carry):
                        network([g + 8 * i for i in range(8)], CLEAN_8)
                        return carry

                    lax.fori_loop(0, 8, far, 0)
                    d = 4
                else:
                    several([(t // d * 2 * d + t % d, t // d * 2 * d + t % d + d) for t in range(regs // 2)])
                    d //= 2
            lax.fori_loop(0, regs // 8, near, 0)

        lane = lax.broadcasted_iota(jnp.int32, (8, 128), 1)
        spans = jnp.zeros((8, 128), jnp.int32)
        for i in range(parts):
            low = jnp.min(jnp.minimum(held[3, RUN * i], last_cell), axis=1, keepdims=True)
            high = jnp.max(jnp.minimum(held[3, RUN * i + RUN - 1], last_cell), axis=1, keepdims=True)
            low = quotient(low.astype(jnp.int32), tile_cols)
            high = quotient(high.astype(jnp.int32), tile_cols)
            most = jnp.abs(held[0, RUN * i])
            for p in range(1, RUN):
                most = jnp.maximum(most, jnp.abs(held[0, RUN * i + p]))
            some = (jnp.max(most, axis=1, keepdims=True) > 0.0).astype(jnp.int32)
            spans = jnp.where(lane == i, low, jnp.where(lane == 64 + i, high, spans))
            spans = jnp.where(lane == 32 + i, some, spans)
        span_v[...] = spans
        copy = pltpu.make_async_copy(span_v, span_s, sem)
        copy.start()
        copy.wait()

        def plan(c, t):
            s = c // parts
            i = c % parts
            low = span_s[s, i]
            some = span_s[s, 32 + i]
            high = jnp.where(some > 0, span_s[s, 64 + i], low)

            def note(t, row, rows):
                at[t] = c
                row_of[t] = row
                room[t] = rows

            def further(x):
                note(x[1], x[0], STEP)
                return x[0] + STEP, x[1] + 1

            row, t = lax.while_loop(lambda x: high - x[0] >= WINDOW - 1, further, (low // 8 * 8, t))
            note(t, row, WINDOW - 1)
            return t + some

        count = lax.fori_loop(0, -(-slots // regs) * parts, plan, jnp.int32(0))
        for e in range(3):
            at[count + e] = 0
            row_of[count + e] = 0
            room[count + e] = 0

        def spread(x, j):
            pair = jnp.concatenate([x[2 * j : 2 * j + 1], x[2 * j + 1 : 2 * j + 2]], axis=1)
            return jnp.broadcast_to(pair, (16, 256)).astype(BF16)

        def build(t, left, right):
            c = at[t]
            s = c // parts
            i = c % parts
            amount, north, east, cell = [
                held[w, pl.ds(i * RUN, RUN), s, :] for w in range(WORDS)
            ]
            cell = cell.astype(jnp.int32)
            row = quotient(cell, tile_cols) - row_of[t]
            col = remainder(cell, tile_cols)
            inside = (row >= 0) & (row < room[t])
            place = quotient(col, width) * WINDOW + row - middle
            m_here = jnp.where(inside, place, 8 * index_rows).astype(F32)
            n_here = (remainder(col, width) - middle).astype(F32)
            pieces = []
            for value in (amount, amount * east):
                low = value * (1.0 - north)
                high = value * north
                low_top = low.astype(BF16).astype(F32)
                high_top = high.astype(BF16).astype(F32)
                pieces += [(low_top, high_top), (low - low_top, high - high_top)]
            zero = jnp.zeros((16, 256), BF16)
            one = jnp.ones((16, 256), BF16)
            for j in range(pairs):
                here = spread(m_here, j)
                after = here + one
                column = spread(n_here, j)
                values = [(spread(x, j), spread(y, j)) for x, y in pieces]
                for q in range(m_one // 16):
                    own = index[q * 16 : (q + 1) * 16]
                    at_row = jnp.where(own == here, one, zero)
                    at_next = jnp.where(own == after, one, zero)
                    for f, (low, high) in enumerate(values):
                        left[j, f * m_one + q * 16 : f * m_one + (q + 1) * 16] = (
                            at_row * low + at_next * high
                        )
                for q in range(width // 16):
                    right[j, q * 16 : (q + 1) * 16] = jnp.where(
                        index[q * 16 : (q + 1) * 16] == column, one, zero
                    )

        def joined(ref):
            return jnp.concatenate([ref[j] for j in range(pairs)], axis=1)

        def add(t, left, right):
            row = pl.multiple_of(row_of[t], 8)
            product = lax.dot_general(
                joined(left), joined(right), (((1,), (1,)), ((), ())), preferred_element_type=F32
            )
            for q in range(4 * GROUPS):
                acc[q, pl.ds(row, WINDOW), :] += product[q * WINDOW : (q + 1) * WINDOW]

        build(0, left_a, right_a)

        def turn(i, carry):
            build(2 * i + 1, left_b, right_b)
            add(2 * i, left_a, right_a)
            build(2 * i + 2, left_a, right_a)
            add(2 * i + 1, left_b, right_b)
            return carry

        lax.fori_loop(0, (count + 1) // 2, turn, 0)
        lane = lax.broadcasted_iota(jnp.int32, (row_pad, width), 1)
        before = jnp.zeros((row_pad, 1), F32)
        for g in range(GROUPS):
            whole = acc[g, 0:row_pad] + acc[GROUPS + g, 0:row_pad]
            part = acc[2 * GROUPS + g, 0:row_pad] + acc[3 * GROUPS + g, 0:row_pad]
            moved = pltpu.roll(part, 1, 1)
            moved = jnp.where(lane == 0, jnp.broadcast_to(before, (row_pad, width)), moved)
            out[:, g * width : (g + 1) * width] = whole - part + moved
            before = part[:, width - 1 : width]
        edge = lax.broadcasted_iota(jnp.int32, (row_pad, 128), 1)
        out[:, tile_cols : tile_cols + 128] = jnp.where(
            edge == 0, jnp.broadcast_to(before, (row_pad, 128)), 0.0
        )

    return pl.pallas_call(
        kernel,
        out_shape=pltpu.VMEM((row_pad, tile_cols + 128), F32),
        compiler_params=limit(32),
        in_specs=[vmem()],
        out_specs=vmem(),
        scratch_shapes=[
            pltpu.VMEM((WORDS, regs, 8, 128), F32),
            pltpu.VMEM((pairs, m_all, 256), BF16),
            pltpu.VMEM((pairs, m_all, 256), BF16),
            pltpu.VMEM((pairs, width, 256), BF16),
            pltpu.VMEM((pairs, width, 256), BF16),
            pltpu.VMEM((4 * GROUPS, depth, width), F32),
            pltpu.VMEM((index_rows, 256), BF16),
            pltpu.VMEM((8, 128), jnp.int32),
            pltpu.SMEM((8, 128), jnp.int32),
            pltpu.SMEM((entries,), jnp.int32),
            pltpu.SMEM((entries,), jnp.int32),
            pltpu.SMEM((entries,), jnp.int32),
            pltpu.SemaphoreType.DMA,
        ],
        name="deposit",
    )(*on_chip(arrived))


def two_sum(a, b):
    s = a + b
    t = s - a
    return s, (a - (s - t)) + (b - t)


def quick_sum(a, b):
    s = a + b
    return s, b - (s - a)


def halves(a):
    t = a * 4097.0
    top = t - (t - a)
    return top, a - top


def two_prod(a, b, a_halves, b_halves):
    p = a * b
    a1, a2 = a_halves
    b1, b2 = b_halves
    return p, ((a1 * b1 - p) + a1 * b2 + a2 * b1) + a2 * b2


def pair_add(a, b):
    s, e = two_sum(a[0], b[0])
    return quick_sum(s, e + (a[1] + b[1]))


def pair_mul(a, b):
    p, e = two_prod(a[0], b[0], halves(a[0]), halves(b[0]))
    return quick_sum(p, e + (a[0] * b[1] + a[1] * b[0]))


def pair_neg(a):
    return -a[0], -a[1]


def pair_div(a, b):
    q1 = a[0] / b[0]
    zero = jnp.zeros_like(q1)
    rest = pair_add(a, pair_neg(pair_mul((q1, zero), b)))
    q2 = rest[0] / b[0]
    rest = pair_add(rest, pair_neg(pair_mul((q2, zero), b)))
    q3 = rest[0] / b[0]
    s, e = quick_sum(q1, q2)
    return quick_sum(s, e + q3)


def roll_to(x, step, axis):
    return pltpu.roll(x, step % x.shape[axis], axis)


def apply_pair(v, inertia, east, south):
    h, l = v
    h_cut = halves(h)
    total, e = two_prod(inertia[0], h, inertia[1], h_cut)
    rest = e + inertia[0] * l
    for axis, (face, face_cut) in ((1, east), (0, south)):
        other = roll_to(h, -1, axis)
        d = h - other
        t = d - h
        err = (h - (d - t)) - (other + t)
        low = (l - roll_to(l, -1, axis)) + err
        p, e = two_prod(face, d, face_cut, halves(d))
        low = e + face * low
        total, e = two_sum(total, p)
        rest = rest + (e + low)
        total, e = two_sum(total, -roll_to(p, 1, axis))
        rest = rest + (e - roll_to(low, 1, axis))
    return quick_sum(total, rest)


def apply_plain(v, inertia, east, south):
    total = inertia * v
    for axis, face in ((1, east), (0, south)):
        flow = face * (v - roll_to(v, -1, axis))
        total = total + (flow - roll_to(flow, 1, axis))
    return total


def pair_fold(a):
    while a[0].shape[0] > 8:
        n = a[0].shape[0] // 2
        a = pair_add((a[0][:n], a[1][:n]), (a[0][n:], a[1][n:]))
    while a[0].shape[1] > 128:
        n = a[0].shape[1] // 2
        a = pair_add((a[0][:, :n], a[1][:, :n]), (a[0][:, n:], a[1][:, n:]))
    for step in (4, 2, 1):
        a = pair_add(a, (pltpu.roll(a[0], step, 0), pltpu.roll(a[1], step, 0)))
    return a


def basis_kernel(side, tile, other, ocean, inertia, east, south, forcing, sums):
    rows, cols = inertia.shape[0] - 16, inertia.shape[1] - 128
    first = side[0] == 0
    middle = tile[pl.ds(pl.multiple_of(side[0] * rows, 8), rows), :]
    corner = jnp.where(first, other[8:16, :], 0.0)
    top = jnp.where(first, other[0:8, :], tile[rows - 8 : rows, :])
    bottom = jnp.where(
        first, tile[rows : rows + 8, :], other[0:8, :] + tile[2 * rows : 2 * rows + 8, :]
    )
    start = jnp.concatenate([top, middle[0:8] + corner, middle[8:], bottom], axis=0) * ocean[...]
    forcing[...] = start
    weights = [(w[...], halves(w[...])) for w in (inertia, east, south)]
    vectors = [(start, jnp.zeros_like(start))]
    for k in range(ITERS):
        vectors.append(apply_pair(vectors[-1], *weights))
    inner = [(h[8 : 8 + rows, :cols], l[8 : 8 + rows, :cols]) for h, l in vectors]
    cuts = [halves(h) for h, l in inner]
    lane = lax.broadcasted_iota(jnp.int32, (8, 128), 1)
    tops, lows = [], []
    for k in range(MOMENTS):
        i, j = k // 2, (k + 1) // 2
        a, b = inner[i], inner[j]
        p, e = two_prod(a[0], b[0], cuts[i], cuts[j])
        total = pair_fold((p, e + (a[0] * b[1] + a[1] * b[0])))
        tops.append(total[0][0:1])
        lows.append(total[1][0:1])
    blank = [jnp.zeros((16 - MOMENTS, 128), F32)]
    pair = (jnp.concatenate(tops + blank, 0), jnp.concatenate(lows + blank, 0))
    for step in (64, 32, 16, 8, 4, 2, 1):
        pair = pair_add(pair, (pltpu.roll(pair[0], step, 1), pltpu.roll(pair[1], step, 1)))
    lane = lax.broadcasted_iota(jnp.int32, (16, 128), 1)
    slot = lax.broadcasted_iota(jnp.int32, (16, 128), 0)
    row = jnp.sum(
        jnp.where(lane == slot, pair[0], jnp.where(lane == slot + 64, pair[1], 0.0)),
        axis=0,
        keepdims=True,
    )
    sums[...] = jnp.broadcast_to(row, sums.shape)


def basis(side, tile, other, ocean, inertia, east, south, devices):
    return pl.pallas_call(
        basis_kernel,
        out_shape=(
            pltpu.VMEM(inertia.shape, F32),
            pltpu.VMEM((devices, 128), F32),
        ),
        compiler_params=limit(24),
        in_specs=[smem()] + [vmem()] * 6,
        out_specs=(vmem(), vmem()),
        name="basis",
    )(side, *on_chip(tile, other, ocean, inertia, east, south))


def solve_kernel(sums, forcing, inertia, east, south, field, residual):
    rows, cols = field.shape
    s = sums[...]
    pair = (s, jnp.zeros_like(s))
    while pair[0].shape[0] > 8:
        n = pair[0].shape[0] // 2
        pair = pair_add((pair[0][:n], pair[1][:n]), (pair[0][n:], pair[1][n:]))
    for step in (4, 2, 1):
        pair = pair_add(pair, (pltpu.roll(pair[0], step, 0), pltpu.roll(pair[1], step, 0)))
    pair = quick_sum(pair[0], pair[1] + pltpu.roll(pair[0], 64, 1))

    def entry(k):
        return tuple(jnp.broadcast_to(x[0:1, k : k + 1], (8, 128)) for x in pair)

    right = [entry(k) for k in range(MOMENTS)]
    ahead = list(right)
    steps, ratios = [], []
    for k in range(ITERS):
        step = pair_div(right[k], ahead[k + 1])
        steps.append(step[0])
        if k + 1 < ITERS:
            last = MOMENTS - 1 - k
            new = list(right)
            for m in range(k + 1, last):
                new[m] = pair_add(right[m], pair_neg(pair_mul(step, ahead[m + 1])))
            ratio = pair_neg(pair_mul(step, pair_div(new[k + 1], right[k])))
            for m in range(k + 1, last):
                ahead[m] = pair_add(new[m], pair_mul(ratio, ahead[m]))
            right = new
            ratios.append(ratio[0])
    weights = (inertia[...], east[...], south[...])
    left = forcing[...]
    heading = left
    total = None
    for k in range(ITERS):
        step = steps[k][0:1, 0:1]
        total = step * heading if total is None else total + step * heading
        left = left - step * apply_plain(heading, *weights)
        if k + 1 < ITERS:
            heading = left + ratios[k][0:1, 0:1] * heading
    field[...] = total[8 : 8 + rows, :cols]
    residual[...] = left[8 : 8 + rows, :cols]


def solve(sums, forcing, inertia, east, south, rows, cols):
    shape = jax.ShapeDtypeStruct((rows, cols), F32)
    return pl.pallas_call(
        solve_kernel,
        out_shape=(shape, shape),
        compiler_params=limit(16),
        in_specs=[vmem()] * 5,
        out_specs=(vmem(), vmem()),
        name="solve",
    )(*on_chip(sums, forcing, inertia, east, south))


def around(value, axis, steps):
    count = lax.axis_size(axis)
    return lax.ppermute(value, axis, [(i, (i + steps) % count) for i in range(count)])


def body(
    innovation,
    obs_error,
    obs_offset,
    obs_cell,
    obs_owner,
    block_count,
    land_mask,
    inertia,
    sea_depth,
):
    n_lat = lax.axis_size("lat")
    n_lon = lax.axis_size(LON)
    n_obs = lax.axis_size("obs")
    tiles = n_lat * n_lon
    rows, cols = land_mask.shape
    sent = pack(obs_owner, block_count, innovation, obs_error, obs_offset, obs_cell, tiles)
    arrived = lax.all_to_all(
        sent.reshape(tiles, CAP * WORDS, 1, 128), LAT_LON, split_axis=0, concat_axis=0, tiled=True
    ).reshape(tiles * CAP * WORDS, 128)

    conduct = land_mask.astype(F32) * sea_depth
    lane = lax.broadcasted_iota(jnp.int32, (1, 128), 1)
    stacked = jnp.stack([conduct, inertia])
    from_west = around(stacked[:, :, cols - 128 :], LON, 1)
    from_east = around(stacked[:, :, :128], LON, -1)
    wide = jnp.concatenate([stacked, jnp.where(lane < 64, from_east, from_west)], axis=2)
    above = around(wide[:, rows - 8 :], LAT_OBS, 1)
    below = around(wide[:, :8], LAT_OBS, -1)
    part = deposit(arrived, rows * n_obs, cols)
    part, above, below = lax.optimization_barrier((part, above, below))
    tile = part + around(part, "obs", 1)
    tile, above, below = lax.optimization_barrier((tile, above, below))
    conduct, inertia = jnp.concatenate([above, wide, below], axis=1)
    ocean = (conduct > 0.0).astype(F32)
    east = jnp.sqrt(conduct * jnp.roll(conduct, -1, 1))
    south = jnp.sqrt(conduct * jnp.roll(conduct, -1, 0))
    spill = tile[:, cols:]
    side = lax.axis_index("obs").astype(jnp.int32)
    leaving = jnp.where(
        side == 0, jnp.where(lane == 0, spill[:, :1], tile[:, cols - 128 : cols]), tile[:, :128]
    )
    split = []
    for i in range(n_lon):
        split.append((2 * i, 2 * ((i + 1) % n_lon)))
        split.append((2 * i + 1, 2 * ((i - 1) % n_lon) + 1))
    came = lax.ppermute(leaving, LON + ("obs",), split)
    swapped = around(came, "obs", 1)
    from_west = jnp.where(side == 0, came, swapped)
    from_east = jnp.where(side == 0, swapped, came)
    tile = jnp.concatenate(
        [
            tile[:, :128] + jnp.where(lane == 0, from_west, 0.0),
            tile[:, 128:cols],
            jnp.where(lane < 64, from_east, from_west) + spill,
        ],
        axis=1,
    )
    outer = jnp.where(side == 0, tile[:16], tile[2 * rows - 8 : 2 * rows + 8])
    swap = []
    for i in range(n_lat):
        swap.append((2 * i + 1, (2 * i + 2) % (2 * n_lat)))
        swap.append((2 * i, (2 * i - 1) % (2 * n_lat)))
    other = lax.ppermute(outer, LAT_OBS, swap)
    forcing, sums = basis(
        side.reshape(1), tile, other, ocean, inertia, east, south, tiles * n_obs
    )
    sums = lax.all_to_all(
        sums.reshape(tiles * n_obs, 1, 128), LAT_LON_OBS, split_axis=0, concat_axis=0, tiled=True
    ).reshape(tiles * n_obs, 128)
    return solve(sums, forcing, inertia, east, south, rows, cols)


def solution(mesh):
    split = Mesh(
        mesh.devices.reshape(mesh.shape["lat"], 4, 4, mesh.shape["obs"]),
        ("lat", "lon_0", "lon_1", "obs"),
    )
    return jax.shard_map(
        body,
        mesh=split,
        in_specs=(
            P(LAT_LON_OBS, None),
            P(LAT_LON_OBS, None),
            P(None, LAT_LON_OBS, None),
            P(LAT_LON_OBS, None),
            P(LAT_LON_OBS, None),
            P(LAT_LON_OBS),
            P(LAT_OBS, LON),
            P(LAT_OBS, LON),
            P(LAT_OBS, LON),
        ),
        out_specs=(P(LAT_OBS, LON), P(LAT_OBS, LON)),
        check_vma=False,
    )
```

```python
import jax
import jax.numpy as jnp
from jax import lax
from jax.experimental import pallas as pl
from jax.experimental.pallas import tpu as pltpu
from jax.sharding import Mesh
from jax.sharding import PartitionSpec as P

ITERS = 5
MOMENTS = 2 * ITERS
CAP = 3
WORDS = 4
LON = ("lon_0", "lon_1")
LAT_OBS = ("lat", "obs")
LAT_LON_OBS = ("lat", "lon_0", "lon_1", "obs")
LAT_LON = ("lat", "lon_0", "lon_1")
F32 = jnp.float32
BF16 = jnp.bfloat16
GROUPS = 4
WINDOW = 24
STEP = 16
RUN = 32


def vmem():
    return pl.BlockSpec(memory_space=pltpu.VMEM)


def smem():
    return pl.BlockSpec(memory_space=pltpu.SMEM)


def on_chip(*values):
    return [pltpu.with_memory_space_constraint(v, pltpu.MemorySpace.VMEM) for v in values]


def limit(mib):
    return pltpu.CompilerParams(vmem_limit_bytes=mib * 2**20)


def pack_kernel(owner, count, innovation, error, offset, cell, out, rows, seen):
    blocks = innovation.shape[0]
    tiles = out.shape[0] // (CAP * WORDS)
    err = error[...]
    rows[pl.ds(0, blocks, stride=WORDS), :] = innovation[...] / (err * err)
    rows[pl.ds(1, blocks, stride=WORDS), :] = offset[0]
    rows[pl.ds(2, blocks, stride=WORDS), :] = offset[1]
    rows[pl.ds(3, blocks, stride=WORDS), :] = cell[...].astype(F32)
    out[...] = jnp.zeros(out.shape, F32)

    def clear(tile, carry):
        seen[tile] = 0
        return carry

    lax.fori_loop(0, tiles, clear, 0, unroll=8)

    live_total = count[0]

    def place(block, carry):
        live = block < live_total
        tile = owner[0, block]
        rank = seen[tile]
        seen[tile] = rank + live.astype(jnp.int32)
        source = jnp.where(live, block, 0)
        slot = jnp.where(live, tile * CAP + rank, owner[0, 0] * CAP)
        out[pl.ds(slot * WORDS, WORDS), :] = rows[pl.ds(source * WORDS, WORDS), :]
        return carry

    lax.fori_loop(0, blocks, place, 0, unroll=8)


def pack(owner, count, innovation, error, offset, cell, tiles):
    blocks = innovation.shape[0]
    return pl.pallas_call(
        pack_kernel,
        out_shape=jax.ShapeDtypeStruct((tiles * CAP * WORDS, 128), F32),
        in_specs=[smem(), smem(), vmem(), vmem(), vmem(), vmem()],
        out_specs=vmem(),
        scratch_shapes=[pltpu.VMEM((blocks * WORDS, 128), F32), pltpu.SMEM((tiles,), jnp.int32)],
        name="pack",
    )(owner, count, innovation, error, offset, cell)


SORT_8 = (
    (0, 1), (2, 3), (4, 5), (6, 7), (0, 2), (1, 3), (4, 6), (5, 7), (1, 2), (5, 6),
    (0, 4), (1, 5), (2, 6), (3, 7), (2, 4), (3, 5), (1, 2), (3, 4), (5, 6),
)
CLEAN_8 = (
    (0, 4), (1, 5), (2, 6), (3, 7), (0, 2), (1, 3), (4, 6), (5, 7), (0, 1), (2, 3), (4, 5), (6, 7),
)


def quotient(x, n):
    return x >> (n.bit_length() - 1) if n & (n - 1) == 0 else x // n


def remainder(x, n):
    return x & (n - 1) if n & (n - 1) == 0 else x % n


def deposit(arrived, tile_rows, tile_cols):
    slots = arrived.shape[0] // WORDS
    width = tile_cols // GROUPS
    m_one = GROUPS * WINDOW
    m_all = 4 * m_one
    depth = tile_rows + WINDOW - 8
    filled = -(-slots // 8)
    regs = 8
    while regs < filled:
        regs *= 2
    total = -(-slots // 8)
    row_pad = (tile_rows + 1 + 7) // 8 * 8
    index_rows = max(m_one, width)
    middle = index_rows // 2
    last_cell = float(tile_rows * tile_cols - 1)
    parts = regs // RUN
    pairs = RUN // 2
    entries = total * (tile_rows // STEP + 1) + 8

    def kernel(src, out, held, left_a, left_b, right_a, right_b, acc, index, span_v, span_s, at, row_of, room, sem):
        index[...] = (lax.broadcasted_iota(jnp.int32, index.shape, 0) - middle).astype(F32).astype(BF16)
        acc[...] = jnp.zeros(acc.shape, F32)
        sub = lax.broadcasted_iota(jnp.int32, (8, 128), 0)

        def load(p):
            return [held[w, p] for w in range(WORDS)]

        def store(p, x):
            for w in range(WORDS):
                held[w, p] = x[w]

        def ordered(a, b):
            m = a[3] <= b[3]
            return (
                [jnp.where(m, x, y) for x, y in zip(a, b)],
                [jnp.where(m, y, x) for x, y in zip(a, b)],
            )

        def network(places, pairs):
            xs = [load(p) for p in places]
            for a, b in pairs:
                xs[a], xs[b] = ordered(xs[a], xs[b])
            for p, x in zip(places, xs):
                store(p, x)

        def first(g, carry):
            xs = []
            for i in range(8):
                base = pl.multiple_of((g * 8 + i) * 8 * WORDS, 8 * WORDS)
                xs.append([src[pl.ds(base + w, 8, stride=WORDS), :] for w in range(WORDS)])
            for a, b in SORT_8:
                xs[a], xs[b] = ordered(xs[a], xs[b])
            for i in range(8):
                store(g * 8 + i, xs[i])
            return carry

        lax.fori_loop(0, filled // 8, first, 0)
        for p in range(filled, regs):
            for w in range(WORDS):
                held[w, p] = jnp.full((8, 128), 1.0e9 if w == 3 else 0.0, F32)

        def near(g, carry):
            network([g * 8 + i for i in range(8)], CLEAN_8)
            return carry

        def several(pairs):
            for p, q in pairs:
                x, y = ordered(load(p), load(q))
                store(p, x)
                store(q, y)

        size = 16
        while size <= regs:
            h = size // 2
            several([(t // h * size + t % h, t // h * size + size - 1 - t % h) for t in range(regs // 2)])
            d = h // 2
            while d >= 8:
                several([(t // d * 2 * d + t % d, t // d * 2 * d + t % d + d) for t in range(regs // 2)])
                d //= 2
            lax.fori_loop(0, regs // 8, near, 0)
            size *= 2

        def turned(x, mask):
            return jnp.take_along_axis(x, sub ^ mask, axis=0, mode="promise_in_bounds")

        for k in range(3):
            mask = (2 << k) - 1
            low = (sub & (1 << k)) == 0
            for p in range(regs // 2):
                a = load(p)
                b = [turned(x, mask) for x in load(regs - 1 - p)]
                m = (a[3] <= b[3]) == low
                store(p, [jnp.where(m, x, y) for x, y in zip(a, b)])
                store(regs - 1 - p, [turned(jnp.where(m, y, x), mask) for x, y in zip(a, b)])
            for bit in range(k - 1, -1, -1):
                low_bit = (sub & (1 << bit)) == 0
                for p in range(regs):
                    a = load(p)
                    c = [turned(x, 1 << bit) for x in a]
                    m = jnp.where(low_bit, a[3], c[3]) <= jnp.where(low_bit, c[3], a[3])
                    store(p, [jnp.where(m, x, y) for x, y in zip(a, c)])
            d = regs // 2
            while d >= 8:
                if d == 32:

                    def far(g, carry):
                        network([g + 8 * i for i in range(8)], CLEAN_8)
                        return carry

                    lax.fori_loop(0, 8, far, 0)
                    d = 4
                else:
                    several([(t // d * 2 * d + t % d, t // d * 2 * d + t % d + d) for t in range(regs // 2)])
                    d //= 2
            lax.fori_loop(0, regs // 8, near, 0)

        lane = lax.broadcasted_iota(jnp.int32, (8, 128), 1)
        spans = jnp.zeros((8, 128), jnp.int32)
        for i in range(parts):
            low = jnp.min(jnp.minimum(held[3, RUN * i], last_cell), axis=1, keepdims=True)
            high = jnp.max(jnp.minimum(held[3, RUN * i + RUN - 1], last_cell), axis=1, keepdims=True)
            low = quotient(low.astype(jnp.int32), tile_cols)
            high = quotient(high.astype(jnp.int32), tile_cols)
            most = jnp.abs(held[0, RUN * i])
            for p in range(1, RUN):
                most = jnp.maximum(most, jnp.abs(held[0, RUN * i + p]))
            some = (jnp.max(most, axis=1, keepdims=True) > 0.0).astype(jnp.int32)
            spans = jnp.where(lane == i, low, jnp.where(lane == 64 + i, high, spans))
            spans = jnp.where(lane == 32 + i, some, spans)
        span_v[...] = spans
        copy = pltpu.make_async_copy(span_v, span_s, sem)
        copy.start()
        copy.wait()

        def plan(c, t):
            s = c // parts
            i = c % parts
            low = span_s[s, i]
            some = span_s[s, 32 + i]
            high = jnp.where(some > 0, span_s[s, 64 + i], low)

            def note(t, row, rows):
                at[t] = c
                row_of[t] = row
                room[t] = rows

            def further(x):
                note(x[1], x[0], STEP)
                return x[0] + STEP, x[1] + 1

            row, t = lax.while_loop(lambda x: high - x[0] >= WINDOW - 1, further, (low // 8 * 8, t))
            note(t, row, WINDOW - 1)
            return t + some

        count = lax.fori_loop(0, -(-slots // regs) * parts, plan, jnp.int32(0))
        for e in range(3):
            at[count + e] = 0
            row_of[count + e] = 0
            room[count + e] = 0

        def spread(x, j):
            pair = jnp.concatenate([x[2 * j : 2 * j + 1], x[2 * j + 1 : 2 * j + 2]], axis=1)
            return jnp.broadcast_to(pair, (16, 256)).astype(BF16)

        def build(t, left, right):
            c = at[t]
            s = c // parts
            i = c % parts
            amount, north, east, cell = [
                held[w, pl.ds(i * RUN, RUN), s, :] for w in range(WORDS)
            ]
            cell = cell.astype(jnp.int32)
            row = quotient(cell, tile_cols) - row_of[t]
            col = remainder(cell, tile_cols)
            inside = (row >= 0) & (row < room[t])
            place = quotient(col, width) * WINDOW + row - middle
            m_here = jnp.where(inside, place, 8 * index_rows).astype(F32)
            n_here = (remainder(col, width) - middle).astype(F32)
            pieces = []
            for value in (amount, amount * east):
                low = value * (1.0 - north)
                high = value * north
                low_top = low.astype(BF16).astype(F32)
                high_top = high.astype(BF16).astype(F32)
                pieces += [(low_top, high_top), (low - low_top, high - high_top)]
            zero = jnp.zeros((16, 256), BF16)
            one = jnp.ones((16, 256), BF16)
            for j in range(pairs):
                here = spread(m_here, j)
                after = here + one
                column = spread(n_here, j)
                values = [(spread(x, j), spread(y, j)) for x, y in pieces]
                for q in range(m_one // 16):
                    own = index[q * 16 : (q + 1) * 16]
                    at_row = jnp.where(own == here, one, zero)
                    at_next = jnp.where(own == after, one, zero)
                    for f, (low, high) in enumerate(values):
                        left[j, f * m_one + q * 16 : f * m_one + (q + 1) * 16] = (
                            at_row * low + at_next * high
                        )
                for q in range(width // 16):
                    right[j, q * 16 : (q + 1) * 16] = jnp.where(
                        index[q * 16 : (q + 1) * 16] == column, one, zero
                    )

        def joined(ref):
            return jnp.concatenate([ref[j] for j in range(pairs)], axis=1)

        def add(t, left, right):
            row = pl.multiple_of(row_of[t], 8)
            product = lax.dot_general(
                joined(left), joined(right), (((1,), (1,)), ((), ())), preferred_element_type=F32
            )
            for q in range(4 * GROUPS):
                acc[q, pl.ds(row, WINDOW), :] += product[q * WINDOW : (q + 1) * WINDOW]

        build(0, left_a, right_a)

        def turn(i, carry):
            build(2 * i + 1, left_b, right_b)
            add(2 * i, left_a, right_a)
            build(2 * i + 2, left_a, right_a)
            add(2 * i + 1, left_b, right_b)
            return carry

        lax.fori_loop(0, (count + 1) // 2, turn, 0)
        lane = lax.broadcasted_iota(jnp.int32, (row_pad, width), 1)
        before = jnp.zeros((row_pad, 1), F32)
        for g in range(GROUPS):
            whole = acc[g, 0:row_pad] + acc[GROUPS + g, 0:row_pad]
            part = acc[2 * GROUPS + g, 0:row_pad] + acc[3 * GROUPS + g, 0:row_pad]
            moved = pltpu.roll(part, 1, 1)
            moved = jnp.where(lane == 0, jnp.broadcast_to(before, (row_pad, width)), moved)
            out[:, g * width : (g + 1) * width] = whole - part + moved
            before = part[:, width - 1 : width]
        edge = lax.broadcasted_iota(jnp.int32, (row_pad, 128), 1)
        out[:, tile_cols : tile_cols + 128] = jnp.where(
            edge == 0, jnp.broadcast_to(before, (row_pad, 128)), 0.0
        )

    return pl.pallas_call(
        kernel,
        out_shape=pltpu.VMEM((row_pad, tile_cols + 128), F32),
        compiler_params=limit(32),
        in_specs=[vmem()],
        out_specs=vmem(),
        scratch_shapes=[
            pltpu.VMEM((WORDS, regs, 8, 128), F32),
            pltpu.VMEM((pairs, m_all, 256), BF16),
            pltpu.VMEM((pairs, m_all, 256), BF16),
            pltpu.VMEM((pairs, width, 256), BF16),
            pltpu.VMEM((pairs, width, 256), BF16),
            pltpu.VMEM((4 * GROUPS, depth, width), F32),
            pltpu.VMEM((index_rows, 256), BF16),
            pltpu.VMEM((8, 128), jnp.int32),
            pltpu.SMEM((8, 128), jnp.int32),
            pltpu.SMEM((entries,), jnp.int32),
            pltpu.SMEM((entries,), jnp.int32),
            pltpu.SMEM((entries,), jnp.int32),
            pltpu.SemaphoreType.DMA,
        ],
        name="deposit",
    )(*on_chip(arrived))


def two_sum(a, b):
    s = a + b
    t = s - a
    return s, (a - (s - t)) + (b - t)


def quick_sum(a, b):
    s = a + b
    return s, b - (s - a)


def halves(a):
    t = a * 4097.0
    top = t - (t - a)
    return top, a - top


def two_prod(a, b, a_halves, b_halves):
    p = a * b
    a1, a2 = a_halves
    b1, b2 = b_halves
    return p, ((a1 * b1 - p) + a1 * b2 + a2 * b1) + a2 * b2


def pair_add(a, b):
    s, e = two_sum(a[0], b[0])
    return quick_sum(s, e + (a[1] + b[1]))


def pair_mul(a, b):
    p, e = two_prod(a[0], b[0], halves(a[0]), halves(b[0]))
    return quick_sum(p, e + (a[0] * b[1] + a[1] * b[0]))


def pair_neg(a):
    return -a[0], -a[1]


def pair_div(a, b):
    q1 = a[0] / b[0]
    zero = jnp.zeros_like(q1)
    rest = pair_add(a, pair_neg(pair_mul((q1, zero), b)))
    q2 = rest[0] / b[0]
    rest = pair_add(rest, pair_neg(pair_mul((q2, zero), b)))
    q3 = rest[0] / b[0]
    s, e = quick_sum(q1, q2)
    return quick_sum(s, e + q3)


def roll_to(x, step, axis):
    return pltpu.roll(x, step % x.shape[axis], axis)


def apply_pair(v, inertia, east, south):
    h, l = v
    h_cut = halves(h)
    total, e = two_prod(inertia[0], h, inertia[1], h_cut)
    rest = e + inertia[0] * l
    for axis, (face, face_cut) in ((1, east), (0, south)):
        other = roll_to(h, -1, axis)
        d = h - other
        t = d - h
        err = (h - (d - t)) - (other + t)
        low = (l - roll_to(l, -1, axis)) + err
        p, e = two_prod(face, d, face_cut, halves(d))
        low = e + face * low
        total, e = two_sum(total, p)
        rest = rest + (e + low)
        total, e = two_sum(total, -roll_to(p, 1, axis))
        rest = rest + (e - roll_to(low, 1, axis))
    return quick_sum(total, rest)


def apply_plain(v, inertia, east, south):
    total = inertia * v
    for axis, face in ((1, east), (0, south)):
        flow = face * (v - roll_to(v, -1, axis))
        total = total + (flow - roll_to(flow, 1, axis))
    return total


def pair_fold(a):
    while a[0].shape[0] > 8:
        n = a[0].shape[0] // 2
        a = pair_add((a[0][:n], a[1][:n]), (a[0][n:], a[1][n:]))
    while a[0].shape[1] > 128:
        n = a[0].shape[1] // 2
        a = pair_add((a[0][:, :n], a[1][:, :n]), (a[0][:, n:], a[1][:, n:]))
    for step in (4, 2, 1):
        a = pair_add(a, (pltpu.roll(a[0], step, 0), pltpu.roll(a[1], step, 0)))
    return a


def basis_kernel(side, tile, other, ocean, inertia, east, south, forcing, sums):
    rows, cols = inertia.shape[0] - 16, inertia.shape[1] - 128
    first = side[0] == 0
    middle = tile[pl.ds(pl.multiple_of(side[0] * rows, 8), rows), :]
    corner = jnp.where(first, other[8:16, :], 0.0)
    top = jnp.where(first, other[0:8, :], tile[rows - 8 : rows, :])
    bottom = jnp.where(
        first, tile[rows : rows + 8, :], other[0:8, :] + tile[2 * rows : 2 * rows + 8, :]
    )
    start = jnp.concatenate([top, middle[0:8] + corner, middle[8:], bottom], axis=0) * ocean[...]
    forcing[...] = start
    weights = [(w[...], halves(w[...])) for w in (inertia, east, south)]
    vectors = [(start, jnp.zeros_like(start))]
    for k in range(ITERS):
        vectors.append(apply_pair(vectors[-1], *weights))
    inner = [(h[8 : 8 + rows, :cols], l[8 : 8 + rows, :cols]) for h, l in vectors]
    cuts = [halves(h) for h, l in inner]
    lane = lax.broadcasted_iota(jnp.int32, (8, 128), 1)
    tops, lows = [], []
    for k in range(MOMENTS):
        i, j = k // 2, (k + 1) // 2
        a, b = inner[i], inner[j]
        p, e = two_prod(a[0], b[0], cuts[i], cuts[j])
        total = pair_fold((p, e + (a[0] * b[1] + a[1] * b[0])))
        tops.append(total[0][0:1])
        lows.append(total[1][0:1])
    blank = [jnp.zeros((16 - MOMENTS, 128), F32)]
    pair = (jnp.concatenate(tops + blank, 0), jnp.concatenate(lows + blank, 0))
    for step in (64, 32, 16, 8, 4, 2, 1):
        pair = pair_add(pair, (pltpu.roll(pair[0], step, 1), pltpu.roll(pair[1], step, 1)))
    lane = lax.broadcasted_iota(jnp.int32, (16, 128), 1)
    slot = lax.broadcasted_iota(jnp.int32, (16, 128), 0)
    row = jnp.sum(
        jnp.where(lane == slot, pair[0], jnp.where(lane == slot + 64, pair[1], 0.0)),
        axis=0,
        keepdims=True,
    )
    sums[...] = jnp.broadcast_to(row, sums.shape)


def basis(side, tile, other, ocean, inertia, east, south, devices):
    return pl.pallas_call(
        basis_kernel,
        out_shape=(
            pltpu.VMEM(inertia.shape, F32),
            pltpu.VMEM((devices, 128), F32),
        ),
        compiler_params=limit(24),
        in_specs=[smem()] + [vmem()] * 6,
        out_specs=(vmem(), vmem()),
        name="basis",
    )(side, *on_chip(tile, other, ocean, inertia, east, south))


def solve_kernel(sums, forcing, inertia, east, south, field, residual):
    rows, cols = field.shape
    s = sums[...]
    pair = (s, jnp.zeros_like(s))
    while pair[0].shape[0] > 8:
        n = pair[0].shape[0] // 2
        pair = pair_add((pair[0][:n], pair[1][:n]), (pair[0][n:], pair[1][n:]))
    for step in (4, 2, 1):
        pair = pair_add(pair, (pltpu.roll(pair[0], step, 0), pltpu.roll(pair[1], step, 0)))
    pair = quick_sum(pair[0], pair[1] + pltpu.roll(pair[0], 64, 1))

    def entry(k):
        return tuple(jnp.broadcast_to(x[0:1, k : k + 1], (8, 128)) for x in pair)

    right = [entry(k) for k in range(MOMENTS)]
    ahead = list(right)
    steps, ratios = [], []
    for k in range(ITERS):
        step = pair_div(right[k], ahead[k + 1])
        steps.append(step[0])
        if k + 1 < ITERS:
            last = MOMENTS - 1 - k
            new = list(right)
            for m in range(k + 1, last):
                new[m] = pair_add(right[m], pair_neg(pair_mul(step, ahead[m + 1])))
            ratio = pair_neg(pair_mul(step, pair_div(new[k + 1], right[k])))
            for m in range(k + 1, last):
                ahead[m] = pair_add(new[m], pair_mul(ratio, ahead[m]))
            right = new
            ratios.append(ratio[0])
    weights = (inertia[...], east[...], south[...])
    left = forcing[...]
    heading = left
    total = None
    for k in range(ITERS):
        step = steps[k][0:1, 0:1]
        total = step * heading if total is None else total + step * heading
        left = left - step * apply_plain(heading, *weights)
        if k + 1 < ITERS:
            heading = left + ratios[k][0:1, 0:1] * heading
    field[...] = total[8 : 8 + rows, :cols]
    residual[...] = left[8 : 8 + rows, :cols]


def solve(sums, forcing, inertia, east, south, rows, cols):
    shape = jax.ShapeDtypeStruct((rows, cols), F32)
    return pl.pallas_call(
        solve_kernel,
        out_shape=(shape, shape),
        compiler_params=limit(16),
        in_specs=[vmem()] * 5,
        out_specs=(vmem(), vmem()),
        name="solve",
    )(*on_chip(sums, forcing, inertia, east, south))


def around(value, axis, steps):
    count = lax.axis_size(axis)
    return lax.ppermute(value, axis, [(i, (i + steps) % count) for i in range(count)])


def body(
    innovation,
    obs_error,
    obs_offset,
    obs_cell,
    obs_owner,
    block_count,
    land_mask,
    inertia,
    sea_depth,
):
    n_lat = lax.axis_size("lat")
    n_lon = lax.axis_size(LON)
    n_obs = lax.axis_size("obs")
    tiles = n_lat * n_lon
    rows, cols = land_mask.shape
    sent = pack(obs_owner, block_count, innovation, obs_error, obs_offset, obs_cell, tiles)
    arrived = lax.all_to_all(
        sent.reshape(tiles, CAP * WORDS, 1, 128), LAT_LON, split_axis=0, concat_axis=0, tiled=True
    ).reshape(tiles * CAP * WORDS, 128)

    conduct = land_mask.astype(F32) * sea_depth
    lane = lax.broadcasted_iota(jnp.int32, (1, 128), 1)
    stacked = jnp.stack([conduct, inertia])
    from_west = around(stacked[:, :, cols - 128 :], LON, 1)
    from_east = around(stacked[:, :, :128], LON, -1)
    wide = jnp.concatenate([stacked, jnp.where(lane < 64, from_east, from_west)], axis=2)
    above = around(wide[:, rows - 8 :], LAT_OBS, 1)
    below = around(wide[:, :8], LAT_OBS, -1)
    part = deposit(arrived, rows * n_obs, cols)
    part, above, below = lax.optimization_barrier((part, above, below))
    tile = part + around(part, "obs", 1)
    tile, above, below = lax.optimization_barrier((tile, above, below))
    conduct, inertia = jnp.concatenate([above, wide, below], axis=1)
    ocean = (conduct > 0.0).astype(F32)
    east = jnp.sqrt(conduct * jnp.roll(conduct, -1, 1))
    south = jnp.sqrt(conduct * jnp.roll(conduct, -1, 0))
    spill = tile[:, cols:]
    side = lax.axis_index("obs").astype(jnp.int32)
    from_west = around(jnp.where(lane == 0, spill[:, :1], tile[:, cols - 128 : cols]), LON, 1)
    from_east = around(tile[:, :128], LON, -1)
    tile = jnp.concatenate(
        [
            tile[:, :128] + jnp.where(lane == 0, from_west, 0.0),
            tile[:, 128:cols],
            jnp.where(lane < 64, from_east, from_west) + spill,
        ],
        axis=1,
    )
    outer = jnp.where(side == 0, tile[:16], tile[2 * rows - 8 : 2 * rows + 8])
    swap = []
    for i in range(n_lat):
        swap.append((2 * i + 1, (2 * i + 2) % (2 * n_lat)))
        swap.append((2 * i, (2 * i - 1) % (2 * n_lat)))
    other = lax.ppermute(outer, LAT_OBS, swap)
    forcing, sums = basis(
        side.reshape(1), tile, other, ocean, inertia, east, south, tiles * n_obs
    )
    sums = lax.all_to_all(
        sums.reshape(tiles * n_obs, 1, 128), LAT_LON_OBS, split_axis=0, concat_axis=0, tiled=True
    ).reshape(tiles * n_obs, 128)
    return solve(sums, forcing, inertia, east, south, rows, cols)


def solution(mesh):
    split = Mesh(
        mesh.devices.reshape(mesh.shape["lat"], 4, 4, mesh.shape["obs"]),
        ("lat", "lon_0", "lon_1", "obs"),
    )
    return jax.shard_map(
        body,
        mesh=split,
        in_specs=(
            P(LAT_LON_OBS, None),
            P(LAT_LON_OBS, None),
            P(None, LAT_LON_OBS, None),
            P(LAT_LON_OBS, None),
            P(LAT_LON_OBS, None),
            P(LAT_LON_OBS),
            P(LAT_OBS, LON),
            P(LAT_OBS, LON),
            P(LAT_OBS, LON),
        ),
        out_specs=(P(LAT_OBS, LON), P(LAT_OBS, LON)),
        check_vma=False,
    )
```
